32 devices in a mesh: gx: 8 (over z, core), gy: 4 (over y, x).
Axes of the slice: x: 2, y: 2, z: 4, core: 2. Of those that a mesh axis runs over, the one named last changes fastest.
Arguments:
- earlier_heat_field: float32 [6, 1024, 512], P(None, 'gx', 'gy'), may hold values from -6 to 6
- substance_per_voxel: int32 [6, 1024, 512], P(None, 'gx', 'gy'), may hold values from 0 to 7
- patch_wattage_category: int32 [64, 32], P('gx', 'gy'), may hold values from 0 to 63
- planar_coupling: float32 [8], replicated, may hold values from 0.3 to 3
- vertical_coupling_per_substance: float32 [8], replicated, may hold values from 0.05 to 0.5
- heat_mass_ratio: float32 [8], replicated, may hold values from 2e-05 to 0.0002
- wattage_per_category: float32 [64], replicated, may hold values from 2e-06 to 2e-05
Outputs:
- temperature: float32 [6, 1024, 512], P(None, 'gx', 'gy')
The draws below stay inside these ranges and needn't reach their ends.
All inputs are finite; a program needn't handle non-finite values.
Results may differ from the reference program's by a relative error of at most 0.0003.
Values sent between devices are 32-bit elements; how exact they have to be, the bound alone decides.
No kernel may reach another device: no remote copies, remote signals or barrier semaphores. Data moves between devices by JAX's collectives and lax.ppermute only.
A program may use at most 192 MiB of HBM per device.

```python
import math
import jax
import jax.numpy as jnp
from jax import lax

DIE_COUNT = 6
MATERIALS = 8
POWER_LEVELS = 64
TILE = 16
LEVELS = 6
SWEEPS = 2
COARSE_ITERS = 12
CX = 128
GRID_LENGTH = 1024
GRID_WIDTH = 512


def draw_substance_per_voxel(key, part):
    block_key = jax.random.fold_in(key, 11)
    noise_key = jax.random.fold_in(key, 23)
    pick_key = jax.random.fold_in(key, 37)
    blocks = jax.random.randint(block_key, (DIE_COUNT, GRID_LENGTH // CX, GRID_WIDTH // CX), 0, MATERIALS)
    spread = jnp.repeat(jnp.repeat(blocks, CX, axis=1), CX, axis=2)
    shape = (DIE_COUNT, GRID_LENGTH, GRID_WIDTH)
    noise = jax.random.randint(noise_key, shape, 0, MATERIALS)
    pick = jax.random.randint(pick_key, shape, 0, 4)
    return jnp.where(pick == 0, noise, spread).astype(jnp.int32)


def plant(values, stream_key, smallest, high):
    dims = values.shape
    place = [jax.random.randint(jax.random.fold_in(stream_key, axis), (), 0, dims[axis]) for axis in range(len(dims))]
    values = values.at[tuple(place)].set(smallest)
    longest = dims.index(max(dims))
    place[longest] = (place[longest] + 1) % dims[longest]
    return values.at[tuple(place)].set(high)


def shard_levels(rng, dims, shards, least, top_value):
    loudness, own = 1.0, jax.random.fold_in(rng, 6)
    for axis_at, blocks in shards:
        draws = jnp.exp(jax.random.uniform(jax.random.fold_in(own, axis_at), (blocks,), jnp.float32, least / len(shards), top_value / len(shards)))
        loudness = loudness * jnp.repeat(draws, dims[axis_at] // blocks).reshape([-1 if axis == axis_at else 1 for axis in range(len(dims))])
    return loudness


def scatter_about(own_key, dims, width, limit, shards=(), held_as=jnp.bfloat16):
    loudness = shard_levels(own_key, dims, shards, -0.22, 0.18) if shards else 1.0
    values = jax.random.normal(own_key, dims, jnp.float32) * width * loudness
    return jnp.minimum(jnp.maximum(values, -limit), limit).astype(held_as)


def setup_inputs(seed: int = 0) -> dict:
    seeds = jax.random.split(jax.random.key(seed), 8)
    return {
        "earlier_heat_field": scatter_about(seeds[0], (DIE_COUNT, GRID_LENGTH, GRID_WIDTH), 1.0, 6.0, ((1, 8), (2, 4)), jnp.float32),
        "substance_per_voxel": draw_substance_per_voxel(jax.random.fold_in(seeds[7], 71), 0),
        "patch_wattage_category": plant(jax.random.randint(seeds[2], (GRID_LENGTH // TILE, GRID_WIDTH // TILE), 0, POWER_LEVELS), jax.random.fold_in(seeds[2], 1), 0, POWER_LEVELS - 1).astype(jnp.int32),
        "planar_coupling": jnp.clip(jnp.exp(jax.random.uniform(seeds[3], (MATERIALS,), jnp.float32, math.log(0.3), math.log(3.0))), 0.3, 3.0),
        "vertical_coupling_per_substance": jnp.clip(jnp.exp(jax.random.uniform(seeds[4], (MATERIALS,), jnp.float32, math.log(0.05), math.log(0.5))), 0.05, 0.5),
        "heat_mass_ratio": jnp.clip(jnp.exp(jax.random.uniform(seeds[5], (MATERIALS,), jnp.float32, math.log(1.9999999494757503e-05), math.log(0.0002))), 1.9999999494757503e-05, 0.0002),
        "wattage_per_category": jnp.clip(jnp.exp(jax.random.uniform(seeds[6], (POWER_LEVELS,), jnp.float32, math.log(1.9999999949504854e-06), math.log(1.9999999494757503e-05))), 1.9999999949504854e-06, 1.9999999494757503e-05),
    }


def previous(values, dimension):
    widths = [(0, 0)] * values.ndim
    widths[dimension] = (1, 0)
    return lax.slice_in_dim(jnp.pad(values, widths), 0, values.shape[dimension], axis=dimension)


def following(values, dimension):
    widths = [(0, 0)] * values.ndim
    widths[dimension] = (0, 1)
    return lax.slice_in_dim(jnp.pad(values, widths), 1, values.shape[dimension] + 1, axis=dimension)


def stencil(lateral, vertical, capacity_diagonal, inside, factor):
    row_before = factor * 0.5 * (lateral + previous(lateral, 1))
    row_after = factor * 0.5 * (lateral + following(lateral, 1))
    col_before = factor * 0.5 * (lateral + previous(lateral, 2))
    col_after = factor * 0.5 * (lateral + following(lateral, 2))
    faces = 0.5 * (vertical[1:] + vertical[:-1])
    no_face = jnp.zeros_like(vertical[:1])
    layer_below = jnp.concatenate([no_face, faces], 0)
    layer_above = jnp.concatenate([faces, no_face], 0)
    diagonal = capacity_diagonal + row_before + row_after + col_before + col_after + layer_below + layer_above
    diagonal = jnp.where(inside > 0, diagonal, 1.0)
    return (row_before, row_after, col_before, col_after, layer_below, layer_above, diagonal)


def coupled(values, weights):
    summed = weights[0] * previous(values, 1) + weights[1] * following(values, 1)
    summed = summed + weights[2] * previous(values, 2) + weights[3] * following(values, 2)
    return summed + weights[4] * previous(values, 0) + weights[5] * following(values, 0)


def parity(extent):
    summed = lax.broadcasted_iota(jnp.int32, extent, 0) + lax.broadcasted_iota(jnp.int32, extent, 1)
    return (summed + lax.broadcasted_iota(jnp.int32, extent, 2)) % 2


def restrict(values):
    layers, height, breadth = values.shape
    blocks = values.reshape(layers, height // 2, 2, breadth // 2, 2)
    return (blocks[:, :, 0, :, 0] + blocks[:, :, 1, :, 0] + blocks[:, :, 0, :, 1] + blocks[:, :, 1, :, 1]) * 0.25


def prolong(values):
    return jnp.repeat(jnp.repeat(values, 2, axis=1), 2, axis=2)


def lookup(labels, entries):
    summed = jnp.zeros(labels.shape, entries.dtype)
    for number in range(entries.shape[0]):
        summed = summed + jnp.where(labels == number, entries[number], 0.0)
    return summed


def conjugate(source_vector, weights):
    solution = jnp.zeros_like(source_vector)
    residue = source_vector
    precond = residue / weights[6]
    search = precond
    inner = jnp.sum(residue * precond)
    for step_index in range(COARSE_ITERS):
        image = weights[6] * search - coupled(search, weights)
        alpha_step = inner / jnp.sum(search * image)
        solution = solution + alpha_step * search
        residue = residue - alpha_step * image
        precond = residue / weights[6]
        inner_next = jnp.sum(residue * precond)
        search = precond + (inner_next / inner) * search
        inner = inner_next
    return solution


def smooth(present_guess, source_vector, weights, colours):
    for sweep_index in range(SWEEPS):
        for colour in (0, 1):
            candidate = (source_vector + coupled(present_guess, weights)) / weights[6]
            present_guess = jnp.where(colours == colour, candidate, present_guess)
    return present_guess


def reference(earlier_heat_field, substance_per_voxel, patch_wattage_category, planar_coupling, vertical_coupling_per_substance, heat_mass_ratio, wattage_per_category):
    lateral = lookup(substance_per_voxel, planar_coupling)
    vertical = lookup(substance_per_voxel, vertical_coupling_per_substance)
    capacity_diagonal = lookup(substance_per_voxel, heat_mass_ratio)
    heat = jnp.repeat(jnp.repeat(lookup(patch_wattage_category, wattage_per_category), TILE, axis=0), TILE, axis=1)
    source_vector = capacity_diagonal * earlier_heat_field
    source_vector = jnp.concatenate([source_vector[:1] + heat[None], source_vector[1:]], 0)
    coefficients = [(lateral, vertical, capacity_diagonal)]
    for level_index in range(LEVELS):
        last = coefficients[-1]
        coefficients.append((restrict(last[0]), restrict(last[1]), restrict(last[2])))
    present_guess = earlier_heat_field
    saved = []
    for level_index in range(LEVELS):
        level_coef = coefficients[level_index]
        weights = stencil(level_coef[0], level_coef[1], level_coef[2], jnp.ones_like(source_vector), 0.25 ** level_index)
        colours = parity(source_vector.shape)
        present_guess = smooth(present_guess, source_vector, weights, colours)
        residual = source_vector - (weights[6] * present_guess - coupled(present_guess, weights))
        saved.append((present_guess, source_vector, weights, colours))
        source_vector = restrict(residual)
        present_guess = jnp.zeros_like(source_vector)
    coarse_coef = coefficients[LEVELS]
    coarse_weights = stencil(coarse_coef[0], coarse_coef[1], coarse_coef[2], jnp.ones_like(source_vector), 0.25 ** LEVELS)
    correction = conjugate(source_vector, coarse_weights)
    for level_index in reversed(range(LEVELS)):
        present_guess, source_vector, weights, colours = saved[level_index]
        present_guess = smooth(present_guess + prolong(correction), source_vector, weights, colours)
        correction = present_guess
    return correction
```

```python
import functools

import jax
import jax.numpy as jnp
from jax import lax
from jax.experimental import pallas as pl
from jax.experimental.pallas import tpu as pltpu
from jax.sharding import PartitionSpec as P

TILE = 16
LEVELS = 6
LOCAL = 3
COARSE_ITERS = 12
LANES = 128
PAD = 8
HI = lax.Precision.HIGHEST
F32 = jnp.float32
VMEM = pl.BlockSpec(memory_space=pltpu.VMEM)
SMEM = pl.BlockSpec(memory_space=pltpu.SMEM)
PARAMS = pltpu.CompilerParams(vmem_limit_bytes=60 * 1024 * 1024)


def up8(n):
    return -(-n // 8) * 8


def halo_cells():
    need, above = [], 0
    for level in range(LOCAL):
        need.append(above + 4)
        above = -(-need[-1] // 2)
    f = 0
    for level in reversed(range(LOCAL)):
        inner = max(need[level], 2 * f + 1)
        f = inner + (4 if level == 0 else 3)
    unit = 2**LOCAL
    return -(-f // unit) * unit


def iota(shape, axis):
    return lax.broadcasted_iota(jnp.int32, shape, axis)


def rows(t, off=0):
    return pl.ds(pl.multiple_of(t * 8, 8) + (PAD + off), 8)


def dot(a, b):
    return jnp.dot(a, b, precision=HI, preferred_element_type=F32)


def prep_kernel(par, watt, cat_ref, u_ref, sub_ref, heat_ref, a_ref, b_ref, *, halo):
    layers, height, width = u_ref.shape
    cat = cat_ref[...]
    power = jnp.zeros(cat.shape, F32)
    for n in range(watt.shape[0]):
        power = power + jnp.where(cat == n, watt[n], 0.0)
    spread_r = (iota((height, cat.shape[0]), 0) // TILE == iota((height, cat.shape[0]), 1)).astype(F32)
    spread_c = (iota((cat.shape[1], width), 1) // TILE == iota((cat.shape[1], width), 0)).astype(F32)
    heat_ref[...] = dot(dot(spread_r, power), spread_c)
    even = par[0] == 0
    for q in range(2 * layers + 1):
        if q < layers:
            plane = u_ref[q]
        elif q < 2 * layers:
            plane = (sub_ref[q - layers] + 1).astype(F32)
        else:
            plane = heat_ref[...]
        turned = plane.T
        low, high = turned[:halo], turned[width - halo :]
        a_ref[q] = jnp.where(even, high, low)
        b_ref[q] = jnp.where(even, low, high)


def split_kernel(par, u_ref, sub_ref, heat_ref, ra, rb, out, a_ref, b_ref, scr, *, halo):
    layers, height, width = u_ref.shape
    even_y, even_x = par[0] == 0, par[1] == 0
    half, hh = height // 2, halo // 2
    source, target = iota((width + LANES, 2 * LANES), 0), iota((width + LANES, 2 * LANES), 1)
    cell = 2 * (target % LANES) + target // LANES
    want = jnp.where(
        cell < halo, width + cell, jnp.where(cell < halo + width, cell - halo, cell)
    )
    pick = ((source == want) & (cell < 2 * halo + width)).astype(F32)
    for q in range(2 * layers + 1):
        if q < layers:
            plane = u_ref[q]
        elif q < 2 * layers:
            plane = (sub_ref[q - layers] + 1).astype(F32)
        else:
            plane = heat_ref[...]
        left = jnp.where(even_y, rb[q], ra[q])
        right = jnp.where(even_y, ra[q], rb[q])
        sides = jnp.concatenate([left, right, jnp.zeros((LANES - 2 * halo, height), F32)], 0).T
        both = dot(jnp.concatenate([plane, sides], 1), pick)
        scr[0] = both[:, :LANES]
        scr[1] = both[:, LANES:]
        for p in range(2):
            for j in range(2):
                z = scr[j, pl.ds(p, half, stride=2), :]
                out[q, 2 * p + j] = z
                at = (4 * q + 2 * p + j) * hh
                first, last = z[:hh], z[half - hh :]
                a_ref[at : at + hh] = jnp.where(even_x, last, first)
                b_ref[at : at + hh] = jnp.where(even_x, first, last)


def split_sum(s, p, j, k, t, layers):
    u = s["u"]
    at = rows(t)
    total = s["fri"][j, k, at] * u[2 * (1 - p) + j, k, at]
    if p == 0:
        total += s["fro"][j, k, at] * u[2 + j, k, rows(t, -1)]
    else:
        total += s["fro"][j, k, rows(t, 1)] * u[j, k, rows(t, 1)]
    total += s["fci"][p, k, at] * u[2 * p + 1 - j, k, at]
    if j == 0:
        total += s["fco"][p, k, at] * pltpu.roll(u[2 * p + 1, k, at], 1, 1)
    else:
        total += s["fcr"][p, k, at] * pltpu.roll(u[2 * p, k, at], LANES - 1, 1)
    pj = 2 * p + j
    if k > 0:
        total += s["fl"][pj, k, at] * u[pj, k - 1, at]
    if k < layers - 1:
        total += s["fl"][pj, k + 1, at] * u[pj, k + 1, at]
    return total


def split_half(s, colour, lo, hi, layers):
    def body(t, carry):
        for k in range(layers):
            for p in range(2):
                for j in range(2):
                    if (p + j + k) % 2 == colour:
                        pj = 2 * p + j
                        total = s["f"][pj, k, rows(t)] + split_sum(s, p, j, k, t, layers)
                        s["u"][pj, k, rows(t)] = total * s["invd"][pj, k, rows(t)]
        return carry

    lax.fori_loop(lo, hi, body, 0)


def sides_of(tiles, lane):
    count = len(tiles)
    turned_r = [pltpu.roll(x, 1, 1) for x in tiles]
    turned_l = [pltpu.roll(x, LANES - 1, 1) for x in tiles]
    left = [
        jnp.where(lane == 0, turned_r[i - 1] if i else 0.0, turned_r[i]) for i in range(count)
    ]
    right = [
        jnp.where(lane == LANES - 1, turned_l[i + 1] if i < count - 1 else 0.0, turned_l[i])
        for i in range(count)
    ]
    return left, right


def nat_setup(s, factor):
    tiles, layers, height, _ = s["lat"].shape
    lane = iota((8, LANES), 1)
    c = 0.5 * factor

    def body(t, carry):
        for k in range(layers):
            lat = [s["lat"][i, k, rows(t)] for i in range(tiles)]
            left, right = sides_of(lat, lane)
            for i in range(tiles):
                stor = s["stor"][i, k, rows(t)]
                above = c * (lat[i] + s["lat"][i, k, rows(t, -1)])
                below = c * (lat[i] + s["lat"][i, k, rows(t, 1)])
                before, after = c * (lat[i] + left[i]), c * (lat[i] + right[i])
                diag = stor + above + below + before + after
                vert = s["vert"][i, k, rows(t)]
                if k > 0:
                    face = 0.5 * (vert + s["vert"][i, k - 1, rows(t)])
                    s["wl"][i, k, rows(t)] = face
                    diag += face
                if k < layers - 1:
                    diag += 0.5 * (vert + s["vert"][i, k + 1, rows(t)])
                inside = stor > 0.0
                s["wr"][i, k, rows(t)] = above
                s["wc"][i, k, rows(t)] = before
                s["wcr"][i, k, rows(t)] = after
                s["diag"][i, k, rows(t)] = diag
                s["invd"][i, k, rows(t)] = jnp.where(inside, 1.0 / jnp.where(inside, diag, 1.0), 0.0)
        return carry

    s["wr"][:, :, height - PAD :] = jnp.zeros((tiles, layers, PAD, LANES), F32)
    lax.fori_loop(0, (height - 2 * PAD) // 8, body, 0)


def nat_sum(s, mid, sides, i, k, t, layers):
    u = s["u"]
    total = s["wr"][i, k, rows(t)] * u[i, k, rows(t, -1)]
    total += s["wr"][i, k, rows(t, 1)] * u[i, k, rows(t, 1)]
    total += s["wc"][i, k, rows(t)] * sides[k][0][i] + s["wcr"][i, k, rows(t)] * sides[k][1][i]
    if k > 0:
        total += s["wl"][i, k, rows(t)] * mid[k - 1][i]
    if k < layers - 1:
        total += s["wl"][i, k + 1, rows(t)] * mid[k + 1][i]
    return total


def nat_half(s, colour, lo, hi):
    tiles, layers = s["u"].shape[:2]
    lane = iota((8, LANES), 1)
    odd = (iota((8, LANES), 0) + lane) % 2

    def body(t, carry):
        mid = [[s["u"][i, k, rows(t)] for i in range(tiles)] for k in range(layers)]
        sides = [sides_of(m, lane) for m in mid]
        for k in range(layers):
            chosen = odd == (colour + k) % 2
            for i in range(tiles):
                total = s["f"][i, k, rows(t)] + nat_sum(s, mid, sides, i, k, t, layers)
                s["u"][i, k, rows(t)] = jnp.where(chosen, total * s["invd"][i, k, rows(t)], mid[k][i])
        return carry

    lax.fori_loop(lo, hi, body, 0)


def nat_first(s, lo, hi):
    tiles, layers, height, _ = s["u"].shape
    odd = (iota((8, LANES), 0) + iota((8, LANES), 1)) % 2
    zeros = jnp.zeros((tiles, layers, PAD, LANES), F32)
    s["u"][:, :, :PAD] = zeros
    s["u"][:, :, height - PAD :] = zeros

    def body(t, carry):
        for k in range(layers):
            for i in range(tiles):
                value = s["f"][i, k, rows(t)] * s["invd"][i, k, rows(t)]
                s["u"][i, k, rows(t)] = jnp.where(odd == k % 2, value, 0.0)
        return carry

    lax.fori_loop(lo, hi, body, 0)


def nat_residual(s, res, lo, hi):
    tiles, layers = s["u"].shape[:2]
    lane = iota((8, LANES), 1)

    def body(t, carry):
        mid = [[s["u"][i, k, rows(t)] for i in range(tiles)] for k in range(layers)]
        sides = [sides_of(m, lane) for m in mid]
        for k in range(layers):
            for i in range(tiles):
                total = s["f"][i, k, rows(t)] + nat_sum(s, mid, sides, i, k, t, layers)
                res[i, k, rows(t)] = total - s["diag"][i, k, rows(t)] * mid[k][i]
        return carry

    lax.fori_loop(lo, hi, body, 0)


def nat_down(s, res, steps):
    nat_first(s, 0, steps)
    for colour in (1, 0, 1):
        nat_half(s, colour, 0, steps)
    nat_residual(s, res, 0, steps)


def restrict_to(source, target):
    tiles, layers = source.shape[:2]
    count, height = target.shape[0], target.shape[2] - 2 * PAD
    zeros = jnp.zeros((count, layers, PAD, LANES), F32)
    target[:, :, :PAD] = zeros
    target[:, :, PAD + height :] = zeros
    cell = iota((LANES, LANES), 0) // 2
    for k in range(layers):
        parts = [
            source[i, k, pl.ds(PAD, height, stride=2), :]
            + source[i, k, pl.ds(PAD + 1, height, stride=2), :]
            for i in range(tiles)
        ]
        for o in range(count):
            total = None
            for i in range(tiles):
                shift = LANES // 2 * i - LANES * o
                if -LANES < shift < LANES:
                    pick = jnp.where(cell + shift == iota((LANES, LANES), 1), 0.25, 0.0)
                    part = dot(parts[i], pick)
                    total = part if total is None else total + part
            target[o, k, PAD : PAD + height] = total


def prolong_into(s, u_in, coarse, mask):
    tiles, layers, height, _ = s["u"].shape
    n = (height - 2 * PAD) // 2
    cell = iota((LANES, LANES), 1) // 2
    for i in range(tiles):
        o = i // 2
        shift = LANES // 2 * (i % 2)
        pick = (cell + shift == iota((LANES, LANES), 0)).astype(F32)
        for k in range(layers):
            wide = dot(coarse(o, k)[:n], pick)
            for p in range(2):
                at = pl.ds(PAD + p, n, stride=2)
                add = wide
                if mask:
                    add = jnp.where(s["invd"][i, k, at, :] > 0.0, wide, 0.0)
                s["u"][i, k, at, :] = u_in[i, k, at, :] + add


def nat_up(s, lo, hi):
    for sweep in range(2):
        nat_half(s, 0, lo, hi)
        nat_half(s, 1, lo, hi)


SPLIT_KEPT = ("u", "f", "invd", "fri", "fro", "fci", "fco", "fcr", "fl")
NAT_KEPT = ("u", "f", "invd", "wr", "wc", "wcr", "wl")
NAT_OTHER = ("lat", "vert", "stor", "diag")


def down_kernel(par, tables, *refs, halo, half, kinds):
    refs = list(refs)
    sp, ra, rb = refs[:3]
    refs = refs[3:]
    s = dict(zip(SPLIT_KEPT, refs[: len(SPLIT_KEPT)]))
    refs = refs[len(SPLIT_KEPT) :]
    nats = []
    for level in range(1, LOCAL):
        nats.append(dict(zip(NAT_KEPT, refs[: len(NAT_KEPT)])))
        refs = refs[len(NAT_KEPT) :]
    payload = refs.pop(0)
    for name in ("lat", "vert", "stor"):
        s[name] = refs.pop(0)
    heat = refs.pop(0)
    for level in range(1, LOCAL):
        for name in NAT_OTHER:
            nats[level - 1][name] = refs.pop(0)
    ress = [refs.pop(0) for level in range(1, LOCAL)]
    layers = s["u"].shape[1]
    height = s["u"].shape[2]
    hh = halo // 2
    steps = (height - 2 * PAD) // 8
    even = par[0] == 0
    zeros = jnp.zeros((PAD, LANES), F32)

    def place(ref, index, q, pj):
        at = (4 * q + pj) * hh
        first, second = ra[at : at + hh], rb[at : at + hh]
        ref[index + (slice(PAD, PAD + hh),)] = jnp.where(even, second, first)
        ref[index + (slice(PAD + hh, PAD + hh + half),)] = sp[q, pj]
        ref[index + (slice(PAD + hh + half, PAD + 2 * hh + half),)] = jnp.where(even, first, second)

    for pj in range(4):
        for k in range(layers):
            for name in ("u", "lat"):
                s[name][pj, k, :PAD] = zeros
                s[name][pj, k, height - PAD :] = zeros
            place(s["u"], (pj, k), k, pj)
            place(s["stor"], (pj, k), layers + k, pj)
        place(heat, (pj,), 2 * layers, pj)
    for j in range(2):
        for k in range(layers):
            s["fro"][j, k, height - PAD :] = zeros

    first = nats[0]
    clear = [first[name] for name in ("lat", "vert", "stor", "f")] + ress
    for ref in clear:
        for k in range(layers):
            ref[0, k, :PAD] = zeros
            ref[0, k, ref.shape[2] - PAD :] = zeros

    def look(t, carry):
        for k in range(layers):
            sums = [None, None, None]
            for pj in range(4):
                at = (pj, k, rows(t))
                label = s["stor"][at]
                value = [jnp.zeros_like(label)] * 3
                for n in range(kinds):
                    hit = label == float(n + 1)
                    value = [jnp.where(hit, tables[i * kinds + n], value[i]) for i in range(3)]
                for i, name in enumerate(("lat", "vert", "stor")):
                    s[name][at] = value[i]
                    sums[i] = value[i] if sums[i] is None else sums[i] + value[i]
                f = value[2] * s["u"][at]
                if k == 0:
                    f = f + heat[pj, rows(t)]
                s["f"][at] = f
            for i, name in enumerate(("lat", "vert", "stor")):
                first[name][0, k, rows(t)] = sums[i] * 0.25
        return carry

    lax.fori_loop(0, steps, look, 0)

    def faces(t, carry):
        at = rows(t)
        for k in range(layers):
            lat = [s["lat"][pj, k, at] for pj in range(4)]
            inner_r = [0.5 * (lat[j] + lat[2 + j]) for j in range(2)]
            before_r = [0.5 * (s["lat"][2 + j, k, rows(t, -1)] + lat[j]) for j in range(2)]
            after_r = [0.5 * (lat[2 + j] + s["lat"][j, k, rows(t, 1)]) for j in range(2)]
            inner_c = [0.5 * (lat[2 * p] + lat[2 * p + 1]) for p in range(2)]
            before_c = [0.5 * (pltpu.roll(lat[2 * p + 1], 1, 1) + lat[2 * p]) for p in range(2)]
            after_c = [0.5 * (lat[2 * p + 1] + pltpu.roll(lat[2 * p], LANES - 1, 1)) for p in range(2)]
            for x in range(2):
                s["fri"][x, k, at] = inner_r[x]
                s["fro"][x, k, at] = before_r[x]
                s["fci"][x, k, at] = inner_c[x]
                s["fco"][x, k, at] = before_c[x]
                s["fcr"][x, k, at] = after_c[x]
            for p in range(2):
                for j in range(2):
                    pj = 2 * p + j
                    stor = s["stor"][pj, k, at]
                    diag = stor + inner_r[j] + (after_r[j] if p else before_r[j])
                    diag += inner_c[p] + (after_c[p] if j else before_c[p])
                    vert = s["vert"][pj, k, at]
                    if k > 0:
                        face = 0.5 * (vert + s["vert"][pj, k - 1, at])
                        s["fl"][pj, k, at] = face
                        diag += face
                    if k < layers - 1:
                        diag += 0.5 * (vert + s["vert"][pj, k + 1, at])
                    inside = stor > 0.0
                    s["invd"][pj, k, at] = jnp.where(inside, 1.0 / jnp.where(inside, diag, 1.0), 0.0)
                    s["stor"][pj, k, at] = diag
        return carry

    lax.fori_loop(0, steps, faces, 0)
    for sweep in range(2):
        split_half(s, 0, 0, steps, layers)
        split_half(s, 1, 0, steps, layers)

    def remain(t, carry):
        for k in range(layers):
            total = None
            for p in range(2):
                for j in range(2):
                    if (p + j + k) % 2 == 0:
                        pj = 2 * p + j
                        r = s["f"][pj, k, rows(t)] + split_sum(s, p, j, k, t, layers)
                        r -= s["stor"][pj, k, rows(t)] * s["u"][pj, k, rows(t)]
                        total = r if total is None else total + r
            first["f"][0, k, rows(t)] = total * 0.25
        return carry

    lax.fori_loop(0, steps, remain, 0)

    for level in range(1, LOCAL):
        now = nats[level - 1]
        nat_setup(now, 0.25**level)
        count = (now["u"].shape[2] - 2 * PAD) // 8
        nat_down(now, ress[level - 1], count)
        if level < LOCAL - 1:
            below = nats[level]
            for name in ("lat", "vert", "stor"):
                restrict_to(now[name], below[name])
            restrict_to(ress[level - 1], below["f"])

    last, res = nats[-1], ress[-1]
    mine = 2 * half >> LOCAL
    off = halo >> (LOCAL - 1)
    group = 4 * mine
    per = LANES // group
    quantities = (res, last["lat"], last["vert"], last["stor"])
    source, target = iota((LANES, LANES), 0), iota((LANES, LANES), 1)
    for pair in range(-(-layers // per)):
        total = jnp.zeros((mine, LANES), F32)
        for inner in range(per):
            k = pair * per + inner
            if k < layers:
                for n, ref in enumerate(quantities):
                    base = inner * group + n * mine
                    hit = (target >= base) & (target < base + mine)
                    hit &= (source - off >= 0) & ((source - off) // 2 == target - base)
                    pick = jnp.where(hit, 0.25, 0.0)
                    part = ref[0, k, pl.ds(PAD + off, mine, stride=2), :]
                    part += ref[0, k, pl.ds(PAD + off + 1, mine, stride=2), :]
                    total += dot(part, pick)
        payload[pair * mine : (pair + 1) * mine] = total


def conjugate(s):
    tiles, layers, height, _ = s["u"].shape
    n = height - 2 * PAD
    row, lane = iota((n, LANES), 0), iota((n, LANES), 1)
    spots = [(i, k) for k in range(layers) for i in range(tiles)]
    body_rows = slice(PAD, PAD + n)

    def apply(v):
        out = []
        for k in range(layers):
            tiles_of = [v[k * tiles + i] for i in range(tiles)]
            left, right = sides_of(tiles_of, lane)
            for i in range(tiles):
                mid = tiles_of[i]
                wr = s["wr"][i, k, body_rows]
                wr_next = s["wr"][i, k, slice(PAD + 1, PAD + 1 + n)]
                total = wr * jnp.where(row == 0, 0.0, pltpu.roll(mid, 1, 0))
                total += wr_next * jnp.where(row == n - 1, 0.0, pltpu.roll(mid, n - 1, 0))
                total += s["wc"][i, k, body_rows] * left[i] + s["wcr"][i, k, body_rows] * right[i]
                if k > 0:
                    total += s["wl"][i, k, body_rows] * v[(k - 1) * tiles + i]
                if k < layers - 1:
                    total += s["wl"][i, k + 1, body_rows] * v[(k + 1) * tiles + i]
                out.append(s["diag"][i, k, body_rows] * mid - total)
        return out

    def inner(a, b):
        total = a[0] * b[0]
        for x, y in zip(a[1:], b[1:]):
            total += x * y
        total = jnp.sum(total, axis=0, keepdims=True)
        return jnp.sum(total, axis=1, keepdims=True)

    inv = [s["invd"][i, k, body_rows] for i, k in spots]
    inside = [x > 0.0 for x in inv]
    r = [jnp.where(inside[m], s["f"][i, k, body_rows], 0.0) for m, (i, k) in enumerate(spots)]
    z = [x * y for x, y in zip(r, inv)]
    count = len(spots)

    def step(_, carry):
        e, r, p, rz = carry[:count], carry[count : 2 * count], carry[2 * count : 3 * count], carry[-1]
        q = apply(p)
        alpha = rz / inner(p, q)
        e = [x + alpha * y for x, y in zip(e, p)]
        r = [jnp.where(m, x - alpha * y, 0.0) for m, x, y in zip(inside, r, q)]
        z = [x * s["invd"][i, k, body_rows] for x, (i, k) in zip(r, spots)]
        fresh = inner(r, z)
        beta = fresh / rz
        p = [x + beta * y for x, y in zip(z, p)]
        return (*e, *r, *p, fresh)

    start = (*[jnp.zeros_like(x) for x in r], *r, *z, inner(r, z))
    out = lax.fori_loop(0, COARSE_ITERS, step, start)
    for (i, k), value in zip(spots, out[:count]):
        s["u"][i, k, body_rows] = value


WHOLE = ("u", "f", "invd", "wr", "wc", "wcr", "wl", "lat", "vert", "stor", "diag")


def up_kernel(place, *refs, halo, half, spans):
    refs = list(refs)
    gathered = refs.pop(0)
    s = dict(zip(SPLIT_KEPT, refs[: len(SPLIT_KEPT)]))
    refs = refs[len(SPLIT_KEPT) :]
    nats = []
    for level in range(1, LOCAL):
        nats.append(dict(zip(NAT_KEPT, refs[: len(NAT_KEPT)])))
        refs = refs[len(NAT_KEPT) :]
    out = refs.pop(0)
    wholes = []
    for level in range(LOCAL, LEVELS + 1):
        wholes.append(dict(zip(WHOLE, refs[: len(WHOLE)])))
        refs = refs[len(WHOLE) :]
    ress = [refs.pop(0) for level in range(LOCAL, LEVELS)]
    fresh = [refs.pop(0) for level in range(LOCAL)]
    wider = refs.pop(0)
    nx, ny = spans
    layers = s["u"].shape[1]
    top = wholes[0]
    tiles, _, tall, _ = top["u"].shape
    mine = 2 * half >> LOCAL
    group = 4 * mine
    per = LANES // group
    lane = iota((mine, LANES), 1)

    for whole in wholes:
        count, _, height, _ = whole["u"].shape
        for name in ("u", "lat"):
            zeros = jnp.zeros((count, layers, PAD, LANES), F32)
            whole[name][:, :, :PAD] = zeros
            whole[name][:, :, height - PAD :] = zeros

    def gather(x, carry):
        at = pl.ds(pl.multiple_of(x * mine, 8) + PAD, mine)
        for k in range(layers):
            for n, name in enumerate(("f", "lat", "vert", "stor")):
                base = (k % per) * group + n * mine
                lines = slice((k // per) * mine, (k // per + 1) * mine)
                for i in range(tiles):
                    total = jnp.zeros((mine, LANES), F32)
                    for y in range(ny):
                        if y * mine // LANES == i:
                            to = y * mine % LANES
                            part = gathered[x * ny + y, lines]
                            if to != base:
                                part = pltpu.roll(part, (to - base) % LANES, 1)
                            total = jnp.where((lane >= to) & (lane < to + mine), part, total)
                    top[name][i, k, at] = total
        return carry

    lax.fori_loop(0, nx, gather, 0)

    for n, level in enumerate(range(LOCAL, LEVELS)):
        now, below = wholes[n], wholes[n + 1]
        nat_setup(now, 0.25**level)
        nat_down(now, ress[n], (now["u"].shape[2] - 2 * PAD) // 8)
        for name in ("lat", "vert", "stor"):
            restrict_to(now[name], below[name])
        restrict_to(ress[n], below["f"])
    nat_setup(wholes[-1], 0.25**LEVELS)
    conjugate(wholes[-1])
    for n in reversed(range(len(wholes) - 1)):
        now, below = wholes[n], wholes[n + 1]
        prolong_into(now, now["u"], lambda o, k: below["u"][o, k, PAD : below["u"].shape[2] - PAD], False)
        nat_up(now, 0, (now["u"].shape[2] - 2 * PAD) // 8)

    x, y = place[0], place[1]
    reach = halo >> LOCAL
    need = (nats[-1]["u"].shape[2] - 2 * PAD) // 2
    height = top["u"].shape[2]
    for i in range(tiles):
        for k in range(layers):
            wider[i, k, :height] = top["u"][i, k]
            wider[i, k, height:] = jnp.zeros((PAD, LANES), F32)
    begin = PAD + x * mine - reach
    shift = y * mine - reach

    def window(o, k):
        parts = [wider[i, k, pl.ds(begin, need)] for i in range(tiles)]
        turn = lax.rem(4 * LANES - shift, LANES)
        lanes = iota((need, LANES), 1)
        first = lax.div(shift + LANES, LANES) - 1
        value = jnp.zeros((need, LANES), F32)
        for i in range(tiles):
            moved = pltpu.roll(parts[i], turn, 1)
            value = jnp.where((first == i) & (lanes < turn) | (first == i) & (turn == 0), moved, value)
            value = jnp.where((first == i - 1) & (lanes >= turn) & (turn != 0), moved, value)
        return value

    coarse = window
    for level in reversed(range(1, LOCAL)):
        now = dict(nats[level - 1])
        before = now["u"]
        now["u"] = fresh[level]
        height = before.shape[2]
        for i in range(before.shape[0]):
            for k in range(layers):
                now["u"][i, k, :PAD] = jnp.zeros((PAD, LANES), F32)
                now["u"][i, k, height - PAD :] = jnp.zeros((PAD, LANES), F32)
        prolong_into(now, before, coarse, level == LOCAL - 1)
        side = halo >> level
        own = 2 * half >> level
        margin = {0: 4, 1: 6, 2: 7}.get(level, 8)
        nat_up(now, (side - margin) // 8, min(-(-(side + own + margin) // 8), (height - 2 * PAD) // 8))
        coarse = functools.partial(lambda ref, o, k: ref[o, k, PAD : ref.shape[2] - PAD], now["u"])

    now = dict(s)
    now["u"] = fresh[0]
    hh = halo // 2
    lo, hi = (hh - 2) // 8, -(-(hh + half + 2) // 8)
    steps = (s["u"].shape[2] - 2 * PAD) // 8

    def add(t, carry):
        for k in range(layers):
            value = fresh[1][0, k, rows(t)]
            for pj in range(4):
                now["u"][pj, k, rows(t)] = s["u"][pj, k, rows(t)] + value
        return carry

    lax.fori_loop(lo - 1, min(hi + 1, steps), add, 0)
    for sweep in range(2):
        split_half(now, 0, lo, hi, layers)
        split_half(now, 1, lo, hi, layers)
    source, target = iota((2 * LANES, 2 * half), 0), iota((2 * LANES, 2 * half), 1)
    pick = ((source % LANES == hh + target // 2) & (source // LANES == target % 2)).astype(F32)
    for k in range(layers):
        for p in range(2):
            body_rows = slice(PAD + hh, PAD + hh + half)
            both = jnp.concatenate([now["u"][2 * p, k, body_rows], now["u"][2 * p + 1, k, body_rows]], 1)
            out[k, pl.ds(p, half, stride=2), :] = dot(both, pick)


def swap(values, axis, first):
    count = lax.axis_size(axis)
    pairs = [(i, i + 1) for i in range(first, count - 1, 2)]
    return lax.ppermute(values, axis, pairs + [(b, a) for a, b in pairs])


def shape(*dims):
    return jax.ShapeDtypeStruct(dims, F32)


def on_device(u0, sub, cat, planar, vertical, ratio, watt):
    nx, ny = lax.axis_size("gx"), lax.axis_size("gy")
    gx, gy = lax.axis_index("gx"), lax.axis_index("gy")
    layers, height, width = u0.shape
    halo = halo_cells()
    half, hh = height // 2, halo // 2
    planes = 2 * layers + 1
    assert height == width == LANES and 2 * halo <= LANES and halo + half <= LANES
    par = jnp.stack([gy % 2, gx % 2]).astype(jnp.int32)

    heat, a, b = pl.pallas_call(
        functools.partial(prep_kernel, halo=halo),
        out_shape=(shape(height, width), shape(planes, halo, height), shape(planes, halo, height)),
        in_specs=[SMEM, SMEM, VMEM, VMEM, VMEM],
        out_specs=(VMEM,) * 3,
        compiler_params=PARAMS,
        name="prep",
    )(par, watt, cat, u0, sub)
    a, b = swap(a, "gy", 0), swap(b, "gy", 1)

    lines = planes * 4 * hh
    sp, a, b = pl.pallas_call(
        functools.partial(split_kernel, halo=halo),
        out_shape=(shape(planes, 4, half, LANES), shape(lines, LANES), shape(lines, LANES)),
        in_specs=[SMEM] + [VMEM] * 5,
        out_specs=(VMEM,) * 3,
        scratch_shapes=[pltpu.VMEM((2, height, LANES), F32)],
        compiler_params=PARAMS,
        name="split",
    )(par, u0, sub, heat, a, b)
    a, b = swap(a, "gx", 0), swap(b, "gx", 1)

    tall = up8(half + 2 * hh) + 2 * PAD
    four, two = (4, layers, tall, LANES), (2, layers, tall, LANES)
    split_shapes = [four if name in ("u", "f", "invd", "fl") else two for name in SPLIT_KEPT]
    nat_shapes = [
        (1, layers, up8((height + 2 * halo) >> level) + 2 * PAD, LANES) for level in range(1, LOCAL)
    ]
    mine = height >> LOCAL
    per = LANES // (4 * mine)
    pairs = -(-layers // per)
    kept = [shape(*d) for d in split_shapes]
    for d in nat_shapes:
        kept += [shape(*d)] * len(NAT_KEPT)
    scratch = [pltpu.VMEM(four, F32)] * 3 + [pltpu.VMEM((4, tall, LANES), F32)]
    for d in nat_shapes:
        scratch += [pltpu.VMEM(d, F32)] * len(NAT_OTHER)
    scratch += [pltpu.VMEM(d, F32) for d in nat_shapes]
    tables = jnp.concatenate([planar, vertical, ratio])
    *saved, payload = pl.pallas_call(
        functools.partial(
            down_kernel, halo=halo, half=half, kinds=planar.shape[0]
        ),
        out_shape=(*kept, shape(pairs * mine, LANES)),
        in_specs=[SMEM, SMEM, VMEM, VMEM, VMEM],
        out_specs=(VMEM,) * (len(kept) + 1),
        scratch_shapes=scratch,
        compiler_params=PARAMS,
        name="down",
    )(par[1:], tables, sp, a, b)

    sent = jnp.broadcast_to(payload[None], (nx * ny,) + payload.shape)
    gathered = lax.all_to_all(sent, ("gx", "gy"), 0, 0)

    scratch = []
    for level in range(LOCAL, LEVELS + 1):
        wide = -(-(ny * width >> level) // LANES)
        d = (wide, layers, up8(nx * height >> level) + 2 * PAD, LANES)
        scratch += [pltpu.VMEM(d, F32)] * len(WHOLE)
    for level in range(LOCAL, LEVELS):
        wide = -(-(ny * width >> level) // LANES)
        scratch.append(pltpu.VMEM((wide, layers, up8(nx * height >> level) + 2 * PAD, LANES), F32))
    scratch += [pltpu.VMEM(four, F32)] + [pltpu.VMEM(d, F32) for d in nat_shapes]
    wide, count, rows_of, _ = scratch[0].shape
    scratch.append(pltpu.VMEM((wide, count, rows_of + PAD, LANES), F32))
    return pl.pallas_call(
        functools.partial(up_kernel, halo=halo, half=half, spans=(nx, ny)),
        out_shape=shape(layers, height, width),
        in_specs=[SMEM] + [VMEM] * (1 + len(kept)),
        out_specs=VMEM,
        scratch_shapes=scratch,
        compiler_params=PARAMS,
        name="up",
    )(jnp.stack([gx, gy]).astype(jnp.int32), gathered, *saved)


def solution(mesh):
    placed = (P(None, "gx", "gy"), P(None, "gx", "gy"), P("gx", "gy"), P(), P(), P(), P())
    return jax.shard_map(
        on_device, mesh=mesh, in_specs=placed, out_specs=P(None, "gx", "gy"), check_vma=False
    )
```

```python
import functools
import math

import jax
import jax.numpy as jnp
from jax import lax
from jax.experimental import pallas as pl
from jax.experimental.pallas import tpu as pltpu
from jax.sharding import PartitionSpec as P

TILE = 16
LEVELS = 6
LOCAL = 3
COARSE_ITERS = 12
LANES = 128
PAD = 8
MOST = dict(split=3, nat=4, first=4, residual=4, setup=4, look=2, faces=2, remain=3, add=4)
HI = lax.Precision.HIGHEST
F32 = jnp.float32
VMEM = pl.BlockSpec(memory_space=pltpu.VMEM)
SMEM = pl.BlockSpec(memory_space=pltpu.SMEM)


def limit(mib, scratch=()):
    held = sum(4 * math.prod(ref.shape) for ref in scratch)
    return pltpu.CompilerParams(vmem_limit_bytes=mib * 1024 * 1024 + held + held // 4)


def up8(n):
    return -(-n // 8) * 8


def halo_cells():
    need, above = [], 0
    for level in range(LOCAL):
        need.append(above + 4)
        above = -(-need[-1] // 2)
    f = 0
    for level in reversed(range(LOCAL)):
        inner = max(need[level], 2 * f + 1)
        f = inner + (4 if level == 0 else 3)
    unit = 2**LOCAL
    return -(-f // unit) * unit


def iota(shape, axis):
    return lax.broadcasted_iota(jnp.int32, shape, axis)


def rows(t, off=0):
    first, count = t
    start = first * 8 if isinstance(first, int) else pl.multiple_of(first * 8, 8)
    return pl.ds(start + (PAD + off), 8 * count)


def over(lo, hi, most, body):
    steps = -(-(hi - lo) // most)
    size = -(-(hi - lo) // steps)
    if steps == 1:
        body((lo, size))
        return

    def step(i, carry):
        body((jnp.minimum(lo + i * size, hi - size), size))
        return carry

    lax.fori_loop(0, steps, step, 0)


def dot(a, b):
    return jnp.dot(a, b, precision=HI, preferred_element_type=F32)


def pick_dot(x, pick, pieces=3):
    pick = pick.astype(jnp.bfloat16)
    total = None
    for n in range(pieces):
        piece = x.astype(jnp.bfloat16)
        part = jnp.dot(piece, pick, preferred_element_type=F32)
        total = part if total is None else total + part
        if n < pieces - 1:
            x = x - piece.astype(F32)
    return total


def prep_kernel(watt, cat_ref, u_ref, sub_ref, heat_ref, a_ref, b_ref, *, halo):
    layers, height, width = u_ref.shape
    cat = cat_ref[...]
    power = jnp.zeros(cat.shape, F32)
    for n in range(watt.shape[0]):
        power = power + jnp.where(cat == n, watt[n], 0.0)
    spread_r = (iota((height, cat.shape[0]), 0) // TILE == iota((height, cat.shape[0]), 1)).astype(F32)
    spread_c = (iota((cat.shape[1], width), 1) // TILE == iota((cat.shape[1], width), 0)).astype(F32)
    heat_ref[...] = dot(dot(spread_r, power), spread_c)
    even = lax.axis_index("gy") % 2 == 0
    for q in range(2 * layers + 1):
        if q < layers:
            plane = u_ref[q]
        elif q < 2 * layers:
            plane = (sub_ref[q - layers] + 1).astype(F32)
        else:
            plane = heat_ref[...]
        turned = plane.T
        low, high = turned[:halo], turned[width - halo :]
        a_ref[q] = jnp.where(even, high, low)
        b_ref[q] = jnp.where(even, low, high)


def split_kernel(u_ref, sub_ref, heat_ref, ra, rb, out, a_ref, b_ref, scr, *, halo):
    layers, height, width = u_ref.shape
    even_y, even_x = lax.axis_index("gy") % 2 == 0, lax.axis_index("gx") % 2 == 0
    half, hh = height // 2, halo // 2
    source, target = iota((width + LANES, 2 * LANES), 0), iota((width + LANES, 2 * LANES), 1)
    cell = 2 * (target % LANES) + target // LANES
    want = jnp.where(
        cell < halo, width + cell, jnp.where(cell < halo + width, cell - halo, cell)
    )
    pick = ((source == want) & (cell < 2 * halo + width)).astype(F32)
    planes = []
    for q in range(2 * layers + 1):
        if q < layers:
            plane = u_ref[q]
        elif q < 2 * layers:
            plane = (sub_ref[q - layers] + 1).astype(F32)
        else:
            plane = heat_ref[...]
        left = jnp.where(even_y, rb[q], ra[q])
        right = jnp.where(even_y, ra[q], rb[q])
        sides = jnp.concatenate([left, right, jnp.zeros((LANES - 2 * halo, height), F32)], 0).T
        planes.append(jnp.concatenate([plane, sides], 1))
    first = pick_dot(jnp.concatenate(planes[:layers] + planes[2 * layers :], 0), pick)
    second = pick_dot(jnp.concatenate(planes[layers : 2 * layers], 0), pick, 1)
    for q in range(2 * layers + 1):
        if layers <= q < 2 * layers:
            both = second[(q - layers) * height : (q - layers + 1) * height]
        else:
            at = q if q < layers else layers
            both = first[at * height : (at + 1) * height]
        scr[q % 2, 0] = both[:, :LANES]
        scr[q % 2, 1] = both[:, LANES:]
        for p in range(2):
            for j in range(2):
                z = scr[q % 2, j, pl.ds(p, half, stride=2), :]
                out[q, 2 * p + j] = z
                at = (4 * q + 2 * p + j) * hh
                first_rows, last_rows = z[:hh], z[half - hh :]
                a_ref[at : at + hh] = jnp.where(even_x, last_rows, first_rows)
                b_ref[at : at + hh] = jnp.where(even_x, first_rows, last_rows)


def split_sum(s, p, j, k, t, layers):
    u = s["u"]
    at = rows(t)
    total = s["fri"][j, k, at] * u[2 * (1 - p) + j, k, at]
    if p == 0:
        total += s["fro"][j, k, at] * u[2 + j, k, rows(t, -1)]
    else:
        total += s["fro"][j, k, rows(t, 1)] * u[j, k, rows(t, 1)]
    total += s["fci"][p, k, at] * u[2 * p + 1 - j, k, at]
    if j == 0:
        total += s["fco"][p, k, at] * pltpu.roll(u[2 * p + 1, k, at], 1, 1)
    else:
        total += s["fcr"][p, k, at] * pltpu.roll(u[2 * p, k, at], LANES - 1, 1)
    pj = 2 * p + j
    if k > 0:
        total += s["fl"][pj, k, at] * u[pj, k - 1, at]
    if k < layers - 1:
        total += s["fl"][pj, k + 1, at] * u[pj, k + 1, at]
    return total


def split_half(s, colour, lo, hi, layers):
    def body(t):
        for k in range(layers):
            for p in range(2):
                for j in range(2):
                    if (p + j + k) % 2 == colour:
                        pj = 2 * p + j
                        total = s["f"][pj, k, rows(t)] + split_sum(s, p, j, k, t, layers)
                        s["u"][pj, k, rows(t)] = total * s["invd"][pj, k, rows(t)]

    over(lo, hi, MOST["split"], body)


def sides_of(tiles, lane):
    count = len(tiles)
    turned_r = [pltpu.roll(x, 1, 1) for x in tiles]
    turned_l = [pltpu.roll(x, LANES - 1, 1) for x in tiles]
    left = [
        jnp.where(lane == 0, turned_r[i - 1] if i else 0.0, turned_r[i]) for i in range(count)
    ]
    right = [
        jnp.where(lane == LANES - 1, turned_l[i + 1] if i < count - 1 else 0.0, turned_l[i])
        for i in range(count)
    ]
    return left, right


def nat_setup(s, factor):
    tiles, layers, height, _ = s["lat"].shape
    c = 0.5 * factor

    def body(t):
        lane = iota((8 * t[1], LANES), 1)
        for k in range(layers):
            lat = [s["lat"][i, k, rows(t)] for i in range(tiles)]
            left, right = sides_of(lat, lane)
            for i in range(tiles):
                stor = s["stor"][i, k, rows(t)]
                above = c * (lat[i] + s["lat"][i, k, rows(t, -1)])
                below = c * (lat[i] + s["lat"][i, k, rows(t, 1)])
                before, after = c * (lat[i] + left[i]), c * (lat[i] + right[i])
                diag = stor + above + below + before + after
                vert = s["vert"][i, k, rows(t)]
                if k > 0:
                    face = 0.5 * (vert + s["vert"][i, k - 1, rows(t)])
                    s["wl"][i, k, rows(t)] = face
                    diag += face
                if k < layers - 1:
                    diag += 0.5 * (vert + s["vert"][i, k + 1, rows(t)])
                inside = stor > 0.0
                s["wr"][i, k, rows(t)] = above
                s["wc"][i, k, rows(t)] = before
                s["wcr"][i, k, rows(t)] = after
                s["diag"][i, k, rows(t)] = diag
                s["invd"][i, k, rows(t)] = jnp.where(inside, 1.0 / jnp.where(inside, diag, 1.0), 0.0)

    s["wr"][:, :, height - PAD :] = jnp.zeros((tiles, layers, PAD, LANES), F32)
    over(0, (height - 2 * PAD) // 8, MOST["setup"], body)


def nat_sum(s, mid, sides, i, k, t, layers):
    u = s["u"]
    total = s["wr"][i, k, rows(t)] * u[i, k, rows(t, -1)]
    total += s["wr"][i, k, rows(t, 1)] * u[i, k, rows(t, 1)]
    total += s["wc"][i, k, rows(t)] * sides[k][0][i] + s["wcr"][i, k, rows(t)] * sides[k][1][i]
    if k > 0:
        total += s["wl"][i, k, rows(t)] * mid[k - 1][i]
    if k < layers - 1:
        total += s["wl"][i, k + 1, rows(t)] * mid[k + 1][i]
    return total


def nat_half(s, colour, lo, hi):
    tiles, layers = s["u"].shape[:2]

    def body(t):
        lane = iota((8 * t[1], LANES), 1)
        odd = (iota((8 * t[1], LANES), 0) + lane) % 2
        mid = [[s["u"][i, k, rows(t)] for i in range(tiles)] for k in range(layers)]
        sides = [sides_of(m, lane) for m in mid]
        for k in range(layers):
            chosen = odd == (colour + k) % 2
            for i in range(tiles):
                total = s["f"][i, k, rows(t)] + nat_sum(s, mid, sides, i, k, t, layers)
                s["u"][i, k, rows(t)] = jnp.where(chosen, total * s["invd"][i, k, rows(t)], mid[k][i])

    over(lo, hi, MOST["nat"], body)


def nat_first(s, lo, hi):
    tiles, layers, height, _ = s["u"].shape
    zeros = jnp.zeros((tiles, layers, PAD, LANES), F32)
    s["u"][:, :, :PAD] = zeros
    s["u"][:, :, height - PAD :] = zeros

    def body(t):
        odd = (iota((8 * t[1], LANES), 0) + iota((8 * t[1], LANES), 1)) % 2
        for k in range(layers):
            for i in range(tiles):
                value = s["f"][i, k, rows(t)] * s["invd"][i, k, rows(t)]
                s["u"][i, k, rows(t)] = jnp.where(odd == k % 2, value, 0.0)

    over(lo, hi, MOST["first"], body)


def nat_residual(s, res, lo, hi):
    tiles, layers = s["u"].shape[:2]

    def body(t):
        lane = iota((8 * t[1], LANES), 1)
        mid = [[s["u"][i, k, rows(t)] for i in range(tiles)] for k in range(layers)]
        sides = [sides_of(m, lane) for m in mid]
        for k in range(layers):
            for i in range(tiles):
                total = s["f"][i, k, rows(t)] + nat_sum(s, mid, sides, i, k, t, layers)
                res[i, k, rows(t)] = total - s["diag"][i, k, rows(t)] * mid[k][i]

    over(lo, hi, MOST["residual"], body)


def nat_down(s, res, steps):
    nat_first(s, 0, steps)
    for colour in (1, 0, 1):
        nat_half(s, colour, 0, steps)
    nat_residual(s, res, 0, steps)


def restrict_all(pairs):
    tiles, layers = pairs[0][0].shape[:2]
    count, height = pairs[0][1].shape[0], pairs[0][1].shape[2] - 2 * PAD
    zeros = jnp.zeros((count, layers, PAD, LANES), F32)
    parts = [[] for i in range(tiles)]
    for source, target in pairs:
        target[:, :, :PAD] = zeros
        target[:, :, PAD + height :] = zeros
        for k in range(layers):
            for i in range(tiles):
                part = source[i, k, pl.ds(PAD, height, stride=2), :]
                parts[i].append(part + source[i, k, pl.ds(PAD + 1, height, stride=2), :])
    parts = [jnp.concatenate(p, 0) for p in parts]
    cell = iota((LANES, LANES), 0) // 2
    for o in range(count):
        total = None
        for i in range(tiles):
            shift = LANES // 2 * i - LANES * o
            if -LANES < shift < LANES:
                pick = jnp.where(cell + shift == iota((LANES, LANES), 1), 0.25, 0.0)
                part = pick_dot(parts[i], pick)
                total = part if total is None else total + part
        for n, (_, target) in enumerate(pairs):
            for k in range(layers):
                at = (n * layers + k) * height
                target[o, k, PAD : PAD + height] = total[at : at + height]


def prolong_into(s, u_in, coarse, mask):
    tiles, layers, height, _ = s["u"].shape
    n = (height - 2 * PAD) // 2
    tall = up8(n)
    cell = iota((LANES, LANES), 1) // 2
    for i in range(tiles):
        o = i // 2
        shift = LANES // 2 * (i % 2)
        pick = (cell + shift == iota((LANES, LANES), 0)).astype(F32)
        every = pick_dot(jnp.concatenate([coarse(o, k)[:tall] for k in range(layers)], 0), pick)
        for k in range(layers):
            wide = every[k * tall : k * tall + n]
            for p in range(2):
                at = pl.ds(PAD + p, n, stride=2)
                add = wide
                if mask:
                    add = jnp.where(s["invd"][i, k, at, :] > 0.0, wide, 0.0)
                s["u"][i, k, at, :] = u_in[i, k, at, :] + add


def nat_up(s, lo, hi):
    for sweep in range(2):
        nat_half(s, 0, lo, hi)
        nat_half(s, 1, lo, hi)


SPLIT_KEPT = ("u", "f", "invd", "fri", "fro", "fci", "fco", "fcr", "fl")
NAT_KEPT = ("u", "f", "invd", "wr", "wc", "wcr", "wl")
NAT_OTHER = ("lat", "vert", "stor", "diag")


def down_kernel(*refs, halo, half, kinds):
    tables, (sp, ra, rb) = refs[:3], refs[3:6]
    refs = list(refs[6:])
    s = dict(zip(SPLIT_KEPT, refs[: len(SPLIT_KEPT)]))
    refs = refs[len(SPLIT_KEPT) :]
    nats = []
    for level in range(1, LOCAL):
        nats.append(dict(zip(NAT_KEPT, refs[: len(NAT_KEPT)])))
        refs = refs[len(NAT_KEPT) :]
    payload = refs.pop(0)
    for name in ("lat", "vert", "stor"):
        s[name] = refs.pop(0)
    heat = refs.pop(0)
    for level in range(1, LOCAL):
        for name in NAT_OTHER:
            nats[level - 1][name] = refs.pop(0)
    ress = [refs.pop(0) for level in range(1, LOCAL)]
    layers = s["u"].shape[1]
    height = s["u"].shape[2]
    hh = halo // 2
    steps = (height - 2 * PAD) // 8
    even = lax.axis_index("gx") % 2 == 0
    zeros = jnp.zeros((PAD, LANES), F32)

    def place(ref, index, q, pj):
        at = (4 * q + pj) * hh
        first, second = ra[at : at + hh], rb[at : at + hh]
        ref[index + (slice(PAD, PAD + hh),)] = jnp.where(even, second, first)
        ref[index + (slice(PAD + hh, PAD + hh + half),)] = sp[q, pj]
        ref[index + (slice(PAD + hh + half, PAD + 2 * hh + half),)] = jnp.where(even, first, second)

    for pj in range(4):
        for k in range(layers):
            for name in ("u", "lat"):
                s[name][pj, k, :PAD] = zeros
                s[name][pj, k, height - PAD :] = zeros
            place(s["u"], (pj, k), k, pj)
            place(s["stor"], (pj, k), layers + k, pj)
        place(heat, (pj,), 2 * layers, pj)
    for j in range(2):
        for k in range(layers):
            s["fro"][j, k, height - PAD :] = zeros

    first = nats[0]
    clear = [first[name] for name in ("lat", "vert", "stor", "f")] + ress
    for ref in clear:
        for k in range(layers):
            ref[0, k, :PAD] = zeros
            ref[0, k, ref.shape[2] - PAD :] = zeros

    def look(t):
        for k in range(layers):
            sums = [None, None, None]
            for pj in range(4):
                at = (pj, k, rows(t))
                label = s["stor"][at]
                value = [jnp.zeros_like(label)] * 3
                for n in range(kinds):
                    hit = label == float(n + 1)
                    value = [jnp.where(hit, tables[i][n], value[i]) for i in range(3)]
                for i, name in enumerate(("lat", "vert", "stor")):
                    s[name][at] = value[i]
                    sums[i] = value[i] if sums[i] is None else sums[i] + value[i]
                f = value[2] * s["u"][at]
                if k == 0:
                    f = f + heat[pj, rows(t)]
                s["f"][at] = f
            for i, name in enumerate(("lat", "vert", "stor")):
                first[name][0, k, rows(t)] = sums[i] * 0.25

    over(0, steps, MOST["look"], look)

    def faces(t):
        at = rows(t)
        for k in range(layers):
            lat = [s["lat"][pj, k, at] for pj in range(4)]
            inner_r = [0.5 * (lat[j] + lat[2 + j]) for j in range(2)]
            before_r = [0.5 * (s["lat"][2 + j, k, rows(t, -1)] + lat[j]) for j in range(2)]
            after_r = [0.5 * (lat[2 + j] + s["lat"][j, k, rows(t, 1)]) for j in range(2)]
            inner_c = [0.5 * (lat[2 * p] + lat[2 * p + 1]) for p in range(2)]
            before_c = [0.5 * (pltpu.roll(lat[2 * p + 1], 1, 1) + lat[2 * p]) for p in range(2)]
            after_c = [0.5 * (lat[2 * p + 1] + pltpu.roll(lat[2 * p], LANES - 1, 1)) for p in range(2)]
            for x in range(2):
                s["fri"][x, k, at] = inner_r[x]
                s["fro"][x, k, at] = before_r[x]
                s["fci"][x, k, at] = inner_c[x]
                s["fco"][x, k, at] = before_c[x]
                s["fcr"][x, k, at] = after_c[x]
            for p in range(2):
                for j in range(2):
                    pj = 2 * p + j
                    stor = s["stor"][pj, k, at]
                    diag = stor + inner_r[j] + (after_r[j] if p else before_r[j])
                    diag += inner_c[p] + (after_c[p] if j else before_c[p])
                    vert = s["vert"][pj, k, at]
                    if k > 0:
                        face = 0.5 * (vert + s["vert"][pj, k - 1, at])
                        s["fl"][pj, k, at] = face
                        diag += face
                    if k < layers - 1:
                        diag += 0.5 * (vert + s["vert"][pj, k + 1, at])
                    inside = stor > 0.0
                    s["invd"][pj, k, at] = jnp.where(inside, 1.0 / jnp.where(inside, diag, 1.0), 0.0)
                    s["stor"][pj, k, at] = diag

    over(0, steps, MOST["faces"], faces)
    for sweep in range(2):
        split_half(s, 0, 0, steps, layers)
        split_half(s, 1, 0, steps, layers)

    def remain(t):
        for k in range(layers):
            total = None
            for p in range(2):
                for j in range(2):
                    if (p + j + k) % 2 == 0:
                        pj = 2 * p + j
                        r = s["f"][pj, k, rows(t)] + split_sum(s, p, j, k, t, layers)
                        r -= s["stor"][pj, k, rows(t)] * s["u"][pj, k, rows(t)]
                        total = r if total is None else total + r
            first["f"][0, k, rows(t)] = total * 0.25

    over(0, steps, MOST["remain"], remain)

    for level in range(1, LOCAL):
        now = nats[level - 1]
        nat_setup(now, 0.25**level)
        count = (now["u"].shape[2] - 2 * PAD) // 8
        nat_down(now, ress[level - 1], count)
        if level < LOCAL - 1:
            below = nats[level]
            pairs = [(now[name], below[name]) for name in ("lat", "vert", "stor")]
            restrict_all(pairs + [(ress[level - 1], below["f"])])

    last, res = nats[-1], ress[-1]
    mine = 2 * half >> LOCAL
    off = halo >> (LOCAL - 1)
    group = 4 * mine
    per = LANES // group
    quantities = (res, last["lat"], last["vert"], last["stor"])
    parts = []
    for k in range(layers):
        for ref in quantities:
            part = ref[0, k, pl.ds(PAD + off, mine, stride=2), :]
            parts.append(part + ref[0, k, pl.ds(PAD + off + 1, mine, stride=2), :])
    source, target = iota((LANES, LANES), 0), iota((LANES, LANES), 1)
    hit = (source >= off) & ((source - off) // 2 == target) & (target < mine)
    packed = pick_dot(jnp.concatenate(parts, 0), jnp.where(hit, 0.25, 0.0))
    for pair in range(-(-layers // per)):
        total = jnp.zeros((mine, LANES), F32)
        for n in range(pair * per * 4, min(layers, (pair + 1) * per) * 4):
            part, base = packed[n * mine : (n + 1) * mine], (n - pair * per * 4) * mine
            total += pltpu.roll(part, base, 1) if base else part
        payload[pair * mine : (pair + 1) * mine] = total


def conjugate(s):
    tiles, layers, height, _ = s["u"].shape
    n = height - 2 * PAD
    row, lane = iota((n, LANES), 0), iota((n, LANES), 1)
    spots = [(i, k) for k in range(layers) for i in range(tiles)]
    body_rows = slice(PAD, PAD + n)

    def apply(v):
        out = []
        for k in range(layers):
            tiles_of = [v[k * tiles + i] for i in range(tiles)]
            left, right = sides_of(tiles_of, lane)
            for i in range(tiles):
                mid = tiles_of[i]
                wr = s["wr"][i, k, body_rows]
                wr_next = s["wr"][i, k, slice(PAD + 1, PAD + 1 + n)]
                total = wr * jnp.where(row == 0, 0.0, pltpu.roll(mid, 1, 0))
                total += wr_next * jnp.where(row == n - 1, 0.0, pltpu.roll(mid, n - 1, 0))
                total += s["wc"][i, k, body_rows] * left[i] + s["wcr"][i, k, body_rows] * right[i]
                if k > 0:
                    total += s["wl"][i, k, body_rows] * v[(k - 1) * tiles + i]
                if k < layers - 1:
                    total += s["wl"][i, k + 1, body_rows] * v[(k + 1) * tiles + i]
                out.append(s["diag"][i, k, body_rows] * mid - total)
        return out

    def inner(a, b):
        total = a[0] * b[0]
        for x, y in zip(a[1:], b[1:]):
            total += x * y
        total = jnp.sum(total, axis=0, keepdims=True)
        return jnp.sum(total, axis=1, keepdims=True)

    inv = [s["invd"][i, k, body_rows] for i, k in spots]
    inside = [x > 0.0 for x in inv]
    r = [jnp.where(inside[m], s["f"][i, k, body_rows], 0.0) for m, (i, k) in enumerate(spots)]
    z = [x * y for x, y in zip(r, inv)]
    count = len(spots)

    def step(_, carry):
        e, r, p, rz = carry[:count], carry[count : 2 * count], carry[2 * count : 3 * count], carry[-1]
        q = apply(p)
        alpha = rz / inner(p, q)
        e = [x + alpha * y for x, y in zip(e, p)]
        r = [jnp.where(m, x - alpha * y, 0.0) for m, x, y in zip(inside, r, q)]
        z = [x * s["invd"][i, k, body_rows] for x, (i, k) in zip(r, spots)]
        fresh = inner(r, z)
        beta = fresh / rz
        p = [x + beta * y for x, y in zip(z, p)]
        return (*e, *r, *p, fresh)

    start = (*[jnp.zeros_like(x) for x in r], *r, *z, inner(r, z))
    out = lax.fori_loop(0, COARSE_ITERS, step, start)
    for (i, k), value in zip(spots, out[:count]):
        s["u"][i, k, body_rows] = value


WHOLE = ("u", "f", "invd", "wr", "wc", "wcr", "wl", "lat", "vert", "stor", "diag")


def up_kernel(*refs, halo, half, spans):
    refs = list(refs)
    gathered = refs.pop(0)
    s = dict(zip(SPLIT_KEPT, refs[: len(SPLIT_KEPT)]))
    refs = refs[len(SPLIT_KEPT) :]
    nats = []
    for level in range(1, LOCAL):
        nats.append(dict(zip(NAT_KEPT, refs[: len(NAT_KEPT)])))
        refs = refs[len(NAT_KEPT) :]
    out = refs.pop(0)
    wholes = []
    for level in range(LOCAL, LEVELS + 1):
        wholes.append(dict(zip(WHOLE, refs[: len(WHOLE)])))
        refs = refs[len(WHOLE) :]
    ress = [refs.pop(0) for level in range(LOCAL, LEVELS)]
    fresh = [refs.pop(0) for level in range(LOCAL)]
    wider = refs.pop(0)
    nx, ny = spans
    layers = s["u"].shape[1]
    top = wholes[0]
    tiles, _, tall, _ = top["u"].shape
    mine = 2 * half >> LOCAL
    group = 4 * mine
    per = LANES // group
    lane = iota((mine, LANES), 1)

    for whole in wholes:
        count, _, height, _ = whole["u"].shape
        for name in ("u", "lat"):
            zeros = jnp.zeros((count, layers, PAD, LANES), F32)
            whole[name][:, :, :PAD] = zeros
            whole[name][:, :, height - PAD :] = zeros

    def gather(x, carry):
        at = pl.ds(pl.multiple_of(x * mine, 8) + PAD, mine)
        for k in range(layers):
            for n, name in enumerate(("f", "lat", "vert", "stor")):
                base = (k % per) * group + n * mine
                lines = slice((k // per) * mine, (k // per + 1) * mine)
                for i in range(tiles):
                    total = jnp.zeros((mine, LANES), F32)
                    for y in range(ny):
                        if y * mine // LANES == i:
                            to = y * mine % LANES
                            part = gathered[x * ny + y, lines]
                            if to != base:
                                part = pltpu.roll(part, (to - base) % LANES, 1)
                            total = jnp.where((lane >= to) & (lane < to + mine), part, total)
                    top[name][i, k, at] = total
        return carry

    lax.fori_loop(0, nx, gather, 0)

    for n, level in enumerate(range(LOCAL, LEVELS)):
        now, below = wholes[n], wholes[n + 1]
        nat_setup(now, 0.25**level)
        nat_down(now, ress[n], (now["u"].shape[2] - 2 * PAD) // 8)
        pairs = [(now[name], below[name]) for name in ("lat", "vert", "stor")]
        restrict_all(pairs + [(ress[n], below["f"])])
    nat_setup(wholes[-1], 0.25**LEVELS)
    conjugate(wholes[-1])
    for n in reversed(range(len(wholes) - 1)):
        now, below = wholes[n], wholes[n + 1]
        prolong_into(now, now["u"], lambda o, k: below["u"][o, k, PAD : below["u"].shape[2] - PAD], False)
        nat_up(now, 0, (now["u"].shape[2] - 2 * PAD) // 8)

    x, y = lax.axis_index("gx"), lax.axis_index("gy")
    reach = halo >> LOCAL
    need = (nats[-1]["u"].shape[2] - 2 * PAD) // 2
    height = top["u"].shape[2]
    for i in range(tiles):
        for k in range(layers):
            wider[i, k, :height] = top["u"][i, k]
            wider[i, k, height:] = jnp.zeros((PAD, LANES), F32)
    begin = PAD + x * mine - reach
    shift = y * mine - reach

    def window(o, k):
        parts = [wider[i, k, pl.ds(begin, need)] for i in range(tiles)]
        turn = lax.rem(4 * LANES - shift, LANES)
        lanes = iota((need, LANES), 1)
        first = lax.div(shift + LANES, LANES) - 1
        value = jnp.zeros((need, LANES), F32)
        for i in range(tiles):
            moved = pltpu.roll(parts[i], turn, 1)
            value = jnp.where((first == i) & (lanes < turn) | (first == i) & (turn == 0), moved, value)
            value = jnp.where((first == i - 1) & (lanes >= turn) & (turn != 0), moved, value)
        return value

    coarse = window
    for level in reversed(range(1, LOCAL)):
        now = dict(nats[level - 1])
        before = now["u"]
        now["u"] = fresh[level]
        height = before.shape[2]
        for i in range(before.shape[0]):
            for k in range(layers):
                now["u"][i, k, :PAD] = jnp.zeros((PAD, LANES), F32)
                now["u"][i, k, height - PAD :] = jnp.zeros((PAD, LANES), F32)
        prolong_into(now, before, coarse, level == LOCAL - 1)
        side = halo >> level
        own = 2 * half >> level
        margin = {0: 4, 1: 6, 2: 7}.get(level, 8)
        nat_up(now, (side - margin) // 8, min(-(-(side + own + margin) // 8), (height - 2 * PAD) // 8))
        coarse = functools.partial(lambda ref, o, k: ref[o, k, PAD : ref.shape[2] - PAD], now["u"])

    now = dict(s)
    now["u"] = fresh[0]
    hh = halo // 2
    lo, hi = (hh - 2) // 8, -(-(hh + half + 2) // 8)
    steps = (s["u"].shape[2] - 2 * PAD) // 8

    def add(t):
        for k in range(layers):
            value = fresh[1][0, k, rows(t)]
            for pj in range(4):
                now["u"][pj, k, rows(t)] = s["u"][pj, k, rows(t)] + value

    over(lo - 1, min(hi + 1, steps), MOST["add"], add)
    for sweep in range(2):
        split_half(now, 0, lo, hi, layers)
        split_half(now, 1, lo, hi, layers)
    source, target = iota((2 * LANES, 2 * half), 0), iota((2 * LANES, 2 * half), 1)
    pick = ((source % LANES == hh + target // 2) & (source // LANES == target % 2)).astype(F32)
    body_rows = slice(PAD + hh, PAD + hh + half)
    spots = [(k, p) for k in range(layers) for p in range(2)]
    both = [
        jnp.concatenate([now["u"][2 * p + j, k, body_rows] for k, p in spots], 0) for j in range(2)
    ]
    every = pick_dot(jnp.concatenate(both, 1), pick)
    for n, (k, p) in enumerate(spots):
        out[k, pl.ds(p, half, stride=2), :] = every[n * half : (n + 1) * half]


def swap(values, axis, first):
    count = lax.axis_size(axis)
    pairs = [(i, i + 1) for i in range(first, count - 1, 2)]
    return lax.ppermute(values, axis, pairs + [(b, a) for a, b in pairs])


def shape(*dims):
    return jax.ShapeDtypeStruct(dims, F32)


def on_device(u0, sub, cat, planar, vertical, ratio, watt):
    nx, ny = lax.axis_size("gx"), lax.axis_size("gy")
    layers, height, width = u0.shape
    halo = halo_cells()
    half, hh = height // 2, halo // 2
    planes = 2 * layers + 1
    assert height == width == LANES and 2 * halo <= LANES and halo + half <= LANES

    heat, a, b = pl.pallas_call(
        functools.partial(prep_kernel, halo=halo),
        out_shape=(shape(height, width), shape(planes, halo, height), shape(planes, halo, height)),
        in_specs=[SMEM, VMEM, VMEM, VMEM],
        out_specs=(VMEM,) * 3,
        compiler_params=limit(8),
        name="prep",
    )(watt, cat, u0, sub)
    a, b = swap(a, "gy", 0), swap(b, "gy", 1)

    lines = planes * 4 * hh
    sp, a, b = pl.pallas_call(
        functools.partial(split_kernel, halo=halo),
        out_shape=(shape(planes, 4, half, LANES), shape(lines, LANES), shape(lines, LANES)),
        in_specs=[VMEM] * 5,
        out_specs=(VMEM,) * 3,
        scratch_shapes=[pltpu.VMEM((2, 2, height, LANES), F32)],
        compiler_params=limit(20),
        name="split",
    )(u0, sub, heat, a, b)
    a, b = swap(a, "gx", 0), swap(b, "gx", 1)

    tall = up8(half + 2 * hh) + 2 * PAD
    four, two = (4, layers, tall, LANES), (2, layers, tall, LANES)
    split_shapes = [four if name in ("u", "f", "invd", "fl") else two for name in SPLIT_KEPT]
    nat_shapes = [
        (1, layers, up8((height + 2 * halo) >> level) + 2 * PAD, LANES) for level in range(1, LOCAL)
    ]
    mine = height >> LOCAL
    per = LANES // (4 * mine)
    pairs = -(-layers // per)
    kept = [shape(*d) for d in split_shapes]
    for d in nat_shapes:
        kept += [shape(*d)] * len(NAT_KEPT)
    scratch = [pltpu.VMEM(four, F32)] * 3 + [pltpu.VMEM((4, tall, LANES), F32)]
    for d in nat_shapes:
        scratch += [pltpu.VMEM(d, F32)] * len(NAT_OTHER)
    scratch += [pltpu.VMEM(d, F32) for d in nat_shapes]
    *saved, payload = pl.pallas_call(
        functools.partial(
            down_kernel, halo=halo, half=half, kinds=planar.shape[0]
        ),
        out_shape=(*kept, shape(pairs * mine, LANES)),
        in_specs=[SMEM] * 3 + [VMEM] * 3,
        out_specs=(VMEM,) * (len(kept) + 1),
        scratch_shapes=scratch,
        compiler_params=limit(36),
        name="down",
    )(planar, vertical, ratio, sp, a, b)

    sent = jnp.broadcast_to(payload[None], (nx * ny,) + payload.shape)
    gathered = lax.all_to_all(sent, ("gx", "gy"), 0, 0)

    scratch = []
    for level in range(LOCAL, LEVELS + 1):
        wide = -(-(ny * width >> level) // LANES)
        d = (wide, layers, up8(nx * height >> level) + 2 * PAD, LANES)
        scratch += [pltpu.VMEM(d, F32)] * len(WHOLE)
    for level in range(LOCAL, LEVELS):
        wide = -(-(ny * width >> level) // LANES)
        scratch.append(pltpu.VMEM((wide, layers, up8(nx * height >> level) + 2 * PAD, LANES), F32))
    scratch += [pltpu.VMEM(four, F32)] + [pltpu.VMEM(d, F32) for d in nat_shapes]
    wide, count, rows_of, _ = scratch[0].shape
    scratch.append(pltpu.VMEM((wide, count, rows_of + PAD, LANES), F32))
    return pl.pallas_call(
        functools.partial(up_kernel, halo=halo, half=half, spans=(nx, ny)),
        out_shape=shape(layers, height, width),
        in_specs=[VMEM] * (1 + len(kept)),
        out_specs=VMEM,
        scratch_shapes=scratch,
        compiler_params=limit(20, scratch),
        name="up",
    )(gathered, *saved)


def solution(mesh):
    placed = (P(None, "gx", "gy"), P(None, "gx", "gy"), P("gx", "gy"), P(), P(), P(), P())
    return jax.shard_map(
        on_device, mesh=mesh, in_specs=placed, out_specs=P(None, "gx", "gy"), check_vma=False
    )
```

```python
import functools
import math

import jax
import jax.numpy as jnp
from jax import lax
from jax.experimental import pallas as pl
from jax.experimental.pallas import tpu as pltpu
from jax.sharding import PartitionSpec as P

TILE = 16
LEVELS = 6
FIRST = 2
LOCAL = 4
COARSE_ITERS = 12
LANES = 128
PAD = 8
MOST = dict(split=3, nat=4, first=4, residual=4, setup=4, look=2, faces=2, remain=3, add=4)
HI = lax.Precision.HIGHEST
F32 = jnp.float32
VMEM = pl.BlockSpec(memory_space=pltpu.VMEM)
SMEM = pl.BlockSpec(memory_space=pltpu.SMEM)
HBM = pl.BlockSpec(memory_space=pltpu.HBM)


def limit(mib, scratch=()):
    held = sum(4 * math.prod(ref.shape) for ref in scratch)
    return pltpu.CompilerParams(vmem_limit_bytes=mib * 1024 * 1024 + held + held // 4)


def up8(n):
    return -(-n // 8) * 8


def halo_cells():
    need, above = [], 0
    for level in range(FIRST):
        need.append(above + 4)
        above = -(-need[-1] // 2)
    f = 0
    for level in reversed(range(FIRST)):
        inner = max(need[level], 2 * f + 1)
        f = inner + (4 if level == 0 else 3)
    unit = 2**FIRST
    return -(-f // unit) * unit


def iota(shape, axis):
    return lax.broadcasted_iota(jnp.int32, shape, axis)


def rows(t, off=0):
    first, count = t
    start = first * 8 if isinstance(first, int) else pl.multiple_of(first * 8, 8)
    return pl.ds(start + (PAD + off), 8 * count)


def over(lo, hi, most, body):
    steps = -(-(hi - lo) // most)
    size = -(-(hi - lo) // steps)
    if steps == 1:
        body((lo, size))
        return

    def step(i, carry):
        body((jnp.minimum(lo + i * size, hi - size), size))
        return carry

    lax.fori_loop(0, steps, step, 0)


def dot(a, b):
    return jnp.dot(a, b, precision=HI, preferred_element_type=F32)


def pick_dot(x, pick, pieces=3):
    pick = pick.astype(jnp.bfloat16)
    total = None
    for n in range(pieces):
        piece = x.astype(jnp.bfloat16)
        part = jnp.dot(piece, pick, preferred_element_type=F32)
        total = part if total is None else total + part
        if n < pieces - 1:
            x = x - piece.astype(F32)
    return total


def prep_kernel(watt_hbm, cat_hbm, u_hbm, sub_hbm, planes, a_ref, b_ref, watt, cat_ref, sub_ref, sems, *, halo):
    layers, height, width = u_hbm.shape
    copies = [
        pltpu.make_async_copy(source, target, sems.at[n])
        for n, (source, target) in enumerate(
            ((u_hbm, planes.at[pl.ds(0, layers)]), (sub_hbm, sub_ref), (cat_hbm, cat_ref), (watt_hbm, watt))
        )
    ]
    for copy in copies:
        copy.start()
    for copy in copies:
        copy.wait()
    cat = cat_ref[...]
    power = jnp.zeros(cat.shape, F32)
    for n in range(watt.shape[0]):
        power = power + jnp.where(cat == n, watt[n], 0.0)
    spread_r = (iota((height, cat.shape[0]), 0) // TILE == iota((height, cat.shape[0]), 1)).astype(F32)
    spread_c = (iota((cat.shape[1], width), 1) // TILE == iota((cat.shape[1], width), 0)).astype(F32)
    planes[2 * layers] = dot(dot(spread_r, power), spread_c)
    even = lax.axis_index("gy") % 2 == 0
    for q in range(2 * layers + 1):
        if layers <= q < 2 * layers:
            planes[q] = (sub_ref[q - layers] + 1).astype(F32)
        turned = planes[q].T
        low, high = turned[:halo], turned[width - halo :]
        a_ref[q] = jnp.where(even, high, low)
        b_ref[q] = jnp.where(even, low, high)


def split_kernel(own, ra, rb, out, a_ref, b_ref, scr, *, halo):
    count, height, width = own.shape
    layers = count // 2
    even_y, even_x = lax.axis_index("gy") % 2 == 0, lax.axis_index("gx") % 2 == 0
    half, hh = height // 2, halo // 2
    source, target = iota((width + LANES, 2 * LANES), 0), iota((width + LANES, 2 * LANES), 1)
    cell = 2 * (target % LANES) + target // LANES
    want = jnp.where(
        cell < halo, width + cell, jnp.where(cell < halo + width, cell - halo, cell)
    )
    pick = ((source == want) & (cell < 2 * halo + width)).astype(F32)
    planes = []
    for q in range(count):
        left = jnp.where(even_y, rb[q], ra[q])
        right = jnp.where(even_y, ra[q], rb[q])
        sides = jnp.concatenate([left, right, jnp.zeros((LANES - 2 * halo, height), F32)], 0).T
        planes.append(jnp.concatenate([own[q], sides], 1))
    first = pick_dot(jnp.concatenate(planes[:layers] + planes[2 * layers :], 0), pick)
    second = pick_dot(jnp.concatenate(planes[layers : 2 * layers], 0), pick, 1)
    for q in range(2 * layers + 1):
        if layers <= q < 2 * layers:
            both = second[(q - layers) * height : (q - layers + 1) * height]
        else:
            at = q if q < layers else layers
            both = first[at * height : (at + 1) * height]
        scr[q % 2, 0] = both[:, :LANES]
        scr[q % 2, 1] = both[:, LANES:]
        for p in range(2):
            for j in range(2):
                z = scr[q % 2, j, pl.ds(p, half, stride=2), :]
                out[q, 2 * p + j] = z
                at = (4 * q + 2 * p + j) * hh
                first_rows, last_rows = z[:hh], z[half - hh :]
                a_ref[at : at + hh] = jnp.where(even_x, last_rows, first_rows)
                b_ref[at : at + hh] = jnp.where(even_x, first_rows, last_rows)


def split_sum(s, p, j, k, t, layers):
    u = s["u"]
    at = rows(t)
    total = s["fri"][j, k, at] * u[2 * (1 - p) + j, k, at]
    if p == 0:
        total += s["fro"][j, k, at] * u[2 + j, k, rows(t, -1)]
    else:
        total += s["fro"][j, k, rows(t, 1)] * u[j, k, rows(t, 1)]
    total += s["fci"][p, k, at] * u[2 * p + 1 - j, k, at]
    if j == 0:
        total += s["fco"][p, k, at] * pltpu.roll(u[2 * p + 1, k, at], 1, 1)
    else:
        total += s["fcr"][p, k, at] * pltpu.roll(u[2 * p, k, at], LANES - 1, 1)
    pj = 2 * p + j
    if k > 0:
        total += s["fl"][pj, k, at] * u[pj, k - 1, at]
    if k < layers - 1:
        total += s["fl"][pj, k + 1, at] * u[pj, k + 1, at]
    return total


def split_half(s, colour, lo, hi, layers):
    def body(t):
        for k in range(layers):
            for p in range(2):
                for j in range(2):
                    if (p + j + k) % 2 == colour:
                        pj = 2 * p + j
                        total = s["f"][pj, k, rows(t)] + split_sum(s, p, j, k, t, layers)
                        s["u"][pj, k, rows(t)] = total * s["invd"][pj, k, rows(t)]

    over(lo, hi, MOST["split"], body)


def sides_of(tiles, edge):
    count = len(tiles)
    left = [pltpu.roll(x, 1, 1) for x in tiles]
    right = [pltpu.roll(x, LANES - 1, 1) for x in tiles]
    if count == 1 and not edge:
        return left, right
    lane = iota(tiles[0].shape, 1)
    return (
        [jnp.where(lane == 0, left[i - 1] if i else 0.0, left[i]) for i in range(count)],
        [
            jnp.where(lane == LANES - 1, right[i + 1] if i < count - 1 else 0.0, right[i])
            for i in range(count)
        ],
    )


def nat_setup(s, factor):
    tiles, layers, height, _ = s["lat"].shape
    c = 0.5 * factor

    def body(t):
        for k in range(layers):
            lat = [s["lat"][i, k, rows(t)] for i in range(tiles)]
            left, right = sides_of(lat, s["edge"])
            for i in range(tiles):
                stor = s["stor"][i, k, rows(t)]
                above = c * (lat[i] + s["lat"][i, k, rows(t, -1)])
                below = c * (lat[i] + s["lat"][i, k, rows(t, 1)])
                before, after = c * (lat[i] + left[i]), c * (lat[i] + right[i])
                diag = stor + above + below + before + after
                vert = s["vert"][i, k, rows(t)]
                if k > 0:
                    face = 0.5 * (vert + s["vert"][i, k - 1, rows(t)])
                    s["wl"][i, k, rows(t)] = face
                    diag += face
                if k < layers - 1:
                    diag += 0.5 * (vert + s["vert"][i, k + 1, rows(t)])
                inside = stor > 0.0
                s["wr"][i, k, rows(t)] = above
                s["wc"][i, k, rows(t)] = before
                s["wcr"][i, k, rows(t)] = after
                s["diag"][i, k, rows(t)] = diag
                s["invd"][i, k, rows(t)] = jnp.where(inside, 1.0 / jnp.where(inside, diag, 1.0), 0.0)

    s["wr"][:, :, height - PAD :] = jnp.zeros((tiles, layers, PAD, LANES), F32)
    over(0, (height - 2 * PAD) // 8, MOST["setup"], body)


def nat_sum(s, mid, sides, i, k, t, layers):
    u = s["u"]
    total = s["wr"][i, k, rows(t)] * u[i, k, rows(t, -1)]
    total += s["wr"][i, k, rows(t, 1)] * u[i, k, rows(t, 1)]
    total += s["wc"][i, k, rows(t)] * sides[k][0][i] + s["wcr"][i, k, rows(t)] * sides[k][1][i]
    if k > 0:
        total += s["wl"][i, k, rows(t)] * mid[k - 1][i]
    if k < layers - 1:
        total += s["wl"][i, k + 1, rows(t)] * mid[k + 1][i]
    return total


def nat_half(s, colour, lo, hi):
    tiles, layers = s["u"].shape[:2]

    def body(t):
        odd = (iota((8 * t[1], LANES), 0) + iota((8 * t[1], LANES), 1)) % 2
        mid = [[s["u"][i, k, rows(t)] for i in range(tiles)] for k in range(layers)]
        sides = [sides_of(m, s["edge"]) for m in mid]
        for k in range(layers):
            chosen = odd == (colour + k) % 2
            for i in range(tiles):
                total = s["f"][i, k, rows(t)] + nat_sum(s, mid, sides, i, k, t, layers)
                s["u"][i, k, rows(t)] = jnp.where(chosen, total * s["invd"][i, k, rows(t)], mid[k][i])

    over(lo, hi, MOST["nat"], body)


def nat_first(s, lo, hi):
    tiles, layers, height, _ = s["u"].shape
    zeros = jnp.zeros((tiles, layers, PAD, LANES), F32)
    s["u"][:, :, :PAD] = zeros
    s["u"][:, :, height - PAD :] = zeros

    def body(t):
        odd = (iota((8 * t[1], LANES), 0) + iota((8 * t[1], LANES), 1)) % 2
        for k in range(layers):
            for i in range(tiles):
                value = s["f"][i, k, rows(t)] * s["invd"][i, k, rows(t)]
                s["u"][i, k, rows(t)] = jnp.where(odd == k % 2, value, 0.0)

    over(lo, hi, MOST["first"], body)


def nat_residual(s, res, lo, hi):
    tiles, layers = s["u"].shape[:2]

    def body(t):
        mid = [[s["u"][i, k, rows(t)] for i in range(tiles)] for k in range(layers)]
        sides = [sides_of(m, s["edge"]) for m in mid]
        for k in range(layers):
            for i in range(tiles):
                total = s["f"][i, k, rows(t)] + nat_sum(s, mid, sides, i, k, t, layers)
                res[i, k, rows(t)] = total - s["diag"][i, k, rows(t)] * mid[k][i]

    over(lo, hi, MOST["residual"], body)


def nat_down(s, res, steps):
    nat_first(s, 0, steps)
    for colour in (1, 0, 1):
        nat_half(s, colour, 0, steps)
    nat_residual(s, res, 0, steps)


def restrict_all(pairs):
    tiles, layers = pairs[0][0].shape[:2]
    count, height = pairs[0][1].shape[0], pairs[0][1].shape[2] - 2 * PAD
    zeros = jnp.zeros((count, layers, PAD, LANES), F32)
    parts = [[] for i in range(tiles)]
    for source, target in pairs:
        target[:, :, :PAD] = zeros
        target[:, :, PAD + height :] = zeros
        for k in range(layers):
            for i in range(tiles):
                part = source[i, k, pl.ds(PAD, height, stride=2), :]
                parts[i].append(part + source[i, k, pl.ds(PAD + 1, height, stride=2), :])
    parts = [jnp.concatenate(p, 0) for p in parts]
    cell = iota((LANES, LANES), 0) // 2
    for o in range(count):
        total = None
        for i in range(tiles):
            shift = LANES // 2 * i - LANES * o
            if -LANES < shift < LANES:
                pick = jnp.where(cell + shift == iota((LANES, LANES), 1), 0.25, 0.0)
                part = pick_dot(parts[i], pick)
                total = part if total is None else total + part
        for n, (_, target) in enumerate(pairs):
            for k in range(layers):
                at = (n * layers + k) * height
                target[o, k, PAD : PAD + height] = total[at : at + height]


def prolong_into(s, u_in, coarse, mask):
    tiles, layers, height, _ = s["u"].shape
    n = (height - 2 * PAD) // 2
    tall = up8(n)
    cell = iota((LANES, LANES), 1) // 2
    for i in range(tiles):
        o = i // 2
        shift = LANES // 2 * (i % 2)
        pick = (cell + shift == iota((LANES, LANES), 0)).astype(F32)
        every = pick_dot(jnp.concatenate([coarse(o, k)[:tall] for k in range(layers)], 0), pick)
        for k in range(layers):
            wide = every[k * tall : k * tall + n]
            for p in range(2):
                at = pl.ds(PAD + p, n, stride=2)
                add = wide
                if mask:
                    add = jnp.where(s["invd"][i, k, at, :] > 0.0, wide, 0.0)
                s["u"][i, k, at, :] = u_in[i, k, at, :] + add


def nat_up(s, lo, hi):
    for sweep in range(2):
        nat_half(s, 0, lo, hi)
        nat_half(s, 1, lo, hi)


SPLIT_KEPT = ("u", "f", "invd", "fri", "fro", "fci", "fco", "fcr", "fl")
NAT_KEPT = ("u", "f", "invd", "wr", "wc", "wcr", "wl")
NAT_OTHER = ("lat", "vert", "stor", "diag")


def pack_own(payload, last, res, mine, off):
    layers = res.shape[1]
    group = 4 * mine
    per = LANES // group
    quantities = (res, last["lat"], last["vert"], last["stor"])
    parts = []
    for k in range(layers):
        for ref in quantities:
            part = ref[0, k, pl.ds(PAD + off, mine, stride=2), :]
            parts.append(part + ref[0, k, pl.ds(PAD + off + 1, mine, stride=2), :])
    source, target = iota((LANES, LANES), 0), iota((LANES, LANES), 1)
    hit = (source >= off) & ((source - off) // 2 == target) & (target < mine)
    packed = pick_dot(jnp.concatenate(parts, 0), jnp.where(hit, 0.25, 0.0))
    for pair in range(-(-layers // per)):
        total = jnp.zeros((mine, LANES), F32)
        for n in range(pair * per * 4, min(layers, (pair + 1) * per) * 4):
            part, base = packed[n * mine : (n + 1) * mine], (n - pair * per * 4) * mine
            total += pltpu.roll(part, base, 1) if base else part
        payload[pair * mine : (pair + 1) * mine] = total


def down_kernel(*refs, halo, half, kinds):
    tables, (sp, ra, rb) = refs[:3], refs[3:6]
    refs = list(refs[6:])
    s = dict(zip(SPLIT_KEPT, refs[: len(SPLIT_KEPT)]))
    refs = refs[len(SPLIT_KEPT) :]
    nats = []
    for level in range(1, FIRST):
        nats.append(dict(zip(NAT_KEPT, refs[: len(NAT_KEPT)]), edge=False))
        refs = refs[len(NAT_KEPT) :]
    payload = refs.pop(0)
    for name in ("lat", "vert", "stor", "diag"):
        s[name] = refs.pop(0)
    heat = refs.pop(0)
    for level in range(1, FIRST):
        for name in NAT_OTHER:
            nats[level - 1][name] = refs.pop(0)
    ress = [refs.pop(0) for level in range(1, FIRST)]
    layers = s["u"].shape[1]
    height = s["u"].shape[2]
    hh = halo // 2
    steps = (height - 2 * PAD) // 8
    even = lax.axis_index("gx") % 2 == 0
    zeros = jnp.zeros((PAD, LANES), F32)

    def place(ref, index, q, pj):
        at = (4 * q + pj) * hh
        first, second = ra[at : at + hh], rb[at : at + hh]
        ref[index + (slice(PAD, PAD + hh),)] = jnp.where(even, second, first)
        ref[index + (slice(PAD + hh, PAD + hh + half),)] = sp[q, pj]
        ref[index + (slice(PAD + hh + half, PAD + 2 * hh + half),)] = jnp.where(even, first, second)

    for pj in range(4):
        for k in range(layers):
            for name in ("u", "lat"):
                s[name][pj, k, :PAD] = zeros
                s[name][pj, k, height - PAD :] = zeros
            place(s["u"], (pj, k), k, pj)
            place(s["diag"], (pj, k), layers + k, pj)
        place(heat, (pj,), 2 * layers, pj)
    for j in range(2):
        for k in range(layers):
            s["fro"][j, k, height - PAD :] = zeros

    first = nats[0]
    clear = [first[name] for name in ("lat", "vert", "stor", "f")] + ress
    for ref in clear:
        for k in range(layers):
            ref[0, k, :PAD] = zeros
            ref[0, k, ref.shape[2] - PAD :] = zeros

    def look(t):
        for k in range(layers):
            sums = [None, None, None]
            for pj in range(4):
                at = (pj, k, rows(t))
                label = s["diag"][at]
                value = [jnp.zeros_like(label)] * 3
                for n in range(kinds):
                    hit = label == float(n + 1)
                    value = [jnp.where(hit, tables[i][n], value[i]) for i in range(3)]
                for i, name in enumerate(("lat", "vert", "stor")):
                    s[name][at] = value[i]
                    sums[i] = value[i] if sums[i] is None else sums[i] + value[i]
                f = value[2] * s["u"][at]
                if k == 0:
                    f = f + heat[pj, rows(t)]
                s["f"][at] = f
            for i, name in enumerate(("lat", "vert", "stor")):
                first[name][0, k, rows(t)] = sums[i] * 0.25

    over(0, steps, MOST["look"], look)

    def faces(t):
        at = rows(t)
        for k in range(layers):
            lat = [s["lat"][pj, k, at] for pj in range(4)]
            inner_r = [0.5 * (lat[j] + lat[2 + j]) for j in range(2)]
            before_r = [0.5 * (s["lat"][2 + j, k, rows(t, -1)] + lat[j]) for j in range(2)]
            after_r = [0.5 * (lat[2 + j] + s["lat"][j, k, rows(t, 1)]) for j in range(2)]
            inner_c = [0.5 * (lat[2 * p] + lat[2 * p + 1]) for p in range(2)]
            before_c = [0.5 * (pltpu.roll(lat[2 * p + 1], 1, 1) + lat[2 * p]) for p in range(2)]
            after_c = [0.5 * (lat[2 * p + 1] + pltpu.roll(lat[2 * p], LANES - 1, 1)) for p in range(2)]
            for x in range(2):
                s["fri"][x, k, at] = inner_r[x]
                s["fro"][x, k, at] = before_r[x]
                s["fci"][x, k, at] = inner_c[x]
                s["fco"][x, k, at] = before_c[x]
                s["fcr"][x, k, at] = after_c[x]
            for p in range(2):
                for j in range(2):
                    pj = 2 * p + j
                    stor = s["stor"][pj, k, at]
                    diag = stor + inner_r[j] + (after_r[j] if p else before_r[j])
                    diag += inner_c[p] + (after_c[p] if j else before_c[p])
                    vert = s["vert"][pj, k, at]
                    if k > 0:
                        face = 0.5 * (vert + s["vert"][pj, k - 1, at])
                        s["fl"][pj, k, at] = face
                        diag += face
                    if k < layers - 1:
                        diag += 0.5 * (vert + s["vert"][pj, k + 1, at])
                    inside = stor > 0.0
                    s["invd"][pj, k, at] = jnp.where(inside, 1.0 / jnp.where(inside, diag, 1.0), 0.0)
                    s["diag"][pj, k, at] = diag

    over(0, steps, MOST["faces"], faces)
    for sweep in range(2):
        split_half(s, 0, 0, steps, layers)
        split_half(s, 1, 0, steps, layers)

    def remain(t):
        for k in range(layers):
            total = None
            for p in range(2):
                for j in range(2):
                    if (p + j + k) % 2 == 0:
                        pj = 2 * p + j
                        r = s["f"][pj, k, rows(t)] + split_sum(s, p, j, k, t, layers)
                        r -= s["diag"][pj, k, rows(t)] * s["u"][pj, k, rows(t)]
                        total = r if total is None else total + r
            first["f"][0, k, rows(t)] = total * 0.25

    over(0, steps, MOST["remain"], remain)

    for level in range(1, FIRST):
        now = nats[level - 1]
        nat_setup(now, 0.25**level)
        count = (now["u"].shape[2] - 2 * PAD) // 8
        nat_down(now, ress[level - 1], count)
        if level < FIRST - 1:
            below = nats[level]
            pairs = [(now[name], below[name]) for name in ("lat", "vert", "stor")]
            restrict_all(pairs + [(ress[level - 1], below["f"])])

    pack_own(payload, nats[-1], ress[-1], 2 * half >> FIRST, halo >> (FIRST - 1))


def mid_kernel(own, ra, rb, ta, tb, *refs):
    refs = list(refs)
    count = LOCAL - FIRST
    nats = []
    for n in range(count):
        nats.append(dict(zip(NAT_KEPT, refs[: len(NAT_KEPT)]), edge=False))
        refs = refs[len(NAT_KEPT) :]
    payload = refs.pop(0)
    for n in range(count):
        for name in NAT_OTHER:
            nats[n][name] = refs.pop(0)
    ress = refs
    layers = nats[0]["u"].shape[1]
    mine = own.shape[0] // layers
    even_y, even_x = lax.axis_index("gy") % 2 == 0, lax.axis_index("gx") % 2 == 0
    zeros = jnp.zeros((PAD, LANES), F32)
    for now, res in zip(nats, ress):
        for ref in [now[name] for name in ("lat", "vert", "stor", "f")] + [res]:
            for k in range(layers):
                ref[0, k, :PAD] = zeros
                ref[0, k, ref.shape[2] - PAD :] = zeros
    group = iota((mine, LANES), 1) // mine
    for v in range(3):
        for k in range(layers):
            lines = slice(k * mine, (k + 1) * mine)
            if v == 1:
                middle, a, b = own[lines], ra[lines], rb[lines]
            else:
                first, second = (tb, ta) if v == 0 else (ta, tb)
                middle, a, b = [jnp.where(even_x, first[n, lines], second[n, lines]) for n in range(3)]
            left, right = jnp.where(even_y, b, a), jnp.where(even_y, a, b)
            middle, right = pltpu.roll(middle, mine, 1), pltpu.roll(right, 2 * mine, 1)
            for n, name in enumerate(("f", "lat", "vert", "stor")):
                value = jnp.where(group == (n + 1) % 4, middle, right)
                value = jnp.where(group == n, left, value)
                value = jnp.where(group == (n + 3) % 4, 0.0, value)
                if n:
                    value = pltpu.roll(value, LANES - n * mine, 1)
                nats[0][name][0, k, PAD + v * mine : PAD + (v + 1) * mine] = value
    for n, level in enumerate(range(FIRST, LOCAL)):
        now = nats[n]
        nat_setup(now, 0.25**level)
        nat_down(now, ress[n], (now["u"].shape[2] - 2 * PAD) // 8)
        if n < count - 1:
            pairs = [(now[name], nats[n + 1][name]) for name in ("lat", "vert", "stor")]
            restrict_all(pairs + [(ress[n], nats[n + 1]["f"])])
    pack_own(payload, nats[-1], ress[-1], mine >> count, mine >> (count - 1))


def conjugate(s):
    tiles, layers, height, _ = s["u"].shape
    n = height - 2 * PAD
    row = iota((n, LANES), 0)
    spots = [(i, k) for k in range(layers) for i in range(tiles)]
    body_rows = slice(PAD, PAD + n)

    def apply(v):
        out = []
        for k in range(layers):
            tiles_of = [v[k * tiles + i] for i in range(tiles)]
            left, right = sides_of(tiles_of, s["edge"])
            for i in range(tiles):
                mid = tiles_of[i]
                wr = s["wr"][i, k, body_rows]
                wr_next = s["wr"][i, k, slice(PAD + 1, PAD + 1 + n)]
                total = wr * jnp.where(row == 0, 0.0, pltpu.roll(mid, 1, 0))
                total += wr_next * jnp.where(row == n - 1, 0.0, pltpu.roll(mid, n - 1, 0))
                total += s["wc"][i, k, body_rows] * left[i] + s["wcr"][i, k, body_rows] * right[i]
                if k > 0:
                    total += s["wl"][i, k, body_rows] * v[(k - 1) * tiles + i]
                if k < layers - 1:
                    total += s["wl"][i, k + 1, body_rows] * v[(k + 1) * tiles + i]
                out.append(s["diag"][i, k, body_rows] * mid - total)
        return out

    def inner(a, b):
        total = a[0] * b[0]
        for x, y in zip(a[1:], b[1:]):
            total += x * y
        total = jnp.sum(total, axis=0, keepdims=True)
        return jnp.sum(total, axis=1, keepdims=True)

    inv = [s["invd"][i, k, body_rows] for i, k in spots]
    inside = [x > 0.0 for x in inv]
    r = [jnp.where(inside[m], s["f"][i, k, body_rows], 0.0) for m, (i, k) in enumerate(spots)]
    z = [x * y for x, y in zip(r, inv)]
    count = len(spots)

    def step(_, carry):
        e, r, p, rz = carry[:count], carry[count : 2 * count], carry[2 * count : 3 * count], carry[-1]
        q = apply(p)
        alpha = rz / inner(p, q)
        e = [x + alpha * y for x, y in zip(e, p)]
        r = [jnp.where(m, x - alpha * y, 0.0) for m, x, y in zip(inside, r, q)]
        z = [x * s["invd"][i, k, body_rows] for x, (i, k) in zip(r, spots)]
        fresh = inner(r, z)
        beta = fresh / rz
        p = [x + beta * y for x, y in zip(z, p)]
        return (*e, *r, *p, fresh)

    start = (*[jnp.zeros_like(x) for x in r], *r, *z, inner(r, z))
    out = lax.fori_loop(0, COARSE_ITERS, step, start)
    for (i, k), value in zip(spots, out[:count]):
        s["u"][i, k, body_rows] = value


WHOLE = ("u", "f", "invd", "wr", "wc", "wcr", "wl", "lat", "vert", "stor", "diag")


def up_kernel(*refs, halo, half, spans):
    refs = list(refs)
    gathered = refs.pop(0)
    s = dict(zip(SPLIT_KEPT, refs[: len(SPLIT_KEPT)]))
    refs = refs[len(SPLIT_KEPT) :]
    nats = []
    for level in range(1, LOCAL):
        nats.append(dict(zip(NAT_KEPT, refs[: len(NAT_KEPT)]), edge=False))
        refs = refs[len(NAT_KEPT) :]
    out = refs.pop(0)
    wholes = []
    for level in range(LOCAL, LEVELS + 1):
        edge = (spans[1] * 2 * half >> level) % LANES == 0
        wholes.append(dict(zip(WHOLE, refs[: len(WHOLE)]), edge=edge))
        refs = refs[len(WHOLE) :]
    ress = [refs.pop(0) for level in range(LOCAL, LEVELS)]
    fresh = [refs.pop(0) for level in range(LOCAL)]
    wider = refs.pop(0)
    nx, ny = spans
    layers = s["u"].shape[1]
    top = wholes[0]
    tiles, _, tall, _ = top["u"].shape
    mine = 2 * half >> LOCAL
    group = 4 * mine
    per = LANES // group
    lane = iota((mine, LANES), 1)

    for whole in wholes:
        count, _, height, _ = whole["u"].shape
        for name in ("u", "lat"):
            zeros = jnp.zeros((count, layers, PAD, LANES), F32)
            whole[name][:, :, :PAD] = zeros
            whole[name][:, :, height - PAD :] = zeros

    def gather(x, carry):
        at = pl.ds(pl.multiple_of(x * mine, 8) + PAD, mine)
        for i in range(tiles):
            here = [y for y in range(ny) if y * mine // LANES == i]
            for wide in range(-(-layers // per)):
                lines = slice(wide * mine, (wide + 1) * mine)
                parts = []
                for y in here:
                    part = gathered[x * ny + y, lines]
                    to = y * mine % LANES
                    parts.append(pltpu.roll(part, to, 1) if to else part)
                for k in range(wide * per, min(layers, (wide + 1) * per)):
                    for n, name in enumerate(("f", "lat", "vert", "stor")):
                        base = (k % per) * group + n * mine
                        total = jnp.zeros((mine, LANES), F32)
                        for y, part in zip(here, parts):
                            spot = (base + y * mine) % LANES
                            total = jnp.where((lane >= spot) & (lane < spot + mine), part, total)
                        top[name][i, k, at] = pltpu.roll(total, LANES - base, 1) if base else total
        return carry

    lax.fori_loop(0, nx, gather, 0)

    for n, level in enumerate(range(LOCAL, LEVELS)):
        now, below = wholes[n], wholes[n + 1]
        nat_setup(now, 0.25**level)
        nat_down(now, ress[n], (now["u"].shape[2] - 2 * PAD) // 8)
        pairs = [(now[name], below[name]) for name in ("lat", "vert", "stor")]
        restrict_all(pairs + [(ress[n], below["f"])])
    nat_setup(wholes[-1], 0.25**LEVELS)
    conjugate(wholes[-1])
    for n in reversed(range(len(wholes) - 1)):
        now, below = wholes[n], wholes[n + 1]
        prolong_into(now, now["u"], lambda o, k: below["u"][o, k, PAD : below["u"].shape[2] - PAD], False)
        nat_up(now, 0, (now["u"].shape[2] - 2 * PAD) // 8)

    x, y = lax.axis_index("gx"), lax.axis_index("gy")
    reach = (2 * half >> FIRST) >> (LOCAL - FIRST)
    need = (nats[-1]["u"].shape[2] - 2 * PAD) // 2
    height = top["u"].shape[2]
    for i in range(tiles):
        for k in range(layers):
            wider[i, k, :height] = top["u"][i, k]
            wider[i, k, height:] = jnp.zeros((PAD, LANES), F32)
    begin = PAD + x * mine - reach
    shift = y * mine - reach

    def window(o, k):
        parts = [wider[i, k, pl.ds(begin, need)] for i in range(tiles)]
        turn = lax.rem(4 * LANES - shift, LANES)
        lanes = iota((need, LANES), 1)
        first = lax.div(shift + LANES, LANES) - 1
        value = jnp.zeros((need, LANES), F32)
        for i in range(tiles):
            moved = pltpu.roll(parts[i], turn, 1)
            value = jnp.where((first == i) & (lanes < turn) | (first == i) & (turn == 0), moved, value)
            value = jnp.where((first == i - 1) & (lanes >= turn) & (turn != 0), moved, value)
        return value

    coarse = window
    margins, above = [], 0
    for level in range(LOCAL):
        margins.append(above + 4)
        above = -(-margins[-1] // 2)
    for level in reversed(range(1, LOCAL)):
        now = dict(nats[level - 1])
        before = now["u"]
        now["u"] = fresh[level]
        height = before.shape[2]
        for i in range(before.shape[0]):
            for k in range(layers):
                now["u"][i, k, :PAD] = jnp.zeros((PAD, LANES), F32)
                now["u"][i, k, height - PAD :] = jnp.zeros((PAD, LANES), F32)
        prolong_into(now, before, coarse, level == LOCAL - 1)
        own = 2 * half >> level
        side = halo >> level if level < FIRST else (2 * half >> FIRST) >> (level - FIRST)
        reach = margins[level]
        nat_up(now, (side - reach) // 8, min(-(-(side + own + reach) // 8), (height - 2 * PAD) // 8))
        coarse = functools.partial(lambda ref, o, k: ref[o, k, PAD : ref.shape[2] - PAD], now["u"])
        if level == FIRST:
            skip = side - (halo >> FIRST)
            coarse = functools.partial(
                lambda ref, o, k: pltpu.roll(
                    ref[o, k, PAD + skip : ref.shape[2] - PAD], LANES - skip, 1
                ),
                now["u"],
            )

    now = dict(s)
    now["u"] = fresh[0]
    hh = halo // 2
    lo, hi = (hh - 2) // 8, -(-(hh + half + 2) // 8)
    steps = (s["u"].shape[2] - 2 * PAD) // 8

    def add(t):
        for k in range(layers):
            value = fresh[1][0, k, rows(t)]
            for pj in range(4):
                now["u"][pj, k, rows(t)] = s["u"][pj, k, rows(t)] + value

    over(lo - 1, min(hi + 1, steps), MOST["add"], add)
    for sweep in range(2):
        split_half(now, 0, lo, hi, layers)
        split_half(now, 1, lo, hi, layers)
    source, target = iota((2 * LANES, 2 * half), 0), iota((2 * LANES, 2 * half), 1)
    pick = ((source % LANES == hh + target // 2) & (source // LANES == target % 2)).astype(F32)
    body_rows = slice(PAD + hh, PAD + hh + half)
    spots = [(k, p) for k in range(layers) for p in range(2)]
    both = [
        jnp.concatenate([now["u"][2 * p + j, k, body_rows] for k, p in spots], 0) for j in range(2)
    ]
    every = pick_dot(jnp.concatenate(both, 1), pick)
    for n, (k, p) in enumerate(spots):
        out[k, pl.ds(p, half, stride=2), :] = every[n * half : (n + 1) * half]


def swap(values, axis, first):
    count = lax.axis_size(axis)
    pairs = [(i, i + 1) for i in range(first, count - 1, 2)]
    return lax.ppermute(values, axis, pairs + [(b, a) for a, b in pairs])


def shape(*dims):
    return jax.ShapeDtypeStruct(dims, F32)


def packed_shape(layers, mine):
    per = LANES // (4 * mine)
    return shape(-(-layers // per) * mine, LANES)


def whole_shape(level, layers, height, width):
    return -(-(width >> level) // LANES), layers, up8(height >> level) + 2 * PAD, LANES


def other_scratch(shapes):
    out = []
    for d in shapes:
        out += [pltpu.VMEM(d, F32)] * len(NAT_OTHER)
    return out + [pltpu.VMEM(d, F32) for d in shapes]


def on_device(u0, sub, cat, planar, vertical, ratio, watt):
    nx, ny = lax.axis_size("gx"), lax.axis_size("gy")
    layers, height, width = u0.shape
    halo = halo_cells()
    half, hh = height // 2, halo // 2
    planes = 2 * layers + 1
    assert height == width == LANES and 2 * halo <= LANES and halo + half <= LANES

    own, a, b = pl.pallas_call(
        functools.partial(prep_kernel, halo=halo),
        out_shape=(shape(planes, height, width), shape(planes, halo, height), shape(planes, halo, height)),
        in_specs=[HBM] * 4,
        out_specs=(VMEM,) * 3,
        scratch_shapes=[
            pltpu.SMEM(watt.shape, F32),
            pltpu.VMEM(cat.shape, jnp.int32),
            pltpu.VMEM(sub.shape, jnp.int32),
            pltpu.SemaphoreType.DMA((4,)),
        ],
        compiler_params=limit(8),
        name="prep",
    )(watt, cat, u0, sub)
    a, b = swap(a, "gy", 0), swap(b, "gy", 1)

    lines = planes * 4 * hh
    sp, a, b = pl.pallas_call(
        functools.partial(split_kernel, halo=halo),
        out_shape=(shape(planes, 4, half, LANES), shape(lines, LANES), shape(lines, LANES)),
        in_specs=[VMEM] * 3,
        out_specs=(VMEM,) * 3,
        scratch_shapes=[pltpu.VMEM((2, 2, height, LANES), F32)],
        compiler_params=limit(20),
        name="split",
    )(own, a, b)
    a, b = swap(a, "gx", 0), swap(b, "gx", 1)

    tall = up8(half + 2 * hh) + 2 * PAD
    four, two = (4, layers, tall, LANES), (2, layers, tall, LANES)
    kept = [shape(*(four if name in ("u", "f", "invd", "fl") else two)) for name in SPLIT_KEPT]
    nat_shapes = [
        (1, layers, up8((height + 2 * halo) >> level) + 2 * PAD, LANES) for level in range(1, FIRST)
    ]
    for d in nat_shapes:
        kept += [shape(*d)] * len(NAT_KEPT)
    scratch = [pltpu.VMEM(four, F32)] * 4 + [pltpu.VMEM((4, tall, LANES), F32)]
    scratch += other_scratch(nat_shapes)
    *saved, block = pl.pallas_call(
        functools.partial(down_kernel, halo=halo, half=half, kinds=planar.shape[0]),
        out_shape=(*kept, packed_shape(layers, height >> FIRST)),
        in_specs=[SMEM] * 3 + [VMEM] * 3,
        out_specs=(VMEM,) * (len(kept) + 1),
        scratch_shapes=scratch,
        compiler_params=limit(30),
        name="down",
    )(planar, vertical, ratio, sp, a, b)

    a, b = swap(block, "gy", 0), swap(block, "gy", 1)
    column = jnp.stack([block, a, b])
    above, below = swap(column, "gx", 0), swap(column, "gx", 1)
    mine = height >> FIRST
    assert 4 * mine <= LANES
    block_shapes = [
        (1, layers, up8(3 * mine >> n) + 2 * PAD, LANES) for n in range(LOCAL - FIRST)
    ]
    kept = []
    for d in block_shapes:
        kept += [shape(*d)] * len(NAT_KEPT)
    *more, payload = pl.pallas_call(
        mid_kernel,
        out_shape=(*kept, packed_shape(layers, height >> LOCAL)),
        in_specs=[VMEM] * 5,
        out_specs=(VMEM,) * (len(kept) + 1),
        scratch_shapes=other_scratch(block_shapes),
        compiler_params=limit(20),
        name="mid",
    )(block, a, b, above, below)
    saved += more
    nat_shapes += block_shapes

    sent = jnp.broadcast_to(payload[None], (nx * ny,) + payload.shape)
    gathered = lax.all_to_all(sent, ("gx", "gy"), 0, 0)

    scratch = []
    for level in range(LOCAL, LEVELS + 1):
        scratch += [pltpu.VMEM(whole_shape(level, layers, nx * height, ny * width), F32)] * len(WHOLE)
    for level in range(LOCAL, LEVELS):
        scratch.append(pltpu.VMEM(whole_shape(level, layers, nx * height, ny * width), F32))
    scratch += [pltpu.VMEM(four, F32)] + [pltpu.VMEM(d, F32) for d in nat_shapes]
    wide, count, rows_of, _ = scratch[0].shape
    scratch.append(pltpu.VMEM((wide, count, rows_of + PAD, LANES), F32))
    return pl.pallas_call(
        functools.partial(up_kernel, halo=halo, half=half, spans=(nx, ny)),
        out_shape=shape(layers, height, width),
        in_specs=[VMEM] * (1 + len(saved)),
        out_specs=VMEM,
        scratch_shapes=scratch,
        compiler_params=limit(16, scratch),
        name="up",
    )(gathered, *saved)


def solution(mesh):
    placed = (P(None, "gx", "gy"), P(None, "gx", "gy"), P("gx", "gy"), P(), P(), P(), P())
    return jax.shard_map(
        on_device, mesh=mesh, in_specs=placed, out_specs=P(None, "gx", "gy"), check_vma=False
    )
```

```python
import functools
import math

import jax
import jax.numpy as jnp
from jax import lax
from jax.experimental import pallas as pl
from jax.experimental.pallas import tpu as pltpu
from jax.sharding import PartitionSpec as P

TILE = 16
LEVELS = 6
FIRST = 2
LOCAL = 4
COARSE_ITERS = 12
LANES = 128
PAD = 8
MOST = dict(split=6, nat=12, first=12, residual=12, setup=6, look=1, faces=4, remain=6, add=4)
HI = lax.Precision.HIGHEST
F32 = jnp.float32
VMEM = pl.BlockSpec(memory_space=pltpu.VMEM)
SMEM = pl.BlockSpec(memory_space=pltpu.SMEM)
HBM = pl.BlockSpec(memory_space=pltpu.HBM)


def limit(mib, scratch=()):
    held = sum(4 * math.prod(ref.shape) for ref in scratch)
    return pltpu.CompilerParams(vmem_limit_bytes=mib * 1024 * 1024 + held + held // 4)


def up8(n):
    return -(-n // 8) * 8


def halo_cells():
    need, above = [], 0
    for level in range(FIRST):
        need.append(above + 4)
        above = -(-need[-1] // 2)
    f = 0
    for level in reversed(range(FIRST)):
        inner = max(need[level], 2 * f + 1)
        f = inner + (4 if level == 0 else 3)
    unit = 2**FIRST
    return -(-f // unit) * unit


def iota(shape, axis):
    return lax.broadcasted_iota(jnp.int32, shape, axis)


def rows(t, off=0):
    first, count = t
    start = first * 8 if isinstance(first, int) else pl.multiple_of(first * 8, 8)
    return pl.ds(start + (PAD + off), 8 * count)


def over(lo, hi, most, body):
    steps = -(-(hi - lo) // most)
    size = -(-(hi - lo) // steps)
    if steps == 1:
        body((lo, size))
        return

    def step(i, carry):
        body((jnp.minimum(lo + i * size, hi - size), size))
        return carry

    lax.fori_loop(0, steps, step, 0)


def dot(a, b):
    return jnp.dot(a, b, precision=HI, preferred_element_type=F32)


def pick_dot(x, pick, pieces=3):
    pick = pick.astype(jnp.bfloat16)
    total = None
    for n in range(pieces):
        piece = x.astype(jnp.bfloat16)
        part = jnp.dot(piece, pick, preferred_element_type=F32)
        total = part if total is None else total + part
        if n < pieces - 1:
            x = x - piece.astype(F32)
    return total


def prep_kernel(watt_hbm, cat_hbm, u_hbm, sub_hbm, planes, a_ref, b_ref, watt, cat_ref, sub_ref, sems, *, halo):
    layers, height, width = u_hbm.shape
    copies = [
        pltpu.make_async_copy(source, target, sems.at[n])
        for n, (source, target) in enumerate(
            ((u_hbm, planes.at[pl.ds(0, layers)]), (sub_hbm, sub_ref), (cat_hbm, cat_ref), (watt_hbm, watt))
        )
    ]
    for copy in copies:
        copy.start()
    for copy in copies:
        copy.wait()
    cat = cat_ref[...]
    power = jnp.zeros(cat.shape, F32)
    for n in range(watt.shape[0]):
        power = power + jnp.where(cat == n, watt[n], 0.0)
    spread_r = (iota((height, cat.shape[0]), 0) // TILE == iota((height, cat.shape[0]), 1)).astype(F32)
    spread_c = (iota((cat.shape[1], width), 1) // TILE == iota((cat.shape[1], width), 0)).astype(F32)
    planes[2 * layers] = dot(dot(spread_r, power), spread_c)
    even = lax.axis_index("gy") % 2 == 0
    for q in range(2 * layers + 1):
        if layers <= q < 2 * layers:
            planes[q] = (sub_ref[q - layers] + 1).astype(F32)
        turned = planes[q].T
        low, high = turned[:halo], turned[width - halo :]
        a_ref[q] = jnp.where(even, high, low)
        b_ref[q] = jnp.where(even, low, high)


def split_kernel(own, ra, rb, out, a_ref, b_ref, scr, *, halo):
    count, height, width = own.shape
    layers = count // 2
    even_y, even_x = lax.axis_index("gy") % 2 == 0, lax.axis_index("gx") % 2 == 0
    half, hh = height // 2, halo // 2
    source, target = iota((width + LANES, 2 * LANES), 0), iota((width + LANES, 2 * LANES), 1)
    cell = 2 * (target % LANES) + target // LANES
    want = jnp.where(
        cell < halo, width + cell, jnp.where(cell < halo + width, cell - halo, cell)
    )
    pick = ((source == want) & (cell < 2 * halo + width)).astype(F32)
    planes = []
    for q in range(count):
        left = jnp.where(even_y, rb[q], ra[q])
        right = jnp.where(even_y, ra[q], rb[q])
        sides = jnp.concatenate([left, right, jnp.zeros((LANES - 2 * halo, height), F32)], 0).T
        planes.append(jnp.concatenate([own[q], sides], 1))
    first = pick_dot(jnp.concatenate(planes[:layers] + planes[2 * layers :], 0), pick)
    second = pick_dot(jnp.concatenate(planes[layers : 2 * layers], 0), pick, 1)
    for q in range(2 * layers + 1):
        if layers <= q < 2 * layers:
            both = second[(q - layers) * height : (q - layers + 1) * height]
        else:
            at = q if q < layers else layers
            both = first[at * height : (at + 1) * height]
        scr[q % 2, 0] = both[:, :LANES]
        scr[q % 2, 1] = both[:, LANES:]
        for p in range(2):
            for j in range(2):
                z = scr[q % 2, j, pl.ds(p, half, stride=2), :]
                out[q, 2 * p + j] = z
                at = (4 * q + 2 * p + j) * hh
                first_rows, last_rows = z[:hh], z[half - hh :]
                a_ref[at : at + hh] = jnp.where(even_x, last_rows, first_rows)
                b_ref[at : at + hh] = jnp.where(even_x, first_rows, last_rows)


def split_block(s, colour, t, layers):
    u, at = s["u"], rows(t)
    other = {
        (p, j, k): u[2 * p + j, k, at]
        for k in range(layers)
        for p in range(2)
        for j in range(2)
        if (p + j + k) % 2 != colour
    }
    for k in range(layers):
        for p in range(2):
            for j in range(2):
                if (p + j + k) % 2 != colour:
                    continue
                pj = 2 * p + j
                total = s["f"][pj, k, at] + s["fri"][j, k, at] * other[1 - p, j, k]
                if p == 0:
                    total += s["fro"][j, k, at] * u[2 + j, k, rows(t, -1)]
                else:
                    total += s["fro"][j, k, rows(t, 1)] * u[j, k, rows(t, 1)]
                beside = other[p, 1 - j, k]
                total += s["fci"][p, k, at] * beside
                if j == 0:
                    total += s["fco"][p, k, at] * pltpu.roll(beside, 1, 1)
                else:
                    total += s["fcr"][p, k, at] * pltpu.roll(beside, LANES - 1, 1)
                if k > 0:
                    total += s["fl"][pj, k, at] * other[p, j, k - 1]
                if k < layers - 1:
                    total += s["fl"][pj, k + 1, at] * other[p, j, k + 1]
                yield pj, k, total


def split_half(s, colour, lo, hi, layers):
    def body(t):
        for pj, k, total in split_block(s, colour, t, layers):
            s["u"][pj, k, rows(t)] = total * s["invd"][pj, k, rows(t)]

    over(lo, hi, MOST["split"], body)


def sides_of(tiles, edge):
    count = len(tiles)
    left = [pltpu.roll(x, 1, 1) for x in tiles]
    right = [pltpu.roll(x, LANES - 1, 1) for x in tiles]
    if count == 1 and not edge:
        return left, right
    lane = iota(tiles[0].shape, 1)
    return (
        [jnp.where(lane == 0, left[i - 1] if i else 0.0, left[i]) for i in range(count)],
        [
            jnp.where(lane == LANES - 1, right[i + 1] if i < count - 1 else 0.0, right[i])
            for i in range(count)
        ],
    )


def nat_setup(s, factor):
    tiles, layers, height, _ = s["lat"].shape
    c = 0.5 * factor

    def body(t):
        for k in range(layers):
            lat = [s["lat"][i, k, rows(t)] for i in range(tiles)]
            left, right = sides_of(lat, s["edge"])
            for i in range(tiles):
                stor = s["stor"][i, k, rows(t)]
                above = c * (lat[i] + s["lat"][i, k, rows(t, -1)])
                below = c * (lat[i] + s["lat"][i, k, rows(t, 1)])
                before, after = c * (lat[i] + left[i]), c * (lat[i] + right[i])
                diag = stor + above + below + before + after
                vert = s["vert"][i, k, rows(t)]
                if k > 0:
                    face = 0.5 * (vert + s["vert"][i, k - 1, rows(t)])
                    s["wl"][i, k, rows(t)] = face
                    diag += face
                if k < layers - 1:
                    diag += 0.5 * (vert + s["vert"][i, k + 1, rows(t)])
                inside = stor > 0.0
                s["wr"][i, k, rows(t)] = above
                s["wc"][i, k, rows(t)] = before
                s["wcr"][i, k, rows(t)] = after
                s["diag"][i, k, rows(t)] = diag
                s["invd"][i, k, rows(t)] = jnp.where(inside, 1.0 / jnp.where(inside, diag, 1.0), 0.0)

    s["wr"][:, :, height - PAD :] = jnp.zeros((tiles, layers, PAD, LANES), F32)
    over(0, (height - 2 * PAD) // 8, MOST["setup"], body)


def nat_block(s, t):
    u, at = s["u"], rows(t)
    tiles, layers = u.shape[:2]
    mid = [[u[i, k, at] for i in range(tiles)] for k in range(layers)]
    wl = [None] * tiles
    for k in range(layers):
        left, right = sides_of(mid[k], s["edge"])
        for i in range(tiles):
            total = s["f"][i, k, at] + s["wr"][i, k, at] * u[i, k, rows(t, -1)]
            total += s["wr"][i, k, rows(t, 1)] * u[i, k, rows(t, 1)]
            total += s["wc"][i, k, at] * left[i] + s["wcr"][i, k, at] * right[i]
            if k > 0:
                total += wl[i] * mid[k - 1][i]
            if k < layers - 1:
                wl[i] = s["wl"][i, k + 1, at]
                total += wl[i] * mid[k + 1][i]
            yield i, k, total, mid[k][i]


def nat_half(s, colour, lo, hi):
    def body(t):
        odd = (iota((8 * t[1], LANES), 0) + iota((8 * t[1], LANES), 1)) % 2
        for i, k, total, old in nat_block(s, t):
            value = total * s["invd"][i, k, rows(t)]
            s["u"][i, k, rows(t)] = jnp.where(odd == (colour + k) % 2, value, old)

    over(lo, hi, MOST["nat"], body)


def nat_first(s, lo, hi):
    tiles, layers, height, _ = s["u"].shape
    zeros = jnp.zeros((tiles, layers, PAD, LANES), F32)
    s["u"][:, :, :PAD] = zeros
    s["u"][:, :, height - PAD :] = zeros

    def body(t):
        odd = (iota((8 * t[1], LANES), 0) + iota((8 * t[1], LANES), 1)) % 2
        for k in range(layers):
            for i in range(tiles):
                value = s["f"][i, k, rows(t)] * s["invd"][i, k, rows(t)]
                s["u"][i, k, rows(t)] = jnp.where(odd == k % 2, value, 0.0)

    over(lo, hi, MOST["first"], body)


def nat_residual(s, res, lo, hi):
    def body(t):
        for i, k, total, old in nat_block(s, t):
            res[i, k, rows(t)] = total - s["diag"][i, k, rows(t)] * old

    over(lo, hi, MOST["residual"], body)


def nat_down(s, res, steps):
    nat_first(s, 0, steps)
    for colour in (1, 0, 1):
        nat_half(s, colour, 0, steps)
    nat_residual(s, res, 0, steps)


def restrict_all(pairs):
    tiles, layers = pairs[0][0].shape[:2]
    count, height = pairs[0][1].shape[0], pairs[0][1].shape[2] - 2 * PAD
    zeros = jnp.zeros((count, layers, PAD, LANES), F32)
    parts = [[] for i in range(tiles)]
    for source, target in pairs:
        target[:, :, :PAD] = zeros
        target[:, :, PAD + height :] = zeros
        for k in range(layers):
            for i in range(tiles):
                part = source[i, k, pl.ds(PAD, height, stride=2), :]
                parts[i].append(part + source[i, k, pl.ds(PAD + 1, height, stride=2), :])
    parts = [jnp.concatenate(p, 0) for p in parts]
    cell = iota((LANES, LANES), 0) // 2
    for o in range(count):
        total = None
        for i in range(tiles):
            shift = LANES // 2 * i - LANES * o
            if -LANES < shift < LANES:
                pick = jnp.where(cell + shift == iota((LANES, LANES), 1), 0.25, 0.0)
                part = pick_dot(parts[i], pick)
                total = part if total is None else total + part
        for n, (_, target) in enumerate(pairs):
            for k in range(layers):
                at = (n * layers + k) * height
                target[o, k, PAD : PAD + height] = total[at : at + height]


def prolong_into(s, u_in, coarse, mask):
    tiles, layers, height, _ = s["u"].shape
    n = (height - 2 * PAD) // 2
    tall = up8(n)
    cell = iota((LANES, LANES), 1) // 2
    for i in range(tiles):
        o = i // 2
        shift = LANES // 2 * (i % 2)
        pick = (cell + shift == iota((LANES, LANES), 0)).astype(F32)
        every = pick_dot(jnp.concatenate([coarse(o, k)[:tall] for k in range(layers)], 0), pick)
        for k in range(layers):
            wide = every[k * tall : k * tall + n]
            for p in range(2):
                at = pl.ds(PAD + p, n, stride=2)
                add = wide
                if mask:
                    add = jnp.where(s["invd"][i, k, at, :] > 0.0, wide, 0.0)
                s["u"][i, k, at, :] = u_in[i, k, at, :] + add


def nat_up(s, lo, hi):
    for sweep in range(2):
        nat_half(s, 0, lo, hi)
        nat_half(s, 1, lo, hi)


SPLIT_KEPT = ("u", "f", "invd", "fri", "fro", "fci", "fco", "fcr", "fl")
NAT_KEPT = ("u", "f", "invd", "wr", "wc", "wcr", "wl")
NAT_OTHER = ("lat", "vert", "stor", "diag")


def pack_own(payload, last, res, mine, off):
    layers = res.shape[1]
    group = 4 * mine
    per = LANES // group
    quantities = (res, last["lat"], last["vert"], last["stor"])
    parts = []
    for k in range(layers):
        for ref in quantities:
            part = ref[0, k, pl.ds(PAD + off, mine, stride=2), :]
            parts.append(part + ref[0, k, pl.ds(PAD + off + 1, mine, stride=2), :])
    source, target = iota((LANES, LANES), 0), iota((LANES, LANES), 1)
    hit = (source >= off) & ((source - off) // 2 == target) & (target < mine)
    packed = pick_dot(jnp.concatenate(parts, 0), jnp.where(hit, 0.25, 0.0))
    for pair in range(-(-layers // per)):
        total = jnp.zeros((mine, LANES), F32)
        for n in range(pair * per * 4, min(layers, (pair + 1) * per) * 4):
            part, base = packed[n * mine : (n + 1) * mine], (n - pair * per * 4) * mine
            total += pltpu.roll(part, base, 1) if base else part
        payload[pair * mine : (pair + 1) * mine] = total


def down_kernel(*refs, halo, half, kinds):
    tables, (sp, ra, rb) = refs[:3], refs[3:6]
    refs = list(refs[6:])
    s = dict(zip(SPLIT_KEPT, refs[: len(SPLIT_KEPT)]))
    refs = refs[len(SPLIT_KEPT) :]
    nats = []
    for level in range(1, FIRST):
        nats.append(dict(zip(NAT_KEPT, refs[: len(NAT_KEPT)]), edge=False))
        refs = refs[len(NAT_KEPT) :]
    payload = refs.pop(0)
    for name in ("lat", "vert", "stor", "diag"):
        s[name] = refs.pop(0)
    heat = refs.pop(0)
    for level in range(1, FIRST):
        for name in NAT_OTHER:
            nats[level - 1][name] = refs.pop(0)
    ress = [refs.pop(0) for level in range(1, FIRST)]
    layers = s["u"].shape[1]
    height = s["u"].shape[2]
    hh = halo // 2
    steps = (height - 2 * PAD) // 8
    even = lax.axis_index("gx") % 2 == 0
    zeros = jnp.zeros((PAD, LANES), F32)

    def place(ref, index, q, pj):
        at = (4 * q + pj) * hh
        first, second = ra[at : at + hh], rb[at : at + hh]
        ref[index + (slice(PAD, PAD + hh),)] = jnp.where(even, second, first)
        ref[index + (slice(PAD + hh, PAD + hh + half),)] = sp[q, pj]
        ref[index + (slice(PAD + hh + half, PAD + 2 * hh + half),)] = jnp.where(even, first, second)

    for pj in range(4):
        for k in range(layers):
            for name in ("u", "lat"):
                s[name][pj, k, :PAD] = zeros
                s[name][pj, k, height - PAD :] = zeros
            place(s["u"], (pj, k), k, pj)
            place(s["diag"], (pj, k), layers + k, pj)
        place(heat, (pj,), 2 * layers, pj)
    for j in range(2):
        for k in range(layers):
            s["fro"][j, k, height - PAD :] = zeros

    first = nats[0]
    clear = [first[name] for name in ("lat", "vert", "stor", "f")] + ress
    for ref in clear:
        for k in range(layers):
            ref[0, k, :PAD] = zeros
            ref[0, k, ref.shape[2] - PAD :] = zeros

    def look(t):
        for k in range(layers):
            sums = [None, None, None]
            for pj in range(4):
                at = (pj, k, rows(t))
                label = s["diag"][at]
                value = [jnp.zeros_like(label)] * 3
                for n in range(kinds):
                    hit = label == float(n + 1)
                    value = [jnp.where(hit, tables[i][n], value[i]) for i in range(3)]
                for i, name in enumerate(("lat", "vert", "stor")):
                    s[name][at] = value[i]
                    sums[i] = value[i] if sums[i] is None else sums[i] + value[i]
                f = value[2] * s["u"][at]
                if k == 0:
                    f = f + heat[pj, rows(t)]
                s["f"][at] = f
            for i, name in enumerate(("lat", "vert", "stor")):
                first[name][0, k, rows(t)] = sums[i] * 0.25

    over(0, steps, MOST["look"], look)

    def faces(t):
        at = rows(t)
        for k in range(layers):
            lat = [s["lat"][pj, k, at] for pj in range(4)]
            inner_r = [0.5 * (lat[j] + lat[2 + j]) for j in range(2)]
            before_r = [0.5 * (s["lat"][2 + j, k, rows(t, -1)] + lat[j]) for j in range(2)]
            after_r = [0.5 * (lat[2 + j] + s["lat"][j, k, rows(t, 1)]) for j in range(2)]
            inner_c = [0.5 * (lat[2 * p] + lat[2 * p + 1]) for p in range(2)]
            before_c = [0.5 * (pltpu.roll(lat[2 * p + 1], 1, 1) + lat[2 * p]) for p in range(2)]
            after_c = [0.5 * (lat[2 * p + 1] + pltpu.roll(lat[2 * p], LANES - 1, 1)) for p in range(2)]
            for x in range(2):
                s["fri"][x, k, at] = inner_r[x]
                s["fro"][x, k, at] = before_r[x]
                s["fci"][x, k, at] = inner_c[x]
                s["fco"][x, k, at] = before_c[x]
                s["fcr"][x, k, at] = after_c[x]
            for p in range(2):
                for j in range(2):
                    pj = 2 * p + j
                    stor = s["stor"][pj, k, at]
                    diag = stor + inner_r[j] + (after_r[j] if p else before_r[j])
                    diag += inner_c[p] + (after_c[p] if j else before_c[p])
                    vert = s["vert"][pj, k, at]
                    if k > 0:
                        face = 0.5 * (vert + s["vert"][pj, k - 1, at])
                        s["fl"][pj, k, at] = face
                        diag += face
                    if k < layers - 1:
                        diag += 0.5 * (vert + s["vert"][pj, k + 1, at])
                    inside = stor > 0.0
                    s["invd"][pj, k, at] = jnp.where(inside, 1.0 / jnp.where(inside, diag, 1.0), 0.0)
                    s["diag"][pj, k, at] = diag

    over(0, steps, MOST["faces"], faces)
    for sweep in range(2):
        split_half(s, 0, 0, steps, layers)
        split_half(s, 1, 0, steps, layers)

    def remain(t):
        sums = {}
        for pj, k, total in split_block(s, 0, t, layers):
            r = total - s["diag"][pj, k, rows(t)] * s["u"][pj, k, rows(t)]
            sums[k] = sums[k] + r if k in sums else r
            if pj >= 2:
                first["f"][0, k, rows(t)] = sums[k] * 0.25

    over(0, steps, MOST["remain"], remain)

    for level in range(1, FIRST):
        now = nats[level - 1]
        nat_setup(now, 0.25**level)
        count = (now["u"].shape[2] - 2 * PAD) // 8
        nat_down(now, ress[level - 1], count)
        if level < FIRST - 1:
            below = nats[level]
            pairs = [(now[name], below[name]) for name in ("lat", "vert", "stor")]
            restrict_all(pairs + [(ress[level - 1], below["f"])])

    pack_own(payload, nats[-1], ress[-1], 2 * half >> FIRST, halo >> (FIRST - 1))


def mid_kernel(own, ra, rb, ta, tb, *refs):
    refs = list(refs)
    count = LOCAL - FIRST
    nats = []
    for n in range(count):
        nats.append(dict(zip(NAT_KEPT, refs[: len(NAT_KEPT)]), edge=False))
        refs = refs[len(NAT_KEPT) :]
    payload = refs.pop(0)
    for n in range(count):
        for name in NAT_OTHER:
            nats[n][name] = refs.pop(0)
    ress = refs
    layers = nats[0]["u"].shape[1]
    mine = own.shape[0] // layers
    even_y, even_x = lax.axis_index("gy") % 2 == 0, lax.axis_index("gx") % 2 == 0
    zeros = jnp.zeros((PAD, LANES), F32)
    for now, res in zip(nats, ress):
        for ref in [now[name] for name in ("lat", "vert", "stor", "f")] + [res]:
            for k in range(layers):
                ref[0, k, :PAD] = zeros
                ref[0, k, ref.shape[2] - PAD :] = zeros
    group = iota((mine, LANES), 1) // mine
    for v in range(3):
        for k in range(layers):
            lines = slice(k * mine, (k + 1) * mine)
            if v == 1:
                middle, a, b = own[lines], ra[lines], rb[lines]
            else:
                first, second = (tb, ta) if v == 0 else (ta, tb)
                middle, a, b = [jnp.where(even_x, first[n, lines], second[n, lines]) for n in range(3)]
            left, right = jnp.where(even_y, b, a), jnp.where(even_y, a, b)
            middle, right = pltpu.roll(middle, mine, 1), pltpu.roll(right, 2 * mine, 1)
            for n, name in enumerate(("f", "lat", "vert", "stor")):
                value = jnp.where(group == (n + 1) % 4, middle, right)
                value = jnp.where(group == n, left, value)
                value = jnp.where(group == (n + 3) % 4, 0.0, value)
                if n:
                    value = pltpu.roll(value, LANES - n * mine, 1)
                nats[0][name][0, k, PAD + v * mine : PAD + (v + 1) * mine] = value
    for n, level in enumerate(range(FIRST, LOCAL)):
        now = nats[n]
        nat_setup(now, 0.25**level)
        nat_down(now, ress[n], (now["u"].shape[2] - 2 * PAD) // 8)
        if n < count - 1:
            pairs = [(now[name], nats[n + 1][name]) for name in ("lat", "vert", "stor")]
            restrict_all(pairs + [(ress[n], nats[n + 1]["f"])])
    pack_own(payload, nats[-1], ress[-1], mine >> count, mine >> (count - 1))


def conjugate(s, width):
    tiles, layers, height, _ = s["u"].shape
    assert tiles == 1
    n = height - 2 * PAD
    fold = max(f for f in range(1, layers + 1) if layers % f == 0 and f * width <= LANES)
    deep = layers // fold
    row, lane = iota((n, LANES), 0), iota((n, LANES), 1)
    here, after = slice(PAD, PAD + n), slice(PAD + 1, PAD + 1 + n)

    def folded(get, keep):
        out = []
        for k in range(deep):
            total = None
            for g in range(fold):
                value = get(g * deep + k)
                if value is None:
                    continue
                value = jnp.where(keep, value, 0.0)
                if g:
                    value = pltpu.roll(value, g * width, 1)
                total = value if total is None else total + value
            out.append(jnp.zeros((n, LANES), F32) if total is None else total)
        return out

    used = lane < width
    above = folded(lambda k: s["wr"][0, k, here], used & (row > 0))
    below = folded(lambda k: s["wr"][0, k, after], used & (row < n - 1))
    before = folded(lambda k: s["wc"][0, k, here], used & (lane > 0))
    behind = folded(lambda k: s["wcr"][0, k, here], lane < width - 1)
    under = folded(lambda k: s["wl"][0, k, here] if k else None, used)
    over_ = folded(lambda k: s["wl"][0, k + 1, here] if k < layers - 1 else None, used)
    diag = folded(lambda k: s["diag"][0, k, here], used)
    inv = folded(lambda k: s["invd"][0, k, here], used)
    r = folded(lambda k: s["f"][0, k, here], used)

    def apply(v):
        out = []
        for k in range(deep):
            total = above[k] * pltpu.roll(v[k], 1, 0) + below[k] * pltpu.roll(v[k], n - 1, 0)
            total += before[k] * pltpu.roll(v[k], 1, 1) + behind[k] * pltpu.roll(v[k], LANES - 1, 1)
            lower = v[k - 1] if k else pltpu.roll(v[deep - 1], width, 1)
            upper = v[k + 1] if k < deep - 1 else pltpu.roll(v[0], LANES - width, 1)
            out.append(diag[k] * v[k] - (total + under[k] * lower + over_[k] * upper))
        return out

    def inner(a, b):
        total = a[0] * b[0]
        for x, y in zip(a[1:], b[1:]):
            total += x * y
        return jnp.sum(jnp.sum(total, axis=0, keepdims=True), axis=1, keepdims=True)

    def step(_, carry):
        e, r, p = carry[:deep], carry[deep : 2 * deep], carry[2 * deep :]
        q = apply(p)
        z = [x * y for x, y in zip(r, inv)]
        w = [x * y for x, y in zip(q, inv)]
        rz, pq, zq, wq = inner(r, z), inner(p, q), inner(z, q), inner(w, q)
        alpha = rz / pq
        beta = (rz + alpha * (alpha * wq - 2.0 * zq)) / rz
        e = [x + alpha * y for x, y in zip(e, p)]
        r = [x - alpha * y for x, y in zip(r, q)]
        p = [x - alpha * y + beta * d for x, y, d in zip(z, w, p)]
        return (*e, *r, *p)

    start = (*[jnp.zeros((n, LANES), F32)] * deep, *r, *[x * y for x, y in zip(r, inv)])
    out = lax.fori_loop(0, COARSE_ITERS, step, start)
    for g in range(fold):
        for k in range(deep):
            value = pltpu.roll(out[k], LANES - g * width, 1) if g else out[k]
            s["u"][0, g * deep + k, here] = jnp.where(used, value, 0.0)


WHOLE = ("u", "f", "invd", "wr", "wc", "wcr", "wl", "lat", "vert", "stor", "diag")


def up_kernel(*refs, halo, half, spans):
    refs = list(refs)
    gathered = refs.pop(0)
    s = dict(zip(SPLIT_KEPT, refs[: len(SPLIT_KEPT)]))
    refs = refs[len(SPLIT_KEPT) :]
    nats = []
    for level in range(1, LOCAL):
        nats.append(dict(zip(NAT_KEPT, refs[: len(NAT_KEPT)]), edge=False))
        refs = refs[len(NAT_KEPT) :]
    out = refs.pop(0)
    wholes = []
    for level in range(LOCAL, LEVELS + 1):
        edge = (spans[1] * 2 * half >> level) % LANES == 0
        wholes.append(dict(zip(WHOLE, refs[: len(WHOLE)]), edge=edge))
        refs = refs[len(WHOLE) :]
    ress = [refs.pop(0) for level in range(LOCAL, LEVELS)]
    fresh = [refs.pop(0) for level in range(LOCAL)]
    wider = refs.pop(0)
    nx, ny = spans
    layers = s["u"].shape[1]
    top = wholes[0]
    tiles, _, tall, _ = top["u"].shape
    mine = 2 * half >> LOCAL
    group = 4 * mine
    per = LANES // group
    lane = iota((mine, LANES), 1)

    for whole in wholes:
        count, _, height, _ = whole["u"].shape
        for name in ("u", "lat"):
            zeros = jnp.zeros((count, layers, PAD, LANES), F32)
            whole[name][:, :, :PAD] = zeros
            whole[name][:, :, height - PAD :] = zeros

    def gather(x):
        at = pl.ds(pl.multiple_of(x * mine, 8) + PAD, mine)
        for i in range(tiles):
            here = [y for y in range(ny) if y * mine // LANES == i]
            for wide in range(-(-layers // per)):
                lines = slice(wide * mine, (wide + 1) * mine)
                parts = []
                for y in here:
                    part = gathered[x * ny + y, lines]
                    to = y * mine % LANES
                    parts.append(pltpu.roll(part, to, 1) if to else part)
                for k in range(wide * per, min(layers, (wide + 1) * per)):
                    for n, name in enumerate(("f", "lat", "vert", "stor")):
                        base = (k % per) * group + n * mine
                        total = jnp.zeros((mine, LANES), F32)
                        for y, part in zip(here, parts):
                            spot = (base + y * mine) % LANES
                            total = jnp.where((lane >= spot) & (lane < spot + mine), part, total)
                        top[name][i, k, at] = pltpu.roll(total, LANES - base, 1) if base else total

    def gather_some(step, carry):
        for n in range(4):
            gather(jnp.minimum(4 * step + n, nx - 1))
        return carry

    lax.fori_loop(0, -(-nx // 4), gather_some, 0)

    for n, level in enumerate(range(LOCAL, LEVELS)):
        now, below = wholes[n], wholes[n + 1]
        nat_setup(now, 0.25**level)
        nat_down(now, ress[n], (now["u"].shape[2] - 2 * PAD) // 8)
        pairs = [(now[name], below[name]) for name in ("lat", "vert", "stor")]
        restrict_all(pairs + [(ress[n], below["f"])])
    nat_setup(wholes[-1], 0.25**LEVELS)
    conjugate(wholes[-1], spans[1] * 2 * half >> LEVELS)
    for n in reversed(range(len(wholes) - 1)):
        now, below = wholes[n], wholes[n + 1]
        prolong_into(now, now["u"], lambda o, k: below["u"][o, k, PAD : below["u"].shape[2] - PAD], False)
        nat_up(now, 0, (now["u"].shape[2] - 2 * PAD) // 8)

    x, y = lax.axis_index("gx"), lax.axis_index("gy")
    reach = (2 * half >> FIRST) >> (LOCAL - FIRST)
    need = (nats[-1]["u"].shape[2] - 2 * PAD) // 2
    height = top["u"].shape[2]
    for i in range(tiles):
        for k in range(layers):
            wider[i, k, :height] = top["u"][i, k]
            wider[i, k, height:] = jnp.zeros((PAD, LANES), F32)
    begin = PAD + x * mine - reach
    shift = y * mine - reach

    def window(o, k):
        parts = [wider[i, k, pl.ds(begin, need)] for i in range(tiles)]
        turn = lax.rem(4 * LANES - shift, LANES)
        lanes = iota((need, LANES), 1)
        first = lax.div(shift + LANES, LANES) - 1
        value = jnp.zeros((need, LANES), F32)
        for i in range(tiles):
            moved = pltpu.roll(parts[i], turn, 1)
            value = jnp.where((first == i) & (lanes < turn) | (first == i) & (turn == 0), moved, value)
            value = jnp.where((first == i - 1) & (lanes >= turn) & (turn != 0), moved, value)
        return value

    coarse = window
    margins, above = [], 0
    for level in range(LOCAL):
        margins.append(above + 4)
        above = -(-margins[-1] // 2)
    for level in reversed(range(1, LOCAL)):
        now = dict(nats[level - 1])
        before = now["u"]
        now["u"] = fresh[level]
        height = before.shape[2]
        for i in range(before.shape[0]):
            for k in range(layers):
                now["u"][i, k, :PAD] = jnp.zeros((PAD, LANES), F32)
                now["u"][i, k, height - PAD :] = jnp.zeros((PAD, LANES), F32)
        prolong_into(now, before, coarse, level == LOCAL - 1)
        own = 2 * half >> level
        side = halo >> level if level < FIRST else (2 * half >> FIRST) >> (level - FIRST)
        reach = margins[level]
        nat_up(now, (side - reach) // 8, min(-(-(side + own + reach) // 8), (height - 2 * PAD) // 8))
        coarse = functools.partial(lambda ref, o, k: ref[o, k, PAD : ref.shape[2] - PAD], now["u"])
        if level == FIRST:
            skip = side - (halo >> FIRST)
            coarse = functools.partial(
                lambda ref, o, k: pltpu.roll(
                    ref[o, k, PAD + skip : ref.shape[2] - PAD], LANES - skip, 1
                ),
                now["u"],
            )

    now = dict(s)
    now["u"] = fresh[0]
    hh = halo // 2
    lo, hi = (hh - 2) // 8, -(-(hh + half + 2) // 8)
    steps = (s["u"].shape[2] - 2 * PAD) // 8

    def add(t):
        for k in range(layers):
            value = fresh[1][0, k, rows(t)]
            for pj in range(4):
                now["u"][pj, k, rows(t)] = s["u"][pj, k, rows(t)] + value

    over(lo - 1, min(hi + 1, steps), MOST["add"], add)
    for sweep in range(2):
        split_half(now, 0, lo, hi, layers)
        split_half(now, 1, lo, hi, layers)
    source, target = iota((2 * LANES, 2 * half), 0), iota((2 * LANES, 2 * half), 1)
    pick = ((source % LANES == hh + target // 2) & (source // LANES == target % 2)).astype(F32)
    body_rows = slice(PAD + hh, PAD + hh + half)
    spots = [(k, p) for k in range(layers) for p in range(2)]
    both = [
        jnp.concatenate([now["u"][2 * p + j, k, body_rows] for k, p in spots], 0) for j in range(2)
    ]
    every = pick_dot(jnp.concatenate(both, 1), pick)
    for n, (k, p) in enumerate(spots):
        out[k, pl.ds(p, half, stride=2), :] = every[n * half : (n + 1) * half]


def swap(values, axis, first):
    count = lax.axis_size(axis)
    pairs = [(i, i + 1) for i in range(first, count - 1, 2)]
    return lax.ppermute(values, axis, pairs + [(b, a) for a, b in pairs])


def shape(*dims):
    return jax.ShapeDtypeStruct(dims, F32)


def packed_shape(layers, mine):
    per = LANES // (4 * mine)
    return shape(-(-layers // per) * mine, LANES)


def whole_shape(level, layers, height, width):
    return -(-(width >> level) // LANES), layers, up8(height >> level) + 2 * PAD, LANES


def other_scratch(shapes):
    out = []
    for d in shapes:
        out += [pltpu.VMEM(d, F32)] * len(NAT_OTHER)
    return out + [pltpu.VMEM(d, F32) for d in shapes]


def on_device(u0, sub, cat, planar, vertical, ratio, watt):
    nx, ny = lax.axis_size("gx"), lax.axis_size("gy")
    layers, height, width = u0.shape
    halo = halo_cells()
    half, hh = height // 2, halo // 2
    planes = 2 * layers + 1
    assert height == width == LANES and 2 * halo <= LANES and halo + half <= LANES

    own, a, b = pl.pallas_call(
        functools.partial(prep_kernel, halo=halo),
        out_shape=(shape(planes, height, width), shape(planes, halo, height), shape(planes, halo, height)),
        in_specs=[HBM] * 4,
        out_specs=(VMEM,) * 3,
        scratch_shapes=[
            pltpu.SMEM(watt.shape, F32),
            pltpu.VMEM(cat.shape, jnp.int32),
            pltpu.VMEM(sub.shape, jnp.int32),
            pltpu.SemaphoreType.DMA((4,)),
        ],
        compiler_params=limit(8),
        name="prep",
    )(*[pltpu.with_memory_space_constraint(x, pltpu.HBM) for x in (watt, cat, u0, sub)])
    a, b = swap(a, "gy", 0), swap(b, "gy", 1)

    lines = planes * 4 * hh
    sp, a, b = pl.pallas_call(
        functools.partial(split_kernel, halo=halo),
        out_shape=(shape(planes, 4, half, LANES), shape(lines, LANES), shape(lines, LANES)),
        in_specs=[VMEM] * 3,
        out_specs=(VMEM,) * 3,
        scratch_shapes=[pltpu.VMEM((2, 2, height, LANES), F32)],
        compiler_params=limit(20),
        name="split",
    )(own, a, b)
    a, b = swap(a, "gx", 0), swap(b, "gx", 1)

    tall = up8(half + 2 * hh) + 2 * PAD
    four, two = (4, layers, tall, LANES), (2, layers, tall, LANES)
    kept = [shape(*(four if name in ("u", "f", "invd", "fl") else two)) for name in SPLIT_KEPT]
    nat_shapes = [
        (1, layers, up8((height + 2 * halo) >> level) + 2 * PAD, LANES) for level in range(1, FIRST)
    ]
    for d in nat_shapes:
        kept += [shape(*d)] * len(NAT_KEPT)
    scratch = [pltpu.VMEM(four, F32)] * 4 + [pltpu.VMEM((4, tall, LANES), F32)]
    scratch += other_scratch(nat_shapes)
    *saved, block = pl.pallas_call(
        functools.partial(down_kernel, halo=halo, half=half, kinds=planar.shape[0]),
        out_shape=(*kept, packed_shape(layers, height >> FIRST)),
        in_specs=[SMEM] * 3 + [VMEM] * 3,
        out_specs=(VMEM,) * (len(kept) + 1),
        scratch_shapes=scratch,
        compiler_params=limit(30),
        name="down",
    )(planar, vertical, ratio, sp, a, b)

    a, b = swap(block, "gy", 0), swap(block, "gy", 1)
    column = jnp.stack([block, a, b])
    above, below = swap(column, "gx", 0), swap(column, "gx", 1)
    mine = height >> FIRST
    assert 4 * mine <= LANES
    block_shapes = [
        (1, layers, up8(3 * mine >> n) + 2 * PAD, LANES) for n in range(LOCAL - FIRST)
    ]
    kept = []
    for d in block_shapes:
        kept += [shape(*d)] * len(NAT_KEPT)
    *more, payload = pl.pallas_call(
        mid_kernel,
        out_shape=(*kept, packed_shape(layers, height >> LOCAL)),
        in_specs=[VMEM] * 5,
        out_specs=(VMEM,) * (len(kept) + 1),
        scratch_shapes=other_scratch(block_shapes),
        compiler_params=limit(20),
        name="mid",
    )(block, a, b, above, below)
    saved += more
    nat_shapes += block_shapes

    sent = jnp.broadcast_to(payload[None], (nx * ny,) + payload.shape)
    gathered = lax.all_to_all(sent, ("gx", "gy"), 0, 0)

    scratch = []
    for level in range(LOCAL, LEVELS + 1):
        scratch += [pltpu.VMEM(whole_shape(level, layers, nx * height, ny * width), F32)] * len(WHOLE)
    for level in range(LOCAL, LEVELS):
        scratch.append(pltpu.VMEM(whole_shape(level, layers, nx * height, ny * width), F32))
    scratch += [pltpu.VMEM(four, F32)] + [pltpu.VMEM(d, F32) for d in nat_shapes]
    wide, count, rows_of, _ = scratch[0].shape
    scratch.append(pltpu.VMEM((wide, count, rows_of + PAD, LANES), F32))
    return pl.pallas_call(
        functools.partial(up_kernel, halo=halo, half=half, spans=(nx, ny)),
        out_shape=shape(layers, height, width),
        in_specs=[VMEM] * (1 + len(saved)),
        out_specs=VMEM,
        scratch_shapes=scratch,
        compiler_params=limit(16, scratch),
        name="up",
    )(gathered, *saved)


def solution(mesh):
    placed = (P(None, "gx", "gy"), P(None, "gx", "gy"), P("gx", "gy"), P(), P(), P(), P())
    return jax.shard_map(
        on_device, mesh=mesh, in_specs=placed, out_specs=P(None, "gx", "gy"), check_vma=False
    )
```

```python
import functools
import math

import jax
import jax.numpy as jnp
from jax import lax
from jax.experimental import pallas as pl
from jax.experimental.pallas import tpu as pltpu
from jax.sharding import PartitionSpec as P

TILE = 16
LEVELS = 6
FIRST = 2
LOCAL = 4
COARSE_ITERS = 12
LANES = 128
PAD = 8
MOST = dict(split=6, nat=12, first=12, residual=12, setup=6, look=1, faces=4, remain=6, add=4)
HI = lax.Precision.HIGHEST
F32 = jnp.float32
VMEM = pl.BlockSpec(memory_space=pltpu.VMEM)
SMEM = pl.BlockSpec(memory_space=pltpu.SMEM)
HBM = pl.BlockSpec(memory_space=pltpu.HBM)


def limit(mib, scratch=()):
    held = sum(4 * math.prod(ref.shape) for ref in scratch)
    return pltpu.CompilerParams(vmem_limit_bytes=mib * 1024 * 1024 + held + held // 4)


def up8(n):
    return -(-n // 8) * 8


def halo_cells():
    need, above = [], 0
    for level in range(FIRST):
        need.append(above + 4)
        above = -(-need[-1] // 2)
    f = 0
    for level in reversed(range(FIRST)):
        inner = max(need[level], 2 * f + 1)
        f = inner + (4 if level == 0 else 3)
    unit = 2**FIRST
    return -(-f // unit) * unit


def iota(shape, axis):
    return lax.broadcasted_iota(jnp.int32, shape, axis)


def rows(t, off=0):
    first, count = t
    start = first * 8 if isinstance(first, int) else pl.multiple_of(first * 8, 8)
    return pl.ds(start + (PAD + off), 8 * count)


def over(lo, hi, most, body):
    steps = -(-(hi - lo) // most)
    size = -(-(hi - lo) // steps)
    if steps == 1:
        body((lo, size))
        return

    def step(i, carry):
        body((jnp.minimum(lo + i * size, hi - size), size))
        return carry

    lax.fori_loop(0, steps, step, 0)


def dot(a, b):
    return jnp.dot(a, b, precision=HI, preferred_element_type=F32)


def pick_dot(x, pick, pieces=3):
    pick = pick.astype(jnp.bfloat16)
    total = None
    for n in range(pieces):
        piece = x.astype(jnp.bfloat16)
        part = jnp.dot(piece, pick, preferred_element_type=F32)
        total = part if total is None else total + part
        if n < pieces - 1:
            x = x - piece.astype(F32)
    return total


def prep_kernel(watt_hbm, cat_hbm, u_hbm, sub_hbm, planes, a_ref, b_ref, watt, cat_ref, sub_ref, sems, *, halo):
    layers, height, width = u_hbm.shape
    copies = [
        pltpu.make_async_copy(source, target, sems.at[n])
        for n, (source, target) in enumerate(
            ((u_hbm, planes.at[pl.ds(0, layers)]), (sub_hbm, sub_ref), (cat_hbm, cat_ref), (watt_hbm, watt))
        )
    ]
    for copy in copies:
        copy.start()
    for copy in copies:
        copy.wait()
    cat = cat_ref[...]
    power = jnp.zeros(cat.shape, F32)
    for n in range(watt.shape[0]):
        power = power + jnp.where(cat == n, watt[n], 0.0)
    spread_r = (iota((height, cat.shape[0]), 0) // TILE == iota((height, cat.shape[0]), 1)).astype(F32)
    spread_c = (iota((cat.shape[1], width), 1) // TILE == iota((cat.shape[1], width), 0)).astype(F32)
    planes[2 * layers] = dot(dot(spread_r, power), spread_c)
    even = lax.axis_index("gy") % 2 == 0
    for q in range(2 * layers + 1):
        if layers <= q < 2 * layers:
            planes[q] = (sub_ref[q - layers] + 1).astype(F32)
        turned = planes[q].T
        low, high = turned[:halo], turned[width - halo :]
        a_ref[q] = jnp.where(even, high, low)
        b_ref[q] = jnp.where(even, low, high)


def split_kernel(own, ra, rb, out, a_ref, b_ref, scr, *, halo):
    count, height, width = own.shape
    layers = count // 2
    even_y, even_x = lax.axis_index("gy") % 2 == 0, lax.axis_index("gx") % 2 == 0
    half, hh = height // 2, halo // 2
    source, target = iota((width + LANES, 2 * LANES), 0), iota((width + LANES, 2 * LANES), 1)
    cell = 2 * (target % LANES) + target // LANES
    want = jnp.where(
        cell < halo, width + cell, jnp.where(cell < halo + width, cell - halo, cell)
    )
    pick = ((source == want) & (cell < 2 * halo + width)).astype(F32)
    planes = []
    for q in range(count):
        left = jnp.where(even_y, rb[q], ra[q])
        right = jnp.where(even_y, ra[q], rb[q])
        sides = jnp.concatenate([left, right, jnp.zeros((LANES - 2 * halo, height), F32)], 0).T
        planes.append(jnp.concatenate([own[q], sides], 1))
    first = pick_dot(jnp.concatenate(planes[:layers] + planes[2 * layers :], 0), pick)
    second = pick_dot(jnp.concatenate(planes[layers : 2 * layers], 0), pick, 1)
    for q in range(2 * layers + 1):
        if layers <= q < 2 * layers:
            both = second[(q - layers) * height : (q - layers + 1) * height]
        else:
            at = q if q < layers else layers
            both = first[at * height : (at + 1) * height]
        scr[q % 2, 0] = both[:, :LANES]
        scr[q % 2, 1] = both[:, LANES:]
        for p in range(2):
            for j in range(2):
                z = scr[q % 2, j, pl.ds(p, half, stride=2), :]
                out[q, 2 * p + j] = z
                at = (4 * q + 2 * p + j) * hh
                first_rows, last_rows = z[:hh], z[half - hh :]
                a_ref[at : at + hh] = jnp.where(even_x, last_rows, first_rows)
                b_ref[at : at + hh] = jnp.where(even_x, first_rows, last_rows)


def split_block(s, colour, t, layers):
    u, at = s["u"], rows(t)
    other = {
        (p, j, k): u[2 * p + j, k, at]
        for k in range(layers)
        for p in range(2)
        for j in range(2)
        if (p + j + k) % 2 != colour
    }
    for k in range(layers):
        for p in range(2):
            for j in range(2):
                if (p + j + k) % 2 != colour:
                    continue
                pj = 2 * p + j
                total = s["f"][pj, k, at] + s["fri"][j, k, at] * other[1 - p, j, k]
                if p == 0:
                    total += s["fro"][j, k, at] * u[2 + j, k, rows(t, -1)]
                else:
                    total += s["fro"][j, k, rows(t, 1)] * u[j, k, rows(t, 1)]
                beside = other[p, 1 - j, k]
                total += s["fci"][p, k, at] * beside
                if j == 0:
                    total += s["fco"][p, k, at] * pltpu.roll(beside, 1, 1)
                else:
                    total += s["fcr"][p, k, at] * pltpu.roll(beside, LANES - 1, 1)
                if k > 0:
                    total += s["fl"][pj, k, at] * other[p, j, k - 1]
                if k < layers - 1:
                    total += s["fl"][pj, k + 1, at] * other[p, j, k + 1]
                yield pj, k, total


def split_half(s, colour, lo, hi, layers):
    def body(t):
        for pj, k, total in split_block(s, colour, t, layers):
            s["u"][pj, k, rows(t)] = total * s["invd"][pj, k, rows(t)]

    over(lo, hi, MOST["split"], body)


def split_sweeps(s, lo, hi, layers):
    for sweep in range(2):
        split_half(s, 0, lo, hi, layers)
        split_half(s, 1, lo, hi, layers)


def sides_of(tiles, edge):
    count = len(tiles)
    left = [pltpu.roll(x, 1, 1) for x in tiles]
    right = [pltpu.roll(x, LANES - 1, 1) for x in tiles]
    if count == 1 and not edge:
        return left, right
    lane = iota(tiles[0].shape, 1)
    return (
        [jnp.where(lane == 0, left[i - 1] if i else 0.0, left[i]) for i in range(count)],
        [
            jnp.where(lane == LANES - 1, right[i + 1] if i < count - 1 else 0.0, right[i])
            for i in range(count)
        ],
    )


def nat_setup(s, factor):
    tiles, layers, height, _ = s["lat"].shape
    c = 0.5 * factor

    def body(t):
        for k in range(layers):
            lat = [s["lat"][i, k, rows(t)] for i in range(tiles)]
            left, right = sides_of(lat, s["edge"])
            for i in range(tiles):
                stor = s["stor"][i, k, rows(t)]
                above = c * (lat[i] + s["lat"][i, k, rows(t, -1)])
                below = c * (lat[i] + s["lat"][i, k, rows(t, 1)])
                before, after = c * (lat[i] + left[i]), c * (lat[i] + right[i])
                diag = stor + above + below + before + after
                vert = s["vert"][i, k, rows(t)]
                if k > 0:
                    face = 0.5 * (vert + s["vert"][i, k - 1, rows(t)])
                    s["wl"][i, k, rows(t)] = face
                    diag += face
                if k < layers - 1:
                    diag += 0.5 * (vert + s["vert"][i, k + 1, rows(t)])
                inside = stor > 0.0
                s["wr"][i, k, rows(t)] = above
                s["wc"][i, k, rows(t)] = before
                s["wcr"][i, k, rows(t)] = after
                s["diag"][i, k, rows(t)] = diag
                s["invd"][i, k, rows(t)] = jnp.where(inside, 1.0 / jnp.where(inside, diag, 1.0), 0.0)

    s["wr"][:, :, height - PAD :] = jnp.zeros((tiles, layers, PAD, LANES), F32)
    over(0, (height - 2 * PAD) // 8, MOST["setup"], body)


def nat_block(s, t):
    u, at = s["u"], rows(t)
    tiles, layers = u.shape[:2]
    mid = [[u[i, k, at] for i in range(tiles)] for k in range(layers)]
    wl = [None] * tiles
    for k in range(layers):
        left, right = sides_of(mid[k], s["edge"])
        for i in range(tiles):
            total = s["f"][i, k, at] + s["wr"][i, k, at] * u[i, k, rows(t, -1)]
            total += s["wr"][i, k, rows(t, 1)] * u[i, k, rows(t, 1)]
            total += s["wc"][i, k, at] * left[i] + s["wcr"][i, k, at] * right[i]
            if k > 0:
                total += wl[i] * mid[k - 1][i]
            if k < layers - 1:
                wl[i] = s["wl"][i, k + 1, at]
                total += wl[i] * mid[k + 1][i]
            yield i, k, total, mid[k][i]


def nat_half(s, colour, lo, hi):
    def body(t):
        odd = (iota((8 * t[1], LANES), 0) + iota((8 * t[1], LANES), 1)) % 2
        for i, k, total, old in nat_block(s, t):
            value = total * s["invd"][i, k, rows(t)]
            s["u"][i, k, rows(t)] = jnp.where(odd == (colour + k) % 2, value, old)

    over(lo, hi, MOST["nat"], body)


def nat_first(s, lo, hi):
    tiles, layers, height, _ = s["u"].shape
    zeros = jnp.zeros((tiles, layers, PAD, LANES), F32)
    s["u"][:, :, :PAD] = zeros
    s["u"][:, :, height - PAD :] = zeros

    def body(t):
        odd = (iota((8 * t[1], LANES), 0) + iota((8 * t[1], LANES), 1)) % 2
        for k in range(layers):
            for i in range(tiles):
                value = s["f"][i, k, rows(t)] * s["invd"][i, k, rows(t)]
                s["u"][i, k, rows(t)] = jnp.where(odd == k % 2, value, 0.0)

    over(lo, hi, MOST["first"], body)


def nat_residual(s, res, lo, hi):
    def body(t):
        for i, k, total, old in nat_block(s, t):
            res[i, k, rows(t)] = total - s["diag"][i, k, rows(t)] * old

    over(lo, hi, MOST["residual"], body)


def nat_down(s, res, steps):
    nat_first(s, 0, steps)
    for colour in (1, 0, 1):
        nat_half(s, colour, 0, steps)
    nat_residual(s, res, 0, steps)


def restrict_all(pairs):
    tiles, layers = pairs[0][0].shape[:2]
    count, height = pairs[0][1].shape[0], pairs[0][1].shape[2] - 2 * PAD
    zeros = jnp.zeros((count, layers, PAD, LANES), F32)
    parts = [[] for i in range(tiles)]
    for source, target in pairs:
        target[:, :, :PAD] = zeros
        target[:, :, PAD + height :] = zeros
        for k in range(layers):
            for i in range(tiles):
                part = source[i, k, pl.ds(PAD, height, stride=2), :]
                parts[i].append(part + source[i, k, pl.ds(PAD + 1, height, stride=2), :])
    parts = [jnp.concatenate(p, 0) for p in parts]
    cell = iota((LANES, LANES), 0) // 2
    for o in range(count):
        total = None
        for i in range(tiles):
            shift = LANES // 2 * i - LANES * o
            if -LANES < shift < LANES:
                pick = jnp.where(cell + shift == iota((LANES, LANES), 1), 0.25, 0.0)
                part = pick_dot(parts[i], pick, 2)
                total = part if total is None else total + part
        for n, (_, target) in enumerate(pairs):
            for k in range(layers):
                at = (n * layers + k) * height
                target[o, k, PAD : PAD + height] = total[at : at + height]


def prolong_into(s, u_in, coarse, mask):
    tiles, layers, height, _ = s["u"].shape
    n = (height - 2 * PAD) // 2
    tall = up8(n)
    cell = iota((LANES, LANES), 1) // 2
    for i in range(tiles):
        o = i // 2
        shift = LANES // 2 * (i % 2)
        pick = (cell + shift == iota((LANES, LANES), 0)).astype(F32)
        every = pick_dot(jnp.concatenate([coarse(o, k)[:tall] for k in range(layers)], 0), pick, 2)
        for k in range(layers):
            wide = every[k * tall : k * tall + n]
            for p in range(2):
                at = pl.ds(PAD + p, n, stride=2)
                add = wide
                if mask:
                    add = jnp.where(s["invd"][i, k, at, :] > 0.0, wide, 0.0)
                s["u"][i, k, at, :] = u_in[i, k, at, :] + add


def nat_up(s, lo, hi):
    for sweep in range(2):
        nat_half(s, 0, lo, hi)
        nat_half(s, 1, lo, hi)


SPLIT_KEPT = ("u", "f", "invd", "fri", "fro", "fci", "fco", "fcr", "fl")
NAT_KEPT = ("u", "f", "invd", "wr", "wc", "wcr", "wl")
NAT_OTHER = ("lat", "vert", "stor", "diag")


def pack_own(payload, last, res, mine, off):
    layers = res.shape[1]
    group = 4 * mine
    per = LANES // group
    quantities = (res, last["lat"], last["vert"], last["stor"])
    parts = []
    for k in range(layers):
        for ref in quantities:
            part = ref[0, k, pl.ds(PAD + off, mine, stride=2), :]
            parts.append(part + ref[0, k, pl.ds(PAD + off + 1, mine, stride=2), :])
    source, target = iota((LANES, LANES), 0), iota((LANES, LANES), 1)
    hit = (source >= off) & ((source - off) // 2 == target) & (target < mine)
    packed = pick_dot(jnp.concatenate(parts, 0), jnp.where(hit, 0.25, 0.0), 2)
    for pair in range(-(-layers // per)):
        total = jnp.zeros((mine, LANES), F32)
        for n in range(pair * per * 4, min(layers, (pair + 1) * per) * 4):
            part, base = packed[n * mine : (n + 1) * mine], (n - pair * per * 4) * mine
            total += pltpu.roll(part, base, 1) if base else part
        payload[pair * mine : (pair + 1) * mine] = total


def look_up(s, first, heat, tables, kinds, lo, hi):
    layers = s["u"].shape[1]

    def look(t):
        for k in range(layers):
            sums = [None, None, None]
            for pj in range(4):
                at = (pj, k, rows(t))
                label = s["diag"][at]
                value = [jnp.zeros_like(label)] * 3
                for n in range(kinds):
                    hit = label == float(n + 1)
                    value = [jnp.where(hit, tables[i][n], value[i]) for i in range(3)]
                for i, name in enumerate(("lat", "vert", "stor")):
                    s[name][at] = value[i]
                    sums[i] = value[i] if sums[i] is None else sums[i] + value[i]
                f = value[2] * s["u"][at]
                if k == 0:
                    f = f + heat[pj, rows(t)]
                s["f"][at] = f
            for i, name in enumerate(("lat", "vert", "stor")):
                first[name][0, k, rows(t)] = sums[i] * 0.25

    over(lo, hi, MOST["look"], look)


def split_setup(s, lo, hi):
    layers = s["u"].shape[1]

    def faces(t):
        at = rows(t)
        for k in range(layers):
            lat = [s["lat"][pj, k, at] for pj in range(4)]
            inner_r = [0.5 * (lat[j] + lat[2 + j]) for j in range(2)]
            before_r = [0.5 * (s["lat"][2 + j, k, rows(t, -1)] + lat[j]) for j in range(2)]
            after_r = [0.5 * (lat[2 + j] + s["lat"][j, k, rows(t, 1)]) for j in range(2)]
            inner_c = [0.5 * (lat[2 * p] + lat[2 * p + 1]) for p in range(2)]
            before_c = [0.5 * (pltpu.roll(lat[2 * p + 1], 1, 1) + lat[2 * p]) for p in range(2)]
            after_c = [0.5 * (lat[2 * p + 1] + pltpu.roll(lat[2 * p], LANES - 1, 1)) for p in range(2)]
            for x in range(2):
                s["fri"][x, k, at] = inner_r[x]
                s["fro"][x, k, at] = before_r[x]
                s["fci"][x, k, at] = inner_c[x]
                s["fco"][x, k, at] = before_c[x]
                s["fcr"][x, k, at] = after_c[x]
            for p in range(2):
                for j in range(2):
                    pj = 2 * p + j
                    stor = s["stor"][pj, k, at]
                    diag = stor + inner_r[j] + (after_r[j] if p else before_r[j])
                    diag += inner_c[p] + (after_c[p] if j else before_c[p])
                    vert = s["vert"][pj, k, at]
                    if k > 0:
                        face = 0.5 * (vert + s["vert"][pj, k - 1, at])
                        s["fl"][pj, k, at] = face
                        diag += face
                    if k < layers - 1:
                        diag += 0.5 * (vert + s["vert"][pj, k + 1, at])
                    inside = stor > 0.0
                    s["invd"][pj, k, at] = jnp.where(inside, 1.0 / jnp.where(inside, diag, 1.0), 0.0)
                    s["diag"][pj, k, at] = diag

    over(lo, hi, MOST["faces"], faces)


SHARED = SPLIT_KEPT + ("lat", "vert", "stor", "diag", "heat", "lat1", "vert1", "stor1")


def center_kernel(*refs, halo, half, kinds):
    tables, sp, out = refs[:3], refs[3], refs[4:]
    s = dict(zip(SHARED, out))
    first = {name: s[name + "1"] for name in ("lat", "vert", "stor")}
    layers, height, hh = s["u"].shape[1], s["u"].shape[2], halo // 2
    body_rows = slice(PAD + hh, PAD + hh + half)
    zeros = jnp.zeros((PAD, LANES), F32)
    for pj in range(4):
        for k in range(layers):
            for name in ("u", "lat"):
                s[name][pj, k, :PAD] = zeros
                s[name][pj, k, height - PAD :] = zeros
            s["u"][pj, k, body_rows] = sp[k, pj]
            s["diag"][pj, k, body_rows] = sp[layers + k, pj]
        s["heat"][pj, body_rows] = sp[2 * layers, pj]
    for ref in first.values():
        for k in range(layers):
            ref[0, k, :PAD] = zeros
            ref[0, k, height - PAD :] = zeros
    look_up(s, first, s["heat"], tables, kinds, *bounds(hh, half, 0))
    split_setup(s, *bounds(hh, half, 1))


def bounds(hh, half, inner):
    if inner:
        return -(-(hh + 1) // 8), (hh + half - 1) // 8
    return hh // 8, -(-(hh + half) // 8)


def down_kernel(*refs, halo, half, kinds):
    tables, (ra, rb) = refs[:3], refs[3:5]
    refs = list(refs[5 + len(SHARED) :])
    s = dict(zip(SHARED, refs[: len(SHARED)]))
    refs = refs[len(SHARED) :]
    nats = [{} for level in range(1, FIRST)]
    for n, now in enumerate(nats):
        now.update(zip(NAT_KEPT, refs[: len(NAT_KEPT)]), edge=False)
        refs = refs[len(NAT_KEPT) :]
    payload = refs.pop(0)
    heat = s["heat"]
    for n, now in enumerate(nats):
        for name in NAT_OTHER:
            now[name] = s[name + "1"] if n == 0 and name != "diag" else refs.pop(0)
    ress = [refs.pop(0) for level in range(1, FIRST)]
    layers = s["u"].shape[1]
    height = s["u"].shape[2]
    hh = halo // 2
    steps = (height - 2 * PAD) // 8
    even = lax.axis_index("gx") % 2 == 0
    zeros = jnp.zeros((PAD, LANES), F32)

    def place(ref, index, q, pj):
        at = (4 * q + pj) * hh
        first, second = ra[at : at + hh], rb[at : at + hh]
        ref[index + (slice(PAD, PAD + hh),)] = jnp.where(even, second, first)
        ref[index + (slice(PAD + hh + half, PAD + 2 * hh + half),)] = jnp.where(even, first, second)

    for pj in range(4):
        for k in range(layers):
            place(s["u"], (pj, k), k, pj)
            place(s["diag"], (pj, k), layers + k, pj)
        place(heat, (pj,), 2 * layers, pj)
    for j in range(2):
        for k in range(layers):
            s["fro"][j, k, height - PAD :] = zeros
    first = nats[0]
    for ref in [first["f"]] + ress:
        for k in range(layers):
            ref[0, k, :PAD] = zeros
            ref[0, k, ref.shape[2] - PAD :] = zeros
    lo, hi = bounds(hh, half, 1)
    for begin, end in ((0, lo), (hi, steps)):
        look_up(s, first, heat, tables, kinds, begin, end)
    for begin, end in ((0, lo), (hi, steps)):
        split_setup(s, begin, end)
    split_sweeps(s, 0, steps, layers)

    def remain(t):
        sums = {}
        for pj, k, total in split_block(s, 0, t, layers):
            r = total - s["diag"][pj, k, rows(t)] * s["u"][pj, k, rows(t)]
            sums[k] = sums[k] + r if k in sums else r
            if pj >= 2:
                first["f"][0, k, rows(t)] = sums[k] * 0.25

    over(0, steps, MOST["remain"], remain)

    for level in range(1, FIRST):
        now = nats[level - 1]
        nat_setup(now, 0.25**level)
        count = (now["u"].shape[2] - 2 * PAD) // 8
        nat_down(now, ress[level - 1], count)
        if level < FIRST - 1:
            below = nats[level]
            pairs = [(now[name], below[name]) for name in ("lat", "vert", "stor")]
            restrict_all(pairs + [(ress[level - 1], below["f"])])

    pack_own(payload, nats[-1], ress[-1], 2 * half >> FIRST, halo >> (FIRST - 1))


def mid_kernel(own, ra, rb, ta, tb, *refs):
    refs = list(refs)
    count = LOCAL - FIRST
    nats = []
    for n in range(count):
        nats.append(dict(zip(NAT_KEPT, refs[: len(NAT_KEPT)]), edge=False))
        refs = refs[len(NAT_KEPT) :]
    payload = refs.pop(0)
    for n in range(count):
        for name in NAT_OTHER:
            nats[n][name] = refs.pop(0)
    ress = refs
    layers = nats[0]["u"].shape[1]
    mine = own.shape[0] // layers
    even_y, even_x = lax.axis_index("gy") % 2 == 0, lax.axis_index("gx") % 2 == 0
    zeros = jnp.zeros((PAD, LANES), F32)
    for now, res in zip(nats, ress):
        for ref in [now[name] for name in ("lat", "vert", "stor", "f")] + [res]:
            for k in range(layers):
                ref[0, k, :PAD] = zeros
                ref[0, k, ref.shape[2] - PAD :] = zeros
    group = iota((mine, LANES), 1) // mine
    for v in range(3):
        for k in range(layers):
            lines = slice(k * mine, (k + 1) * mine)
            if v == 1:
                middle, a, b = own[lines], ra[lines], rb[lines]
            else:
                first, second = (tb, ta) if v == 0 else (ta, tb)
                middle, a, b = [jnp.where(even_x, first[n, lines], second[n, lines]) for n in range(3)]
            left, right = jnp.where(even_y, b, a), jnp.where(even_y, a, b)
            middle, right = pltpu.roll(middle, mine, 1), pltpu.roll(right, 2 * mine, 1)
            for n, name in enumerate(("f", "lat", "vert", "stor")):
                value = jnp.where(group == (n + 1) % 4, middle, right)
                value = jnp.where(group == n, left, value)
                value = jnp.where(group == (n + 3) % 4, 0.0, value)
                if n:
                    value = pltpu.roll(value, LANES - n * mine, 1)
                nats[0][name][0, k, PAD + v * mine : PAD + (v + 1) * mine] = value
    for n, level in enumerate(range(FIRST, LOCAL)):
        now = nats[n]
        nat_setup(now, 0.25**level)
        nat_down(now, ress[n], (now["u"].shape[2] - 2 * PAD) // 8)
        if n < count - 1:
            pairs = [(now[name], nats[n + 1][name]) for name in ("lat", "vert", "stor")]
            restrict_all(pairs + [(ress[n], nats[n + 1]["f"])])
    pack_own(payload, nats[-1], ress[-1], mine >> count, mine >> (count - 1))


def conjugate(s, width):
    tiles, layers, height, _ = s["u"].shape
    assert tiles == 1
    n = height - 2 * PAD
    fold = max(f for f in range(1, layers + 1) if layers % f == 0 and f * width <= LANES)
    deep = layers // fold
    row, lane = iota((n, LANES), 0), iota((n, LANES), 1)
    here, after = slice(PAD, PAD + n), slice(PAD + 1, PAD + 1 + n)

    def folded(get, keep):
        out = []
        for k in range(deep):
            total = None
            for g in range(fold):
                value = get(g * deep + k)
                if value is None:
                    continue
                value = jnp.where(keep, value, 0.0)
                if g:
                    value = pltpu.roll(value, g * width, 1)
                total = value if total is None else total + value
            out.append(jnp.zeros((n, LANES), F32) if total is None else total)
        return out

    used = lane < width
    above = folded(lambda k: s["wr"][0, k, here], used & (row > 0))
    below = folded(lambda k: s["wr"][0, k, after], used & (row < n - 1))
    before = folded(lambda k: s["wc"][0, k, here], used & (lane > 0))
    behind = folded(lambda k: s["wcr"][0, k, here], lane < width - 1)
    under = folded(lambda k: s["wl"][0, k, here] if k else None, used)
    over_ = folded(lambda k: s["wl"][0, k + 1, here] if k < layers - 1 else None, used)
    diag = folded(lambda k: s["diag"][0, k, here], used)
    inv = folded(lambda k: s["invd"][0, k, here], used)
    r = folded(lambda k: s["f"][0, k, here], used)

    def apply(v):
        out = []
        for k in range(deep):
            total = above[k] * pltpu.roll(v[k], 1, 0) + below[k] * pltpu.roll(v[k], n - 1, 0)
            total += before[k] * pltpu.roll(v[k], 1, 1) + behind[k] * pltpu.roll(v[k], LANES - 1, 1)
            lower = v[k - 1] if k else pltpu.roll(v[deep - 1], width, 1)
            upper = v[k + 1] if k < deep - 1 else pltpu.roll(v[0], LANES - width, 1)
            out.append(diag[k] * v[k] - (total + under[k] * lower + over_[k] * upper))
        return out

    def inner(a, b):
        total = a[0] * b[0]
        for x, y in zip(a[1:], b[1:]):
            total += x * y
        return jnp.sum(jnp.sum(total, axis=0, keepdims=True), axis=1, keepdims=True)

    def step(_, carry):
        e, r, p = carry[:deep], carry[deep : 2 * deep], carry[2 * deep :]
        q = apply(p)
        z = [x * y for x, y in zip(r, inv)]
        w = [x * y for x, y in zip(q, inv)]
        rz, pq, zq, wq = inner(r, z), inner(p, q), inner(z, q), inner(w, q)
        alpha = rz / pq
        beta = (rz + alpha * (alpha * wq - 2.0 * zq)) / rz
        e = [x + alpha * y for x, y in zip(e, p)]
        r = [x - alpha * y for x, y in zip(r, q)]
        p = [x - alpha * y + beta * d for x, y, d in zip(z, w, p)]
        return (*e, *r, *p)

    start = (*[jnp.zeros((n, LANES), F32)] * deep, *r, *[x * y for x, y in zip(r, inv)])
    out = lax.fori_loop(0, COARSE_ITERS, step, start)
    for g in range(fold):
        for k in range(deep):
            value = pltpu.roll(out[k], LANES - g * width, 1) if g else out[k]
            s["u"][0, g * deep + k, here] = jnp.where(used, value, 0.0)


WHOLE = ("u", "f", "invd", "wr", "wc", "wcr", "wl", "lat", "vert", "stor", "diag")


def up_kernel(*refs, halo, half, spans):
    refs = list(refs)
    gathered = refs.pop(0)
    s = dict(zip(SPLIT_KEPT, refs[: len(SPLIT_KEPT)]))
    refs = refs[len(SPLIT_KEPT) :]
    nats = []
    for level in range(1, LOCAL):
        nats.append(dict(zip(NAT_KEPT, refs[: len(NAT_KEPT)]), edge=False))
        refs = refs[len(NAT_KEPT) :]
    out = refs.pop(0)
    wholes = []
    for level in range(LOCAL, LEVELS + 1):
        edge = (spans[1] * 2 * half >> level) % LANES == 0
        wholes.append(dict(zip(WHOLE, refs[: len(WHOLE)]), edge=edge))
        refs = refs[len(WHOLE) :]
    ress = [refs.pop(0) for level in range(LOCAL, LEVELS)]
    fresh = [refs.pop(0) for level in range(LOCAL)]
    wider = refs.pop(0)
    nx, ny = spans
    layers = s["u"].shape[1]
    top = wholes[0]
    tiles, _, tall, _ = top["u"].shape
    mine = 2 * half >> LOCAL
    group = 4 * mine
    per = LANES // group
    lane = iota((mine, LANES), 1)

    for whole in wholes:
        count, _, height, _ = whole["u"].shape
        for name in ("u", "lat"):
            zeros = jnp.zeros((count, layers, PAD, LANES), F32)
            whole[name][:, :, :PAD] = zeros
            whole[name][:, :, height - PAD :] = zeros

    def gather(x):
        at = pl.ds(pl.multiple_of(x * mine, 8) + PAD, mine)
        for i in range(tiles):
            here = [y for y in range(ny) if y * mine // LANES == i]
            for wide in range(-(-layers // per)):
                lines = slice(wide * mine, (wide + 1) * mine)
                parts = []
                for y in here:
                    part = gathered[x * ny + y, lines]
                    to = y * mine % LANES
                    parts.append(pltpu.roll(part, to, 1) if to else part)
                for k in range(wide * per, min(layers, (wide + 1) * per)):
                    for n, name in enumerate(("f", "lat", "vert", "stor")):
                        base = (k % per) * group + n * mine
                        total = jnp.zeros((mine, LANES), F32)
                        for y, part in zip(here, parts):
                            spot = (base + y * mine) % LANES
                            total = jnp.where((lane >= spot) & (lane < spot + mine), part, total)
                        top[name][i, k, at] = pltpu.roll(total, LANES - base, 1) if base else total

    def gather_some(step, carry):
        for n in range(4):
            gather(jnp.minimum(4 * step + n, nx - 1))
        return carry

    lax.fori_loop(0, -(-nx // 4), gather_some, 0)

    for n, level in enumerate(range(LOCAL, LEVELS)):
        now, below = wholes[n], wholes[n + 1]
        nat_setup(now, 0.25**level)
        nat_down(now, ress[n], (now["u"].shape[2] - 2 * PAD) // 8)
        pairs = [(now[name], below[name]) for name in ("lat", "vert", "stor")]
        restrict_all(pairs + [(ress[n], below["f"])])
    nat_setup(wholes[-1], 0.25**LEVELS)
    conjugate(wholes[-1], spans[1] * 2 * half >> LEVELS)
    for n in reversed(range(len(wholes) - 1)):
        now, below = wholes[n], wholes[n + 1]
        prolong_into(now, now["u"], lambda o, k: below["u"][o, k, PAD : below["u"].shape[2] - PAD], False)
        nat_up(now, 0, (now["u"].shape[2] - 2 * PAD) // 8)

    x, y = lax.axis_index("gx"), lax.axis_index("gy")
    reach = (2 * half >> FIRST) >> (LOCAL - FIRST)
    need = (nats[-1]["u"].shape[2] - 2 * PAD) // 2
    height = top["u"].shape[2]
    for i in range(tiles):
        for k in range(layers):
            wider[i, k, :height] = top["u"][i, k]
            wider[i, k, height:] = jnp.zeros((PAD, LANES), F32)
    begin = PAD + x * mine - reach
    shift = y * mine - reach

    def window(o, k):
        parts = [wider[i, k, pl.ds(begin, need)] for i in range(tiles)]
        turn = lax.rem(4 * LANES - shift, LANES)
        lanes = iota((need, LANES), 1)
        first = lax.div(shift + LANES, LANES) - 1
        value = jnp.zeros((need, LANES), F32)
        for i in range(tiles):
            moved = pltpu.roll(parts[i], turn, 1)
            value = jnp.where((first == i) & (lanes < turn) | (first == i) & (turn == 0), moved, value)
            value = jnp.where((first == i - 1) & (lanes >= turn) & (turn != 0), moved, value)
        return value

    coarse = window
    margins, above = [], 0
    for level in range(LOCAL):
        margins.append(above + 4)
        above = -(-margins[-1] // 2)
    for level in reversed(range(1, LOCAL)):
        now = dict(nats[level - 1])
        before = now["u"]
        now["u"] = fresh[level]
        height = before.shape[2]
        for i in range(before.shape[0]):
            for k in range(layers):
                now["u"][i, k, :PAD] = jnp.zeros((PAD, LANES), F32)
                now["u"][i, k, height - PAD :] = jnp.zeros((PAD, LANES), F32)
        prolong_into(now, before, coarse, level == LOCAL - 1)
        own = 2 * half >> level
        side = halo >> level if level < FIRST else (2 * half >> FIRST) >> (level - FIRST)
        reach = margins[level]
        nat_up(now, (side - reach) // 8, min(-(-(side + own + reach) // 8), (height - 2 * PAD) // 8))
        coarse = functools.partial(lambda ref, o, k: ref[o, k, PAD : ref.shape[2] - PAD], now["u"])
        if level == FIRST:
            skip = side - (halo >> FIRST)
            coarse = functools.partial(
                lambda ref, o, k: pltpu.roll(
                    ref[o, k, PAD + skip : ref.shape[2] - PAD], LANES - skip, 1
                ),
                now["u"],
            )

    now = dict(s)
    now["u"] = fresh[0]
    hh = halo // 2
    lo, hi = (hh - 2) // 8, -(-(hh + half + 2) // 8)
    steps = (s["u"].shape[2] - 2 * PAD) // 8

    def add(t):
        for k in range(layers):
            value = fresh[1][0, k, rows(t)]
            for pj in range(4):
                now["u"][pj, k, rows(t)] = s["u"][pj, k, rows(t)] + value

    over(lo - 1, min(hi + 1, steps), MOST["add"], add)
    split_sweeps(now, lo, hi, layers)
    source, target = iota((2 * LANES, 2 * half), 0), iota((2 * LANES, 2 * half), 1)
    pick = ((source % LANES == hh + target // 2) & (source // LANES == target % 2)).astype(F32)
    body_rows = slice(PAD + hh, PAD + hh + half)
    spots = [(k, p) for k in range(layers) for p in range(2)]
    both = [
        jnp.concatenate([now["u"][2 * p + j, k, body_rows] for k, p in spots], 0) for j in range(2)
    ]
    every = pick_dot(jnp.concatenate(both, 1), pick)
    for n, (k, p) in enumerate(spots):
        out[k, pl.ds(p, half, stride=2), :] = every[n * half : (n + 1) * half]


def swap(values, axis, first):
    count = lax.axis_size(axis)
    pairs = [(i, i + 1) for i in range(first, count - 1, 2)]
    return lax.ppermute(values, axis, pairs + [(b, a) for a, b in pairs])


def shape(*dims):
    return jax.ShapeDtypeStruct(dims, F32)


def packed_shape(layers, mine):
    per = LANES // (4 * mine)
    return shape(-(-layers // per) * mine, LANES)


def whole_shape(level, layers, height, width):
    return -(-(width >> level) // LANES), layers, up8(height >> level) + 2 * PAD, LANES


def other_scratch(shapes):
    out = []
    for d in shapes:
        out += [pltpu.VMEM(d, F32)] * len(NAT_OTHER)
    return out + [pltpu.VMEM(d, F32) for d in shapes]


def on_device(u0, sub, cat, planar, vertical, ratio, watt):
    nx, ny = lax.axis_size("gx"), lax.axis_size("gy")
    layers, height, width = u0.shape
    halo = halo_cells()
    half, hh = height // 2, halo // 2
    planes = 2 * layers + 1
    assert height == width == LANES and 2 * halo <= LANES and halo + half <= LANES

    own, a, b = pl.pallas_call(
        functools.partial(prep_kernel, halo=halo),
        out_shape=(shape(planes, height, width), shape(planes, halo, height), shape(planes, halo, height)),
        in_specs=[HBM] * 4,
        out_specs=(VMEM,) * 3,
        scratch_shapes=[
            pltpu.SMEM(watt.shape, F32),
            pltpu.VMEM(cat.shape, jnp.int32),
            pltpu.VMEM(sub.shape, jnp.int32),
            pltpu.SemaphoreType.DMA((4,)),
        ],
        compiler_params=limit(8),
        name="prep",
    )(*[pltpu.with_memory_space_constraint(x, pltpu.HBM) for x in (watt, cat, u0, sub)])
    a, b = swap(a, "gy", 0), swap(b, "gy", 1)

    lines = planes * 4 * hh
    sp, a, b = pl.pallas_call(
        functools.partial(split_kernel, halo=halo),
        out_shape=(shape(planes, 4, half, LANES), shape(lines, LANES), shape(lines, LANES)),
        in_specs=[VMEM] * 3,
        out_specs=(VMEM,) * 3,
        scratch_shapes=[pltpu.VMEM((2, 2, height, LANES), F32)],
        compiler_params=limit(20),
        name="split",
    )(own, a, b)
    a, b = swap(a, "gx", 0), swap(b, "gx", 1)

    tall = up8(half + 2 * hh) + 2 * PAD
    four, two = (4, layers, tall, LANES), (2, layers, tall, LANES)
    nat_shapes = [
        (1, layers, up8((height + 2 * halo) >> level) + 2 * PAD, LANES) for level in range(1, FIRST)
    ]
    sizes = [four if name in ("u", "f", "invd", "fl") else two for name in SPLIT_KEPT]
    sizes += [four] * 4 + [(4, tall, LANES)] + [nat_shapes[0]] * 3
    shared = pl.pallas_call(
        functools.partial(center_kernel, halo=halo, half=half, kinds=planar.shape[0]),
        out_shape=tuple(shape(*d) for d in sizes),
        in_specs=[SMEM] * 3 + [VMEM],
        out_specs=(VMEM,) * len(sizes),
        compiler_params=limit(24),
        name="center",
    )(planar, vertical, ratio, sp)
    kept = []
    for d in nat_shapes:
        kept += [shape(*d)] * len(NAT_KEPT)
    *saved, block = pl.pallas_call(
        functools.partial(down_kernel, halo=halo, half=half, kinds=planar.shape[0]),
        out_shape=(*[shape(*d) for d in sizes], *kept, packed_shape(layers, height >> FIRST)),
        in_specs=[SMEM] * 3 + [VMEM] * (2 + len(sizes)),
        out_specs=(VMEM,) * (len(sizes) + len(kept) + 1),
        scratch_shapes=other_scratch(nat_shapes)[3:],
        input_output_aliases={5 + n: n for n in range(len(sizes))},
        compiler_params=limit(26),
        name="down",
    )(planar, vertical, ratio, a, b, *shared)
    saved = saved[: len(SPLIT_KEPT)] + saved[len(sizes) :]

    a, b = swap(block, "gy", 0), swap(block, "gy", 1)
    column = jnp.stack([block, a, b])
    above, below = swap(column, "gx", 0), swap(column, "gx", 1)
    mine = height >> FIRST
    assert 4 * mine <= LANES
    block_shapes = [
        (1, layers, up8(3 * mine >> n) + 2 * PAD, LANES) for n in range(LOCAL - FIRST)
    ]
    kept = []
    for d in block_shapes:
        kept += [shape(*d)] * len(NAT_KEPT)
    *more, payload = pl.pallas_call(
        mid_kernel,
        out_shape=(*kept, packed_shape(layers, height >> LOCAL)),
        in_specs=[VMEM] * 5,
        out_specs=(VMEM,) * (len(kept) + 1),
        scratch_shapes=other_scratch(block_shapes),
        compiler_params=limit(20),
        name="mid",
    )(block, a, b, above, below)
    saved += more
    nat_shapes += block_shapes

    sent = jnp.broadcast_to(payload[None], (nx * ny,) + payload.shape)
    gathered = lax.all_to_all(sent, ("gx", "gy"), 0, 0)

    scratch = []
    for level in range(LOCAL, LEVELS + 1):
        scratch += [pltpu.VMEM(whole_shape(level, layers, nx * height, ny * width), F32)] * len(WHOLE)
    for level in range(LOCAL, LEVELS):
        scratch.append(pltpu.VMEM(whole_shape(level, layers, nx * height, ny * width), F32))
    scratch += [pltpu.VMEM(four, F32)] + [pltpu.VMEM(d, F32) for d in nat_shapes]
    wide, count, rows_of, _ = scratch[0].shape
    scratch.append(pltpu.VMEM((wide, count, rows_of + PAD, LANES), F32))
    return pl.pallas_call(
        functools.partial(up_kernel, halo=halo, half=half, spans=(nx, ny)),
        out_shape=shape(layers, height, width),
        in_specs=[VMEM] * (1 + len(saved)),
        out_specs=VMEM,
        scratch_shapes=scratch,
        compiler_params=limit(16, scratch),
        name="up",
    )(gathered, *saved)


def solution(mesh):
    placed = (P(None, "gx", "gy"), P(None, "gx", "gy"), P("gx", "gy"), P(), P(), P(), P())
    return jax.shard_map(
        on_device, mesh=mesh, in_specs=placed, out_specs=P(None, "gx", "gy"), check_vma=False
    )
```

```python
import functools
import math

import jax
import jax.numpy as jnp
from jax import lax
from jax.experimental import pallas as pl
from jax.experimental.pallas import tpu as pltpu
from jax.sharding import PartitionSpec as P

TILE = 16
LEVELS = 6
FIRST = 2
LOCAL = 4
COARSE_ITERS = 12
LANES = 128
PAD = 8
MOST = dict(split=6, nat=12, first=12, residual=12, setup=6, look=1, faces=4, remain=6, add=4)
HI = lax.Precision.HIGHEST
F32 = jnp.float32
VMEM = pl.BlockSpec(memory_space=pltpu.VMEM)
SMEM = pl.BlockSpec(memory_space=pltpu.SMEM)
HBM = pl.BlockSpec(memory_space=pltpu.HBM)


def limit(mib, scratch=()):
    held = sum(4 * math.prod(ref.shape) for ref in scratch)
    return pltpu.CompilerParams(vmem_limit_bytes=mib * 1024 * 1024 + held + held // 4)


def up8(n):
    return -(-n // 8) * 8


def halo_cells():
    need, above = [], 0
    for level in range(FIRST):
        need.append(above + 4)
        above = -(-need[-1] // 2)
    f = 0
    for level in reversed(range(FIRST)):
        inner = max(need[level], 2 * f + 1)
        f = inner + (4 if level == 0 else 3)
    unit = 2**FIRST
    return -(-f // unit) * unit


def iota(shape, axis):
    return lax.broadcasted_iota(jnp.int32, shape, axis)


def rows(t, off=0):
    first, count = t
    start = first * 8 if isinstance(first, int) else pl.multiple_of(first * 8, 8)
    return pl.ds(start + (PAD + off), 8 * count)


def over(lo, hi, most, body):
    steps = -(-(hi - lo) // most)
    size = -(-(hi - lo) // steps)
    if steps == 1:
        body((lo, size))
        return

    def step(i, carry):
        body((jnp.minimum(lo + i * size, hi - size), size))
        return carry

    lax.fori_loop(0, steps, step, 0)


def dot(a, b):
    return jnp.dot(a, b, precision=HI, preferred_element_type=F32)


def pick_dot(x, pick, pieces=3):
    pick = pick.astype(jnp.bfloat16)
    total = None
    for n in range(pieces):
        piece = x.astype(jnp.bfloat16)
        part = jnp.dot(piece, pick, preferred_element_type=F32)
        total = part if total is None else total + part
        if n < pieces - 1:
            x = x - piece.astype(F32)
    return total


def prep_kernel(watt_hbm, cat_hbm, u_hbm, sub_hbm, planes, a_ref, b_ref, watt, cat_ref, sub_ref, sems, *, halo):
    layers, height, width = u_hbm.shape
    copies = [
        pltpu.make_async_copy(source, target, sems.at[n])
        for n, (source, target) in enumerate(
            ((u_hbm, planes.at[pl.ds(0, layers)]), (sub_hbm, sub_ref), (cat_hbm, cat_ref), (watt_hbm, watt))
        )
    ]
    for copy in copies:
        copy.start()
    even = lax.axis_index("gy") % 2 == 0

    def send(q):
        turned = planes[q].T
        low, high = turned[:halo], turned[width - halo :]
        a_ref[q] = jnp.where(even, high, low)
        b_ref[q] = jnp.where(even, low, high)

    copies[0].wait()
    for q in range(layers):
        send(q)
    copies[1].wait()
    for q in range(layers, 2 * layers):
        planes[q] = (sub_ref[q - layers] + 1).astype(F32)
        send(q)
    copies[2].wait()
    copies[3].wait()
    cat = cat_ref[...]
    power = jnp.zeros(cat.shape, F32)
    for n in range(watt.shape[0]):
        power = power + jnp.where(cat == n, watt[n], 0.0)
    spread_r = (iota((height, cat.shape[0]), 0) // TILE == iota((height, cat.shape[0]), 1)).astype(F32)
    spread_c = (iota((cat.shape[1], width), 1) // TILE == iota((cat.shape[1], width), 0)).astype(F32)
    planes[2 * layers] = dot(dot(spread_r, power), spread_c)
    send(2 * layers)


def split_kernel(own, ra, rb, out, a_ref, b_ref, scr, *, halo):
    count, height, width = own.shape
    layers = count // 2
    even_y, even_x = lax.axis_index("gy") % 2 == 0, lax.axis_index("gx") % 2 == 0
    half, hh = height // 2, halo // 2
    source, target = iota((width + LANES, 2 * LANES), 0), iota((width + LANES, 2 * LANES), 1)
    cell = 2 * (target % LANES) + target // LANES
    want = jnp.where(
        cell < halo, width + cell, jnp.where(cell < halo + width, cell - halo, cell)
    )
    pick = ((source == want) & (cell < 2 * halo + width)).astype(F32)
    planes = []
    for q in range(count):
        left = jnp.where(even_y, rb[q], ra[q])
        right = jnp.where(even_y, ra[q], rb[q])
        sides = jnp.concatenate([left, right, jnp.zeros((LANES - 2 * halo, height), F32)], 0).T
        planes.append(jnp.concatenate([own[q], sides], 1))
    first = pick_dot(jnp.concatenate(planes[:layers] + planes[2 * layers :], 0), pick)
    second = pick_dot(jnp.concatenate(planes[layers : 2 * layers], 0), pick, 1)
    for q in range(2 * layers + 1):
        if layers <= q < 2 * layers:
            both = second[(q - layers) * height : (q - layers + 1) * height]
        else:
            at = q if q < layers else layers
            both = first[at * height : (at + 1) * height]
        scr[q % 2, 0] = both[:, :LANES]
        scr[q % 2, 1] = both[:, LANES:]
        for p in range(2):
            for j in range(2):
                z = scr[q % 2, j, pl.ds(p, half, stride=2), :]
                out[q, 2 * p + j] = z
                at = (4 * q + 2 * p + j) * hh
                first_rows, last_rows = z[:hh], z[half - hh :]
                a_ref[at : at + hh] = jnp.where(even_x, last_rows, first_rows)
                b_ref[at : at + hh] = jnp.where(even_x, first_rows, last_rows)


def split_block(s, colour, t, layers):
    u, at = s["u"], rows(t)
    other = {
        (p, j, k): u[2 * p + j, k, at]
        for k in range(layers)
        for p in range(2)
        for j in range(2)
        if (p + j + k) % 2 != colour
    }
    for k in range(layers):
        for p in range(2):
            for j in range(2):
                if (p + j + k) % 2 != colour:
                    continue
                pj = 2 * p + j
                total = s["f"][pj, k, at] + s["fri"][j, k, at] * other[1 - p, j, k]
                if p == 0:
                    total += s["fro"][j, k, at] * u[2 + j, k, rows(t, -1)]
                else:
                    total += s["fro"][j, k, rows(t, 1)] * u[j, k, rows(t, 1)]
                beside = other[p, 1 - j, k]
                total += s["fci"][p, k, at] * beside
                if j == 0:
                    total += s["fco"][p, k, at] * pltpu.roll(beside, 1, 1)
                else:
                    total += s["fcr"][p, k, at] * pltpu.roll(beside, LANES - 1, 1)
                if k > 0:
                    total += s["fl"][pj, k, at] * other[p, j, k - 1]
                if k < layers - 1:
                    total += s["fl"][pj, k + 1, at] * other[p, j, k + 1]
                yield pj, k, total


def split_half(s, colour, lo, hi, layers):
    def body(t):
        for pj, k, total in split_block(s, colour, t, layers):
            s["u"][pj, k, rows(t)] = total * s["invd"][pj, k, rows(t)]

    over(lo, hi, MOST["split"], body)


def split_sweeps(s, lo, hi, layers):
    for sweep in range(2):
        split_half(s, 0, lo, hi, layers)
        split_half(s, 1, lo, hi, layers)


def geometry(layers, width):
    assert width <= LANES
    fold = max(f for f in range(1, layers + 1) if layers % f == 0 and f * width <= LANES)
    return fold, width, layers // fold


def places(extent, geo):
    lane = iota(extent, 1)
    group = jnp.zeros(extent, jnp.int32)
    for g in range(1, geo[0] + 1):
        if g * geo[1] < LANES:
            group = group + (lane >= g * geo[1]).astype(jnp.int32)
    return group, lane - group * geo[1]


def odd_cells(t, geo):
    extent = (8 * t[1], LANES)
    group, col = places(extent, geo)
    return (iota(extent, 0) + col + group * geo[2]) % 2


def nat_setup(s, factor):
    fold, width, deep = s["geo"]
    height = s["lat"].shape[1]
    c = 0.5 * factor

    def body(t):
        at = rows(t)
        group, col = places((8 * t[1], LANES), s["geo"])
        first, last = col == 0, col == width - 1
        between = None
        for k in range(deep):
            lat, stor, vert = s["lat"][k, at], s["stor"][k, at], s["vert"][k, at]
            above = c * (lat + s["lat"][k, rows(t, -1)])
            below = c * (lat + s["lat"][k, rows(t, 1)])
            before = c * (lat + jnp.where(first, 0.0, pltpu.roll(lat, 1, 1)))
            after = c * (lat + jnp.where(last, 0.0, pltpu.roll(lat, LANES - 1, 1)))
            diag = stor + above + below + before + after
            if k > 0:
                face = 0.5 * (vert + s["vert"][k - 1, at])
                s["wl"][k, at] = face
                diag += face
            elif fold > 1:
                between = 0.5 * (vert + pltpu.roll(s["vert"][deep - 1, at], width, 1))
                between = jnp.where((group > 0) & (group < fold), between, 0.0)
                s["wl"][0, at] = between
                diag += between
            if k < deep - 1:
                diag += 0.5 * (vert + s["vert"][k + 1, at])
            elif fold > 1:
                diag += pltpu.roll(between, LANES - width, 1)
            inside = stor > 0.0
            s["wr"][k, at] = above
            s["wc"][k, at] = jnp.where(first, 0.0, before)
            s["wcr"][k, at] = jnp.where(last, 0.0, after)
            s["diag"][k, at] = diag
            s["invd"][k, at] = jnp.where(inside, 1.0 / jnp.where(inside, diag, 1.0), 0.0)

    s["wr"][:, height - PAD :] = jnp.zeros((deep, PAD, LANES), F32)
    over(0, (height - 2 * PAD) // 8, MOST["setup"], body)


def nat_block(s, t):
    u, at = s["u"], rows(t)
    fold, width, deep = s["geo"]
    mid = [u[k, at] for k in range(deep)]
    wl = s["wl"][0, at] if fold > 1 else None
    between = None if wl is None else pltpu.roll(wl * mid[0], LANES - width, 1)
    for k in range(deep):
        total = s["f"][k, at] + s["wr"][k, at] * u[k, rows(t, -1)]
        total += s["wr"][k, rows(t, 1)] * u[k, rows(t, 1)]
        beside = s["wc"][k, at] * pltpu.roll(mid[k], 1, 1)
        beside += s["wcr"][k, at] * pltpu.roll(mid[k], LANES - 1, 1)
        if k > 0:
            total += wl * mid[k - 1]
        elif fold > 1:
            total += wl * pltpu.roll(mid[deep - 1], width, 1)
        if k < deep - 1:
            wl = s["wl"][k + 1, at]
            total += wl * mid[k + 1]
        elif fold > 1:
            total += between
        yield k, total + beside, mid[k]


def nat_half(s, colour, lo, hi):
    def body(t):
        odd = odd_cells(t, s["geo"])
        for k, total, old in nat_block(s, t):
            value = total * s["invd"][k, rows(t)]
            s["u"][k, rows(t)] = jnp.where(odd == (colour + k) % 2, value, old)

    over(lo, hi, MOST["nat"], body)


def nat_first(s, lo, hi):
    deep, height, _ = s["u"].shape
    zeros = jnp.zeros((deep, PAD, LANES), F32)
    s["u"][:, :PAD] = zeros
    s["u"][:, height - PAD :] = zeros

    def body(t):
        odd = odd_cells(t, s["geo"])
        for k in range(deep):
            value = s["f"][k, rows(t)] * s["invd"][k, rows(t)]
            s["u"][k, rows(t)] = jnp.where(odd == k % 2, value, 0.0)

    over(lo, hi, MOST["first"], body)


def nat_residual(s, res, lo, hi):
    def body(t):
        for k, total, old in nat_block(s, t):
            res[k, rows(t)] = total - s["diag"][k, rows(t)] * old

    over(lo, hi, MOST["residual"], body)


def nat_down(s, res, steps):
    nat_first(s, 0, steps)
    for colour in (1, 0, 1):
        nat_half(s, colour, 0, steps)
    nat_residual(s, res, 0, steps)


def move(parts, a, b, relation, scale):
    jobs = {}
    for ka in range(a[2]):
        for kb in range(b[2]):
            key = tuple(
                (ga, gb)
                for ga in range(a[0])
                for gb in range(b[0])
                if ga * a[2] + ka == gb * b[2] + kb
            )
            if key:
                jobs.setdefault(key, []).append((ka, kb))
    c, m = iota((LANES, LANES), 0), iota((LANES, LANES), 1)
    out = [None] * b[2]
    count = parts[0].shape[0]
    for key, members in jobs.items():
        hit = None
        for ga, gb in key:
            ca, mb = c - ga * a[1], m - gb * b[1]
            here = (ca >= 0) & (ca < a[1]) & (mb >= 0) & (mb < b[1]) & relation(ca, mb)
            hit = here if hit is None else hit | here
        moved = pick_dot(
            jnp.concatenate([parts[ka] for ka, _ in members], 0), jnp.where(hit, scale, 0.0), 2
        )
        for n, (_, kb) in enumerate(members):
            part = moved[n * count : (n + 1) * count]
            out[kb] = part if out[kb] is None else out[kb] + part
    return out


def pair_rows(ref, k, start, count):
    part = ref[k, pl.ds(start, count, stride=2), :]
    return part + ref[k, pl.ds(start + 1, count, stride=2), :]


def restrict_all(pairs, a, b):
    deep, height = pairs[0][1].shape[0], pairs[0][1].shape[1] - 2 * PAD
    zeros = jnp.zeros((deep, PAD, LANES), F32)
    for _, target in pairs:
        target[:, :PAD] = zeros
        target[:, PAD + height :] = zeros
    parts = [
        jnp.concatenate([pair_rows(source, k, PAD, height) for source, _ in pairs], 0)
        for k in range(a[2])
    ]
    out = move(parts, a, b, lambda c, m: c // 2 == m, 0.25)
    for n, (_, target) in enumerate(pairs):
        for k in range(deep):
            target[k, PAD : PAD + height] = out[k][n * height : (n + 1) * height]


def prolong_into(s, u_in, coarse, geo, mask):
    deep, height, _ = s["u"].shape
    n = (height - 2 * PAD) // 2
    tall = up8(n)
    parts = [coarse(k)[:tall] for k in range(geo[2])]
    out = move(parts, geo, s["geo"], lambda c, m: c == m // 2, 1.0)
    for k in range(deep):
        wide = out[k][:n]
        for p in range(2):
            at = pl.ds(PAD + p, n, stride=2)
            add = wide
            if mask:
                add = jnp.where(s["invd"][k, at, :] > 0.0, wide, 0.0)
            s["u"][k, at, :] = u_in[k, at, :] + add


def nat_up(s, lo, hi):
    for sweep in range(2):
        nat_half(s, 0, lo, hi)
        nat_half(s, 1, lo, hi)


SPLIT_KEPT = ("u", "f", "invd", "fri", "fro", "fci", "fco", "fcr", "fl")
NAT_KEPT = ("u", "f", "invd", "wr", "wc", "wcr", "wl")
NAT_OTHER = ("lat", "vert", "stor", "diag")


def pack_own(payload, last, res, layers, mine, off):
    group = 4 * mine
    per = LANES // group
    quantities = (res, last["lat"], last["vert"], last["stor"])
    parts = [
        jnp.concatenate([pair_rows(ref, k, PAD + off, mine) for ref in quantities], 0)
        for k in range(last["geo"][2])
    ]
    packed = move(
        parts, last["geo"], (1, mine, layers), lambda c, m: (c >= off) & ((c - off) // 2 == m), 0.25
    )
    for wide in range(-(-layers // per)):
        total = jnp.zeros((mine, LANES), F32)
        for n in range(wide * per * 4, min(layers, (wide + 1) * per) * 4):
            part = packed[n // 4][n % 4 * mine : (n % 4 + 1) * mine]
            base = (n - wide * per * 4) * mine
            total += pltpu.roll(part, base, 1) if base else part
        payload[wide * mine : (wide + 1) * mine] = total


def look_up(s, first, heat, tables, kinds, lo, hi):
    layers = s["u"].shape[1]

    def look(t):
        for k in range(layers):
            sums = [None, None, None]
            for pj in range(4):
                at = (pj, k, rows(t))
                label = s["diag"][at]
                value = [jnp.zeros_like(label)] * 3
                for n in range(kinds):
                    hit = label == float(n + 1)
                    value = [jnp.where(hit, tables[i][n], value[i]) for i in range(3)]
                for i, name in enumerate(("lat", "vert", "stor")):
                    s[name][at] = value[i]
                    sums[i] = value[i] if sums[i] is None else sums[i] + value[i]
                f = value[2] * s["u"][at]
                if k == 0:
                    f = f + heat[pj, rows(t)]
                s["f"][at] = f
            for i, name in enumerate(("lat", "vert", "stor")):
                first[name][k, rows(t)] = sums[i] * 0.25

    over(lo, hi, MOST["look"], look)


def split_setup(s, lo, hi):
    layers = s["u"].shape[1]

    def faces(t):
        at = rows(t)
        for k in range(layers):
            lat = [s["lat"][pj, k, at] for pj in range(4)]
            inner_r = [0.5 * (lat[j] + lat[2 + j]) for j in range(2)]
            before_r = [0.5 * (s["lat"][2 + j, k, rows(t, -1)] + lat[j]) for j in range(2)]
            after_r = [0.5 * (lat[2 + j] + s["lat"][j, k, rows(t, 1)]) for j in range(2)]
            inner_c = [0.5 * (lat[2 * p] + lat[2 * p + 1]) for p in range(2)]
            before_c = [0.5 * (pltpu.roll(lat[2 * p + 1], 1, 1) + lat[2 * p]) for p in range(2)]
            after_c = [0.5 * (lat[2 * p + 1] + pltpu.roll(lat[2 * p], LANES - 1, 1)) for p in range(2)]
            for x in range(2):
                s["fri"][x, k, at] = inner_r[x]
                s["fro"][x, k, at] = before_r[x]
                s["fci"][x, k, at] = inner_c[x]
                s["fco"][x, k, at] = before_c[x]
                s["fcr"][x, k, at] = after_c[x]
            for p in range(2):
                for j in range(2):
                    pj = 2 * p + j
                    stor = s["stor"][pj, k, at]
                    diag = stor + inner_r[j] + (after_r[j] if p else before_r[j])
                    diag += inner_c[p] + (after_c[p] if j else before_c[p])
                    vert = s["vert"][pj, k, at]
                    if k > 0:
                        face = 0.5 * (vert + s["vert"][pj, k - 1, at])
                        s["fl"][pj, k, at] = face
                        diag += face
                    if k < layers - 1:
                        diag += 0.5 * (vert + s["vert"][pj, k + 1, at])
                    inside = stor > 0.0
                    s["invd"][pj, k, at] = jnp.where(inside, 1.0 / jnp.where(inside, diag, 1.0), 0.0)
                    s["diag"][pj, k, at] = diag

    over(lo, hi, MOST["faces"], faces)


SHARED = SPLIT_KEPT + ("lat", "vert", "stor", "diag", "heat", "lat1", "vert1", "stor1")


def center_kernel(*refs, halo, half, kinds):
    tables, sp, out = refs[:3], refs[3], refs[4:]
    s = dict(zip(SHARED, out))
    first = {name: s[name + "1"] for name in ("lat", "vert", "stor")}
    layers, height, hh = s["u"].shape[1], s["u"].shape[2], halo // 2
    body_rows = slice(PAD + hh, PAD + hh + half)
    zeros = jnp.zeros((PAD, LANES), F32)
    for pj in range(4):
        for k in range(layers):
            for name in ("u", "lat"):
                s[name][pj, k, :PAD] = zeros
                s[name][pj, k, height - PAD :] = zeros
            s["u"][pj, k, body_rows] = sp[k, pj]
            s["diag"][pj, k, body_rows] = sp[layers + k, pj]
        s["heat"][pj, body_rows] = sp[2 * layers, pj]
    for ref in first.values():
        for k in range(layers):
            ref[k, :PAD] = zeros
            ref[k, height - PAD :] = zeros
    look_up(s, first, s["heat"], tables, kinds, *bounds(hh, half, 0))
    split_setup(s, *bounds(hh, half, 1))


def bounds(hh, half, inner):
    if inner:
        return -(-(hh + 1) // 8), (hh + half - 1) // 8
    return hh // 8, -(-(hh + half) // 8)


def down_kernel(*refs, halo, half, kinds, geos):
    tables, (ra, rb) = refs[:3], refs[3:5]
    refs = list(refs[5 + len(SHARED) :])
    s = dict(zip(SHARED, refs[: len(SHARED)]))
    refs = refs[len(SHARED) :]
    nats = [{} for level in range(1, FIRST)]
    for n, now in enumerate(nats):
        now.update(zip(NAT_KEPT, refs[: len(NAT_KEPT)]), geo=geos[n])
        refs = refs[len(NAT_KEPT) :]
    payload = refs.pop(0)
    heat = s["heat"]
    for n, now in enumerate(nats):
        for name in NAT_OTHER:
            now[name] = s[name + "1"] if n == 0 and name != "diag" else refs.pop(0)
    ress = [refs.pop(0) for level in range(1, FIRST)]
    layers = s["u"].shape[1]
    height = s["u"].shape[2]
    hh = halo // 2
    steps = (height - 2 * PAD) // 8
    even = lax.axis_index("gx") % 2 == 0
    zeros = jnp.zeros((PAD, LANES), F32)

    def place(ref, index, q, pj):
        at = (4 * q + pj) * hh
        first, second = ra[at : at + hh], rb[at : at + hh]
        ref[index + (slice(PAD, PAD + hh),)] = jnp.where(even, second, first)
        ref[index + (slice(PAD + hh + half, PAD + 2 * hh + half),)] = jnp.where(even, first, second)

    for pj in range(4):
        for k in range(layers):
            place(s["u"], (pj, k), k, pj)
            place(s["diag"], (pj, k), layers + k, pj)
        place(heat, (pj,), 2 * layers, pj)
    for j in range(2):
        for k in range(layers):
            s["fro"][j, k, height - PAD :] = zeros
    first = nats[0]
    for ref in [first["f"]] + ress:
        for k in range(ref.shape[0]):
            ref[k, :PAD] = zeros
            ref[k, ref.shape[1] - PAD :] = zeros
    lo, hi = bounds(hh, half, 1)
    for begin, end in ((0, lo), (hi, steps)):
        look_up(s, first, heat, tables, kinds, begin, end)
    for begin, end in ((0, lo), (hi, steps)):
        split_setup(s, begin, end)
    split_sweeps(s, 0, steps, layers)

    def remain(t):
        sums = {}
        for pj, k, total in split_block(s, 0, t, layers):
            r = total - s["diag"][pj, k, rows(t)] * s["u"][pj, k, rows(t)]
            sums[k] = sums[k] + r if k in sums else r
            if pj >= 2:
                first["f"][k, rows(t)] = sums[k] * 0.25

    over(0, steps, MOST["remain"], remain)

    for level in range(1, FIRST):
        now = nats[level - 1]
        nat_setup(now, 0.25**level)
        count = (now["u"].shape[1] - 2 * PAD) // 8
        nat_down(now, ress[level - 1], count)
        if level < FIRST - 1:
            below = nats[level]
            pairs = [(now[name], below[name]) for name in ("lat", "vert", "stor")]
            restrict_all(pairs + [(ress[level - 1], below["f"])], now["geo"], below["geo"])

    pack_own(payload, nats[-1], ress[-1], layers, 2 * half >> FIRST, halo >> (FIRST - 1))


def mid_kernel(own, ra, rb, ta, tb, *refs, geos):
    refs = list(refs)
    count = LOCAL - FIRST
    nats = []
    for n in range(count):
        nats.append(dict(zip(NAT_KEPT, refs[: len(NAT_KEPT)]), geo=geos[n]))
        refs = refs[len(NAT_KEPT) :]
    payload = refs.pop(0)
    for n in range(count):
        for name in NAT_OTHER:
            nats[n][name] = refs.pop(0)
    ress = refs
    layers = geos[0][0] * geos[0][2]
    mine = own.shape[0] // layers
    assert geos[0][0] == 1
    even_y, even_x = lax.axis_index("gy") % 2 == 0, lax.axis_index("gx") % 2 == 0
    zeros = jnp.zeros((PAD, LANES), F32)
    for now, res in zip(nats, ress):
        for ref in [now[name] for name in ("lat", "vert", "stor", "f")] + [res]:
            for k in range(ref.shape[0]):
                ref[k, :PAD] = zeros
                ref[k, ref.shape[1] - PAD :] = zeros
    group = iota((mine, LANES), 1) // mine

    def assemble(v, middle_of, a_of, b_of):
        for k in range(layers):
            lines = slice(k * mine, (k + 1) * mine)
            middle, a, b = middle_of(lines), a_of(lines), b_of(lines)
            left, right = jnp.where(even_y, b, a), jnp.where(even_y, a, b)
            middle, right = pltpu.roll(middle, mine, 1), pltpu.roll(right, 2 * mine, 1)
            for n, name in enumerate(("f", "lat", "vert", "stor")):
                value = jnp.where(group == (n + 1) % 4, middle, right)
                value = jnp.where(group == n, left, value)
                value = jnp.where(group == (n + 3) % 4, 0.0, value)
                if n:
                    value = pltpu.roll(value, LANES - n * mine, 1)
                nats[0][name][k, PAD + v * mine : PAD + (v + 1) * mine] = value

    def rows_from(ref):
        return [lambda lines, n=n: ref[n, lines] for n in range(3)]

    def outer(above, below):
        assemble(0, *rows_from(above))
        assemble(2, *rows_from(below))

    assemble(1, *[lambda lines, ref=ref: ref[lines] for ref in (own, ra, rb)])
    pl.when(even_x)(lambda: outer(tb, ta))
    pl.when(jnp.logical_not(even_x))(lambda: outer(ta, tb))
    for n, level in enumerate(range(FIRST, LOCAL)):
        now = nats[n]
        nat_setup(now, 0.25**level)
        nat_down(now, ress[n], (now["u"].shape[1] - 2 * PAD) // 8)
        if n < count - 1:
            pairs = [(now[name], nats[n + 1][name]) for name in ("lat", "vert", "stor")]
            restrict_all(pairs + [(ress[n], nats[n + 1]["f"])], geos[n], geos[n + 1])
    pack_own(payload, nats[-1], ress[-1], layers, mine >> count, mine >> (count - 1))


def conjugate(s):
    fold, width, deep = s["geo"]
    n = s["u"].shape[1] - 2 * PAD
    here, after = slice(PAD, PAD + n), slice(PAD + 1, PAD + 1 + n)
    row = iota((n, LANES), 0)
    planes = range(deep)
    above = [jnp.where(row > 0, s["wr"][k, here], 0.0) for k in planes]
    below = [jnp.where(row < n - 1, s["wr"][k, after], 0.0) for k in planes]
    before, behind, diag, inv, r = [
        [s[name][k, here] for k in planes] for name in ("wc", "wcr", "diag", "invd", "f")
    ]
    faces = [s["wl"][k, here] if k or fold > 1 else None for k in planes]

    def apply(v):
        out = []
        for k in planes:
            total = above[k] * pltpu.roll(v[k], 1, 0) + below[k] * pltpu.roll(v[k], n - 1, 0)
            total += before[k] * pltpu.roll(v[k], 1, 1) + behind[k] * pltpu.roll(v[k], LANES - 1, 1)
            if k > 0:
                total += faces[k] * v[k - 1]
            elif fold > 1:
                total += faces[0] * pltpu.roll(v[deep - 1], width, 1)
            if k < deep - 1:
                total += faces[k + 1] * v[k + 1]
            elif fold > 1:
                total += pltpu.roll(faces[0] * v[0], LANES - width, 1)
            out.append(diag[k] * v[k] - total)
        return out

    def inner(a, b):
        total = a[0] * b[0]
        for x, y in zip(a[1:], b[1:]):
            total += x * y
        return jnp.sum(jnp.sum(total, axis=0, keepdims=True), axis=1, keepdims=True)

    def step(_, carry):
        e, r, p = carry[:deep], carry[deep : 2 * deep], carry[2 * deep :]
        q = apply(p)
        z = [x * y for x, y in zip(r, inv)]
        w = [x * y for x, y in zip(q, inv)]
        rz, pq, zq, wq = inner(r, z), inner(p, q), inner(z, q), inner(w, q)
        alpha = rz / pq
        beta = (rz + alpha * (alpha * wq - 2.0 * zq)) / rz
        e = [x + alpha * y for x, y in zip(e, p)]
        r = [x - alpha * y for x, y in zip(r, q)]
        p = [x - alpha * y + beta * d for x, y, d in zip(z, w, p)]
        return (*e, *r, *p)

    start = (*[jnp.zeros((n, LANES), F32)] * deep, *r, *[x * y for x, y in zip(r, inv)])
    out = lax.fori_loop(0, COARSE_ITERS, step, start)
    for k in planes:
        s["u"][k, here] = out[k]


WHOLE = ("u", "f", "invd", "wr", "wc", "wcr", "wl", "lat", "vert", "stor", "diag")


def up_kernel(*refs, halo, half, spans, geos, whole_geos):
    refs = list(refs)
    gathered = refs.pop(0)
    s = dict(zip(SPLIT_KEPT, refs[: len(SPLIT_KEPT)]))
    refs = refs[len(SPLIT_KEPT) :]
    nats = []
    for geo in geos:
        nats.append(dict(zip(NAT_KEPT, refs[: len(NAT_KEPT)]), geo=geo))
        refs = refs[len(NAT_KEPT) :]
    out = refs.pop(0)
    wholes = []
    for geo in whole_geos:
        wholes.append(dict(zip(WHOLE, refs[: len(WHOLE)]), geo=geo))
        refs = refs[len(WHOLE) :]
    ress = [refs.pop(0) for level in range(LOCAL, LEVELS)]
    fresh = [refs.pop(0) for level in range(LOCAL)]
    wider = refs.pop(0)
    nx, ny = spans
    layers = s["u"].shape[1]
    top = wholes[0]
    fold, width, deep = top["geo"]
    mine = 2 * half >> LOCAL
    group = 4 * mine
    per = LANES // group
    lane = iota((mine, LANES), 1)

    for whole in wholes:
        planes, height, _ = whole["u"].shape
        for name in ("u", "lat"):
            zeros = jnp.zeros((planes, PAD, LANES), F32)
            whole[name][:, :PAD] = zeros
            whole[name][:, height - PAD :] = zeros

    def gather(x):
        at = pl.ds(pl.multiple_of(x * mine, 8) + PAD, mine)
        parts = []
        for wide in range(-(-layers // per)):
            lines = slice(wide * mine, (wide + 1) * mine)
            turned = [gathered[x * ny + y, lines] for y in range(ny)]
            parts.append([pltpu.roll(v, y * mine, 1) if y else v for y, v in enumerate(turned)])
        for k in range(deep):
            for n, name in enumerate(("f", "lat", "vert", "stor")):
                value = None
                for g in range(fold):
                    layer = g * deep + k
                    base = (layer % per) * group + n * mine
                    total = jnp.zeros((mine, LANES), F32)
                    for y in range(ny):
                        spot = (base + y * mine) % LANES
                        hit = (lane >= spot) & (lane < spot + mine)
                        total = jnp.where(hit, parts[layer // per][y], total)
                    turn = (g * width - base) % LANES
                    total = pltpu.roll(total, turn, 1) if turn else total
                    value = total if value is None else value + total
                top[name][k, at] = value

    def gather_some(step, carry):
        for n in range(4):
            gather(jnp.minimum(4 * step + n, nx - 1))
        return carry

    lax.fori_loop(0, -(-nx // 4), gather_some, 0)

    for n, level in enumerate(range(LOCAL, LEVELS)):
        now, below = wholes[n], wholes[n + 1]
        nat_setup(now, 0.25**level)
        nat_down(now, ress[n], (now["u"].shape[1] - 2 * PAD) // 8)
        pairs = [(now[name], below[name]) for name in ("lat", "vert", "stor")]
        restrict_all(pairs + [(ress[n], below["f"])], now["geo"], below["geo"])
    nat_setup(wholes[-1], 0.25**LEVELS)
    conjugate(wholes[-1])

    def planes_of(ref):
        return lambda k: ref[k, PAD : ref.shape[1] - PAD]

    for n in reversed(range(len(wholes) - 1)):
        now, below = wholes[n], wholes[n + 1]
        prolong_into(now, now["u"], planes_of(below["u"]), below["geo"], False)
        nat_up(now, 0, (now["u"].shape[1] - 2 * PAD) // 8)

    x, y = lax.axis_index("gx"), lax.axis_index("gy")
    reach = (2 * half >> FIRST) >> (LOCAL - FIRST)
    height = top["u"].shape[1]
    need = (nats[-1]["u"].shape[1] - 2 * PAD) // 2
    lanes = iota((height, LANES), 1)
    for layer in range(layers):
        g, k = layer // deep, layer % deep
        value = top["u"][k]
        if g:
            value = pltpu.roll(value, LANES - g * width, 1)
        wider[layer, :height] = jnp.where(lanes < width, value, 0.0)
        wider[layer, height:] = jnp.zeros((PAD, LANES), F32)
    begin = PAD + x * mine - reach
    turn = lax.rem(LANES + reach - y * mine, LANES)

    def coarse(k):
        return pltpu.roll(wider[k, pl.ds(begin, need)], turn, 1)

    coarse_geo = (1, nats[-1]["geo"][1] // 2, layers)
    margins, above = [], 0
    for level in range(LOCAL):
        margins.append(above + 4)
        above = -(-margins[-1] // 2)
    for level in reversed(range(1, LOCAL)):
        now = dict(nats[level - 1])
        before = now["u"]
        now["u"] = fresh[level]
        planes, height, _ = before.shape
        now["u"][:, :PAD] = jnp.zeros((planes, PAD, LANES), F32)
        now["u"][:, height - PAD :] = jnp.zeros((planes, PAD, LANES), F32)
        prolong_into(now, before, coarse, coarse_geo, level == LOCAL - 1)
        own = 2 * half >> level
        side = halo >> level if level < FIRST else (2 * half >> FIRST) >> (level - FIRST)
        reach = margins[level]
        nat_up(now, (side - reach) // 8, min(-(-(side + own + reach) // 8), (height - 2 * PAD) // 8))
        coarse, coarse_geo = planes_of(now["u"]), now["geo"]
        if level == FIRST:
            assert coarse_geo[0] == 1
            skip, blocks = side - (halo >> FIRST), now["u"]

            def coarse(k):
                return pltpu.roll(
                    blocks[k, PAD + skip : blocks.shape[1] - PAD], LANES - skip, 1
                )

            coarse_geo = (1, (2 * half + 2 * halo) >> FIRST, layers)

    now = dict(s)
    now["u"] = fresh[0]
    hh = halo // 2
    lo, hi = (hh - 2) // 8, -(-(hh + half + 2) // 8)
    steps = (s["u"].shape[2] - 2 * PAD) // 8

    def add(t):
        for k in range(layers):
            value = fresh[1][k, rows(t)]
            for pj in range(4):
                now["u"][pj, k, rows(t)] = s["u"][pj, k, rows(t)] + value

    over(lo - 1, min(hi + 1, steps), MOST["add"], add)
    split_sweeps(now, lo, hi, layers)
    source, target = iota((2 * LANES, 2 * half), 0), iota((2 * LANES, 2 * half), 1)
    pick = ((source % LANES == hh + target // 2) & (source // LANES == target % 2)).astype(F32)
    body_rows = slice(PAD + hh, PAD + hh + half)
    spots = [(k, p) for k in range(layers) for p in range(2)]
    both = [
        jnp.concatenate([now["u"][2 * p + j, k, body_rows] for k, p in spots], 0) for j in range(2)
    ]
    every = pick_dot(jnp.concatenate(both, 1), pick)
    for n, (k, p) in enumerate(spots):
        out[k, pl.ds(p, half, stride=2), :] = every[n * half : (n + 1) * half]


def swap(values, axis, first):
    count = lax.axis_size(axis)
    pairs = [(i, i + 1) for i in range(first, count - 1, 2)]
    return lax.ppermute(values, axis, pairs + [(b, a) for a, b in pairs])


def shape(*dims):
    return jax.ShapeDtypeStruct(dims, F32)


def packed_shape(layers, mine):
    per = LANES // (4 * mine)
    return shape(-(-layers // per) * mine, LANES)


def other_scratch(shapes):
    out = []
    for d in shapes:
        out += [pltpu.VMEM(d, F32)] * len(NAT_OTHER)
    return out + [pltpu.VMEM(d, F32) for d in shapes]


def on_device(u0, sub, cat, planar, vertical, ratio, watt):
    nx, ny = lax.axis_size("gx"), lax.axis_size("gy")
    layers, height, width = u0.shape
    halo = halo_cells()
    half, hh = height // 2, halo // 2
    planes = 2 * layers + 1
    assert height == width == LANES and 2 * halo <= LANES and halo + half <= LANES

    own, a, b = pl.pallas_call(
        functools.partial(prep_kernel, halo=halo),
        out_shape=(shape(planes, height, width), shape(planes, halo, height), shape(planes, halo, height)),
        in_specs=[HBM] * 4,
        out_specs=(VMEM,) * 3,
        scratch_shapes=[
            pltpu.SMEM(watt.shape, F32),
            pltpu.VMEM(cat.shape, jnp.int32),
            pltpu.VMEM(sub.shape, jnp.int32),
            pltpu.SemaphoreType.DMA((4,)),
        ],
        compiler_params=limit(8),
        name="prep",
    )(*[pltpu.with_memory_space_constraint(x, pltpu.HBM) for x in (watt, cat, u0, sub)])
    a, b = swap(a, "gy", 0), swap(b, "gy", 1)

    lines = planes * 4 * hh
    sp, a, b = pl.pallas_call(
        functools.partial(split_kernel, halo=halo),
        out_shape=(shape(planes, 4, half, LANES), shape(lines, LANES), shape(lines, LANES)),
        in_specs=[VMEM] * 3,
        out_specs=(VMEM,) * 3,
        scratch_shapes=[pltpu.VMEM((2, 2, height, LANES), F32)],
        compiler_params=limit(20),
        name="split",
    )(own, a, b)
    a, b = swap(a, "gx", 0), swap(b, "gx", 1)

    tall = up8(half + 2 * hh) + 2 * PAD
    four, two = (4, layers, tall, LANES), (2, layers, tall, LANES)
    sides = [(height + 2 * halo) >> level for level in range(1, FIRST)]
    geos = [geometry(layers, side) for side in sides]
    assert geos[0][0] == 1
    nat_shapes = [(geo[2], up8(side) + 2 * PAD, LANES) for geo, side in zip(geos, sides)]
    sizes = [four if name in ("u", "f", "invd", "fl") else two for name in SPLIT_KEPT]
    sizes += [four] * 4 + [(4, tall, LANES)] + [nat_shapes[0]] * 3
    shared = pl.pallas_call(
        functools.partial(center_kernel, halo=halo, half=half, kinds=planar.shape[0]),
        out_shape=tuple(shape(*d) for d in sizes),
        in_specs=[SMEM] * 3 + [VMEM],
        out_specs=(VMEM,) * len(sizes),
        compiler_params=limit(24),
        name="center",
    )(planar, vertical, ratio, sp)
    kept = []
    for d in nat_shapes:
        kept += [shape(*d)] * len(NAT_KEPT)
    *saved, block = pl.pallas_call(
        functools.partial(
            down_kernel, halo=halo, half=half, kinds=planar.shape[0], geos=tuple(geos)
        ),
        out_shape=(*[shape(*d) for d in sizes], *kept, packed_shape(layers, height >> FIRST)),
        in_specs=[SMEM] * 3 + [VMEM] * (2 + len(sizes)),
        out_specs=(VMEM,) * (len(sizes) + len(kept) + 1),
        scratch_shapes=other_scratch(nat_shapes)[3:],
        input_output_aliases={5 + n: n for n in range(len(sizes))},
        compiler_params=limit(26),
        name="down",
    )(planar, vertical, ratio, a, b, *shared)
    saved = saved[: len(SPLIT_KEPT)] + saved[len(sizes) :]

    a, b = swap(block, "gy", 0), swap(block, "gy", 1)
    column = jnp.stack([block, a, b])
    above, below = swap(column, "gx", 0), swap(column, "gx", 1)
    mine = height >> FIRST
    assert 4 * mine <= LANES
    sides = [3 * mine >> n for n in range(LOCAL - FIRST)]
    block_geos = [geometry(layers, side) for side in sides]
    block_shapes = [(geo[2], up8(side) + 2 * PAD, LANES) for geo, side in zip(block_geos, sides)]
    kept = []
    for d in block_shapes:
        kept += [shape(*d)] * len(NAT_KEPT)
    *more, payload = pl.pallas_call(
        functools.partial(mid_kernel, geos=tuple(block_geos)),
        out_shape=(*kept, packed_shape(layers, height >> LOCAL)),
        in_specs=[VMEM] * 5,
        out_specs=(VMEM,) * (len(kept) + 1),
        scratch_shapes=other_scratch(block_shapes),
        compiler_params=limit(20),
        name="mid",
    )(block, a, b, above, below)
    saved += more
    nat_shapes += block_shapes

    sent = jnp.broadcast_to(payload[None], (nx * ny,) + payload.shape)
    gathered = lax.all_to_all(sent, ("gx", "gy"), 0, 0)

    whole_geos = [geometry(layers, ny * width >> level) for level in range(LOCAL, LEVELS + 1)]
    wholes = [
        (geo[2], up8(nx * height >> level) + 2 * PAD, LANES)
        for geo, level in zip(whole_geos, range(LOCAL, LEVELS + 1))
    ]
    scratch = []
    for d in wholes:
        scratch += [pltpu.VMEM(d, F32)] * len(WHOLE)
    scratch += [pltpu.VMEM(d, F32) for d in wholes[:-1]]
    scratch += [pltpu.VMEM(four, F32)] + [pltpu.VMEM(d, F32) for d in nat_shapes]
    scratch.append(pltpu.VMEM((layers, wholes[0][1] + PAD, LANES), F32))
    return pl.pallas_call(
        functools.partial(
            up_kernel,
            halo=halo,
            half=half,
            spans=(nx, ny),
            geos=tuple(geos + block_geos),
            whole_geos=tuple(whole_geos),
        ),
        out_shape=shape(layers, height, width),
        in_specs=[VMEM] * (1 + len(saved)),
        out_specs=VMEM,
        scratch_shapes=scratch,
        compiler_params=limit(16, scratch),
        name="up",
    )(gathered, *saved)


def solution(mesh):
    placed = (P(None, "gx", "gy"), P(None, "gx", "gy"), P("gx", "gy"), P(), P(), P(), P())
    return jax.shard_map(
        on_device, mesh=mesh, in_specs=placed, out_specs=P(None, "gx", "gy"), check_vma=False
    )
```

```python
import functools
import math

import jax
import jax.numpy as jnp
from jax import lax
from jax.experimental import pallas as pl
from jax.experimental.pallas import tpu as pltpu
from jax.sharding import PartitionSpec as P

TILE = 16
LEVELS = 6
FIRST = 2
LOCAL = 4
COARSE_ITERS = 12
LANES = 128
PAD = 8
MOST = dict(split=12, nat=12, first=12, residual=12, setup=12, look=1, faces=4, remain=12, add=12)
HI = lax.Precision.HIGHEST
F32 = jnp.float32
VMEM = pl.BlockSpec(memory_space=pltpu.VMEM)
SMEM = pl.BlockSpec(memory_space=pltpu.SMEM)
HBM = pl.BlockSpec(memory_space=pltpu.HBM)


def limit(mib, scratch=()):
    held = sum(4 * math.prod(ref.shape) for ref in scratch)
    return pltpu.CompilerParams(vmem_limit_bytes=mib * 1024 * 1024 + held + held // 4)


def up8(n):
    return -(-n // 8) * 8


def halo_cells():
    need, above = [], 0
    for level in range(FIRST):
        need.append(above + 4)
        above = -(-need[-1] // 2)
    f = 0
    for level in reversed(range(FIRST)):
        inner = max(need[level], 2 * f + 1)
        f = inner + (4 if level == 0 else 3)
    unit = 2**FIRST
    return -(-f // unit) * unit


def iota(shape, axis):
    return lax.broadcasted_iota(jnp.int32, shape, axis)


def rows(t, off=0):
    first, count = t
    start = first * 8 if isinstance(first, int) else pl.multiple_of(first * 8, 8)
    return pl.ds(start + (PAD + off), 8 * count)


def over(lo, hi, most, body):
    steps = -(-(hi - lo) // most)
    size = -(-(hi - lo) // steps)
    if steps == 1:
        body((lo, size))
        return

    def step(i, carry):
        body((jnp.minimum(lo + i * size, hi - size), size))
        return carry

    lax.fori_loop(0, steps, step, 0)


def dot(a, b):
    return jnp.dot(a, b, precision=HI, preferred_element_type=F32)


def pick_dot(x, pick, pieces=3):
    pick = pick.astype(jnp.bfloat16)
    total = None
    for n in range(pieces):
        piece = x.astype(jnp.bfloat16)
        part = jnp.dot(piece, pick, preferred_element_type=F32)
        total = part if total is None else total + part
        if n < pieces - 1:
            x = x - piece.astype(F32)
    return total


def prep_kernel(watt_hbm, cat_hbm, u_hbm, sub_hbm, planes, a_ref, b_ref, watt, cat_ref, sub_ref, sems, *, halo):
    layers, height, width = u_hbm.shape
    copies = [
        pltpu.make_async_copy(source, target, sems.at[n])
        for n, (source, target) in enumerate(
            ((u_hbm, planes.at[pl.ds(0, layers)]), (sub_hbm, sub_ref), (cat_hbm, cat_ref), (watt_hbm, watt))
        )
    ]
    for copy in copies:
        copy.start()
    even = lax.axis_index("gy") % 2 == 0

    def send(q):
        turned = planes[q].T
        low, high = turned[:halo], turned[width - halo :]
        a_ref[q] = jnp.where(even, high, low)
        b_ref[q] = jnp.where(even, low, high)

    for copy in copies:
        copy.wait()
    cat = cat_ref[...]
    power = jnp.zeros(cat.shape, F32)
    for n in range(watt.shape[0]):
        power = power + jnp.where(cat == n, watt[n], 0.0)
    spread_r = (iota((height, cat.shape[0]), 0) // TILE == iota((height, cat.shape[0]), 1)).astype(F32)
    spread_c = (iota((cat.shape[1], width), 1) // TILE == iota((cat.shape[1], width), 0)).astype(F32)
    planes[2 * layers] = dot(dot(spread_r, power), spread_c)
    for q in range(2 * layers + 1):
        if layers <= q < 2 * layers:
            planes[q] = (sub_ref[q - layers] + 1).astype(F32)
        send(q)


def split_kernel(own, ra, rb, out, a_ref, b_ref, scr, *, halo):
    count, height, width = own.shape
    layers = count // 2
    even_y, even_x = lax.axis_index("gy") % 2 == 0, lax.axis_index("gx") % 2 == 0
    half, hh = height // 2, halo // 2
    source, target = iota((width + LANES, 2 * LANES), 0), iota((width + LANES, 2 * LANES), 1)
    cell = 2 * (target % LANES) + target // LANES
    want = jnp.where(
        cell < halo, width + cell, jnp.where(cell < halo + width, cell - halo, cell)
    )
    pick = ((source == want) & (cell < 2 * halo + width)).astype(F32)
    planes = []
    for q in range(count):
        left = jnp.where(even_y, rb[q], ra[q])
        right = jnp.where(even_y, ra[q], rb[q])
        sides = jnp.concatenate([left, right, jnp.zeros((LANES - 2 * halo, height), F32)], 0).T
        planes.append(jnp.concatenate([own[q], sides], 1))
    first = pick_dot(jnp.concatenate(planes[:layers] + planes[2 * layers :], 0), pick)
    second = pick_dot(jnp.concatenate(planes[layers : 2 * layers], 0), pick, 1)
    for q in range(2 * layers + 1):
        if layers <= q < 2 * layers:
            both = second[(q - layers) * height : (q - layers + 1) * height]
        else:
            at = q if q < layers else layers
            both = first[at * height : (at + 1) * height]
        scr[q % 2, 0] = both[:, :LANES]
        scr[q % 2, 1] = both[:, LANES:]
        for p in range(2):
            for j in range(2):
                z = scr[q % 2, j, pl.ds(p, half, stride=2), :]
                out[q, 2 * p + j] = z
                at = (4 * q + 2 * p + j) * hh
                first_rows, last_rows = z[:hh], z[half - hh :]
                a_ref[at : at + hh] = jnp.where(even_x, last_rows, first_rows)
                b_ref[at : at + hh] = jnp.where(even_x, first_rows, last_rows)


def split_block(s, colour, t, layers):
    u, at = s["u"], rows(t)
    other = {
        (p, j, k): u[2 * p + j, k, at]
        for k in range(layers)
        for p in range(2)
        for j in range(2)
        if (p + j + k) % 2 != colour
    }
    for k in range(layers):
        for p in range(2):
            for j in range(2):
                if (p + j + k) % 2 != colour:
                    continue
                pj = 2 * p + j
                total = s["f"][pj, k, at] + s["fri"][j, k, at] * other[1 - p, j, k]
                if p == 0:
                    total += s["fro"][j, k, at] * u[2 + j, k, rows(t, -1)]
                else:
                    total += s["fro"][j, k, rows(t, 1)] * u[j, k, rows(t, 1)]
                beside = other[p, 1 - j, k]
                total += s["fci"][p, k, at] * beside
                if j == 0:
                    total += s["fco"][p, k, at] * pltpu.roll(beside, 1, 1)
                else:
                    total += s["fcr"][p, k, at] * pltpu.roll(beside, LANES - 1, 1)
                if k > 0:
                    total += s["fl"][pj, k, at] * other[p, j, k - 1]
                if k < layers - 1:
                    total += s["fl"][pj, k + 1, at] * other[p, j, k + 1]
                yield pj, k, total


def split_half(s, colour, lo, hi, layers):
    def body(t):
        for pj, k, total in split_block(s, colour, t, layers):
            s["u"][pj, k, rows(t)] = total * s["invd"][pj, k, rows(t)]

    over(lo, hi, MOST["split"], body)


def split_sweeps(s, lo, hi, layers):
    for sweep in range(2):
        split_half(s, 0, lo, hi, layers)
        split_half(s, 1, lo, hi, layers)


def geometry(layers, width):
    assert width <= LANES
    fold = max(f for f in range(1, layers + 1) if layers % f == 0 and f * width <= LANES)
    return fold, width, layers // fold


def places(extent, geo):
    lane = iota(extent, 1)
    group = jnp.zeros(extent, jnp.int32)
    for g in range(1, geo[0] + 1):
        if g * geo[1] < LANES:
            group = group + (lane >= g * geo[1]).astype(jnp.int32)
    return group, lane - group * geo[1]


def odd_cells(t, geo):
    extent = (8 * t[1], LANES)
    group, col = places(extent, geo)
    return (iota(extent, 0) + col + group * geo[2]) % 2


def nat_setup(s, factor):
    fold, width, deep = s["geo"]
    height = s["lat"].shape[1]
    c = 0.5 * factor

    def body(t):
        at = rows(t)
        group, col = places((8 * t[1], LANES), s["geo"])
        first, last = col == 0, col == width - 1
        between = None
        for k in range(deep):
            lat, stor, vert = s["lat"][k, at], s["stor"][k, at], s["vert"][k, at]
            above = c * (lat + s["lat"][k, rows(t, -1)])
            below = c * (lat + s["lat"][k, rows(t, 1)])
            before = c * (lat + jnp.where(first, 0.0, pltpu.roll(lat, 1, 1)))
            after = c * (lat + jnp.where(last, 0.0, pltpu.roll(lat, LANES - 1, 1)))
            diag = stor + above + below + before + after
            if k > 0:
                face = 0.5 * (vert + s["vert"][k - 1, at])
                s["wl"][k, at] = face
                diag += face
            elif fold > 1:
                between = 0.5 * (vert + pltpu.roll(s["vert"][deep - 1, at], width, 1))
                between = jnp.where((group > 0) & (group < fold), between, 0.0)
                s["wl"][0, at] = between
                diag += between
            if k < deep - 1:
                diag += 0.5 * (vert + s["vert"][k + 1, at])
            elif fold > 1:
                diag += pltpu.roll(between, LANES - width, 1)
            inside = stor > 0.0
            s["wr"][k, at] = above
            s["wc"][k, at] = jnp.where(first, 0.0, before)
            s["wcr"][k, at] = jnp.where(last, 0.0, after)
            s["diag"][k, at] = diag
            s["invd"][k, at] = jnp.where(inside, 1.0 / jnp.where(inside, diag, 1.0), 0.0)

    s["wr"][:, height - PAD :] = jnp.zeros((deep, PAD, LANES), F32)
    over(0, (height - 2 * PAD) // 8, MOST["setup"], body)


def nat_block(s, t):
    u, at = s["u"], rows(t)
    fold, width, deep = s["geo"]
    mid = [u[k, at] for k in range(deep)]
    wl = s["wl"][0, at] if fold > 1 else None
    between = None if wl is None else pltpu.roll(wl * mid[0], LANES - width, 1)
    for k in range(deep):
        total = s["f"][k, at] + s["wr"][k, at] * u[k, rows(t, -1)]
        total += s["wr"][k, rows(t, 1)] * u[k, rows(t, 1)]
        beside = s["wc"][k, at] * pltpu.roll(mid[k], 1, 1)
        beside += s["wcr"][k, at] * pltpu.roll(mid[k], LANES - 1, 1)
        if k > 0:
            total += wl * mid[k - 1]
        elif fold > 1:
            total += wl * pltpu.roll(mid[deep - 1], width, 1)
        if k < deep - 1:
            wl = s["wl"][k + 1, at]
            total += wl * mid[k + 1]
        elif fold > 1:
            total += between
        yield k, total + beside, mid[k]


def nat_half(s, colour, lo, hi):
    def body(t):
        odd = odd_cells(t, s["geo"])
        for k, total, old in nat_block(s, t):
            value = total * s["invd"][k, rows(t)]
            s["u"][k, rows(t)] = jnp.where(odd == (colour + k) % 2, value, old)

    over(lo, hi, MOST["nat"], body)


def nat_first(s, lo, hi):
    deep, height, _ = s["u"].shape
    zeros = jnp.zeros((deep, PAD, LANES), F32)
    s["u"][:, :PAD] = zeros
    s["u"][:, height - PAD :] = zeros

    def body(t):
        odd = odd_cells(t, s["geo"])
        for k in range(deep):
            value = s["f"][k, rows(t)] * s["invd"][k, rows(t)]
            s["u"][k, rows(t)] = jnp.where(odd == k % 2, value, 0.0)

    over(lo, hi, MOST["first"], body)


def nat_residual(s, res, lo, hi):
    def body(t):
        for k, total, old in nat_block(s, t):
            res[k, rows(t)] = total - s["diag"][k, rows(t)] * old

    over(lo, hi, MOST["residual"], body)


def nat_down(s, res, steps):
    nat_first(s, 0, steps)
    for colour in (1, 0, 1):
        nat_half(s, colour, 0, steps)
    nat_residual(s, res, 0, steps)


def move(parts, a, b, relation, scale):
    jobs = {}
    for ka in range(a[2]):
        for kb in range(b[2]):
            key = tuple(
                (ga, gb)
                for ga in range(a[0])
                for gb in range(b[0])
                if ga * a[2] + ka == gb * b[2] + kb
            )
            if key:
                jobs.setdefault(key, []).append((ka, kb))
    c, m = iota((LANES, LANES), 0), iota((LANES, LANES), 1)
    out = [None] * b[2]
    count = parts[0].shape[0]
    for key, members in jobs.items():
        hit = None
        for ga, gb in key:
            ca, mb = c - ga * a[1], m - gb * b[1]
            here = (ca >= 0) & (ca < a[1]) & (mb >= 0) & (mb < b[1]) & relation(ca, mb)
            hit = here if hit is None else hit | here
        moved = pick_dot(
            jnp.concatenate([parts[ka] for ka, _ in members], 0), jnp.where(hit, scale, 0.0), 2
        )
        for n, (_, kb) in enumerate(members):
            part = moved[n * count : (n + 1) * count]
            out[kb] = part if out[kb] is None else out[kb] + part
    return out


def pair_rows(ref, k, start, count):
    part = ref[k, pl.ds(start, count, stride=2), :]
    return part + ref[k, pl.ds(start + 1, count, stride=2), :]


def restrict_all(pairs, a, b):
    deep, height = pairs[0][1].shape[0], pairs[0][1].shape[1] - 2 * PAD
    zeros = jnp.zeros((deep, PAD, LANES), F32)
    for _, target in pairs:
        target[:, :PAD] = zeros
        target[:, PAD + height :] = zeros
    parts = [
        jnp.concatenate([pair_rows(source, k, PAD, height) for source, _ in pairs], 0)
        for k in range(a[2])
    ]
    out = move(parts, a, b, lambda c, m: c // 2 == m, 0.25)
    for n, (_, target) in enumerate(pairs):
        for k in range(deep):
            target[k, PAD : PAD + height] = out[k][n * height : (n + 1) * height]


def prolong_into(s, u_in, coarse, geo, mask):
    deep, height, _ = s["u"].shape
    n = (height - 2 * PAD) // 2
    tall = up8(n)
    parts = [coarse(k)[:tall] for k in range(geo[2])]
    out = move(parts, geo, s["geo"], lambda c, m: c == m // 2, 1.0)
    for k in range(deep):
        wide = out[k][:n]
        for p in range(2):
            at = pl.ds(PAD + p, n, stride=2)
            add = wide
            if mask:
                add = jnp.where(s["invd"][k, at, :] > 0.0, wide, 0.0)
            s["u"][k, at, :] = u_in[k, at, :] + add


def nat_up(s, lo, hi):
    for sweep in range(2):
        nat_half(s, 0, lo, hi)
        nat_half(s, 1, lo, hi)


SPLIT_KEPT = ("u", "f", "invd", "fri", "fro", "fci", "fco", "fcr", "fl")
NAT_KEPT = ("u", "f", "invd", "wr", "wc", "wcr", "wl")
NAT_OTHER = ("lat", "vert", "stor", "diag")


def pack_own(payload, last, res, layers, mine, off):
    group = 4 * mine
    per = LANES // group
    quantities = (res, last["lat"], last["vert"], last["stor"])
    parts = [
        jnp.concatenate([pair_rows(ref, k, PAD + off, mine) for ref in quantities], 0)
        for k in range(last["geo"][2])
    ]
    packed = move(
        parts, last["geo"], (1, mine, layers), lambda c, m: (c >= off) & ((c - off) // 2 == m), 0.25
    )
    for wide in range(-(-layers // per)):
        total = jnp.zeros((mine, LANES), F32)
        for n in range(wide * per * 4, min(layers, (wide + 1) * per) * 4):
            part = packed[n // 4][n % 4 * mine : (n % 4 + 1) * mine]
            base = (n - wide * per * 4) * mine
            total += pltpu.roll(part, base, 1) if base else part
        payload[wide * mine : (wide + 1) * mine] = total


def look_up(s, first, heat, kinds, lo, hi):
    layers = s["u"].shape[1]

    def look(t):
        for k in range(layers):
            sums = [None, None, None]
            for pj in range(4):
                at = (pj, k, rows(t))
                label = s["diag"][at]
                value = [jnp.zeros_like(label)] * 3
                for n in range(kinds):
                    hit = label == float(n + 1)
                    value = [jnp.where(hit, s["table"][i * kinds + n], value[i]) for i in range(3)]
                for i, name in enumerate(("lat", "vert", "stor")):
                    s[name][at] = value[i]
                    sums[i] = value[i] if sums[i] is None else sums[i] + value[i]
                f = value[2] * s["u"][at]
                if k == 0:
                    f = f + heat[pj, rows(t)]
                s["f"][at] = f
            for i, name in enumerate(("lat", "vert", "stor")):
                first[name][k, rows(t)] = sums[i] * 0.25

    over(lo, hi, MOST["look"], look)


def split_setup(s, lo, hi):
    layers = s["u"].shape[1]

    def faces(t):
        at = rows(t)
        for k in range(layers):
            lat = [s["lat"][pj, k, at] for pj in range(4)]
            inner_r = [0.5 * (lat[j] + lat[2 + j]) for j in range(2)]
            before_r = [0.5 * (s["lat"][2 + j, k, rows(t, -1)] + lat[j]) for j in range(2)]
            after_r = [0.5 * (lat[2 + j] + s["lat"][j, k, rows(t, 1)]) for j in range(2)]
            inner_c = [0.5 * (lat[2 * p] + lat[2 * p + 1]) for p in range(2)]
            before_c = [0.5 * (pltpu.roll(lat[2 * p + 1], 1, 1) + lat[2 * p]) for p in range(2)]
            after_c = [0.5 * (lat[2 * p + 1] + pltpu.roll(lat[2 * p], LANES - 1, 1)) for p in range(2)]
            for x in range(2):
                s["fri"][x, k, at] = inner_r[x]
                s["fro"][x, k, at] = before_r[x]
                s["fci"][x, k, at] = inner_c[x]
                s["fco"][x, k, at] = before_c[x]
                s["fcr"][x, k, at] = after_c[x]
            for p in range(2):
                for j in range(2):
                    pj = 2 * p + j
                    stor = s["stor"][pj, k, at]
                    diag = stor + inner_r[j] + (after_r[j] if p else before_r[j])
                    diag += inner_c[p] + (after_c[p] if j else before_c[p])
                    vert = s["vert"][pj, k, at]
                    if k > 0:
                        face = 0.5 * (vert + s["vert"][pj, k - 1, at])
                        s["fl"][pj, k, at] = face
                        diag += face
                    if k < layers - 1:
                        diag += 0.5 * (vert + s["vert"][pj, k + 1, at])
                    inside = stor > 0.0
                    s["invd"][pj, k, at] = jnp.where(inside, 1.0 / jnp.where(inside, diag, 1.0), 0.0)
                    s["diag"][pj, k, at] = diag

    over(lo, hi, MOST["faces"], faces)


SHARED = SPLIT_KEPT + ("lat", "vert", "stor", "diag", "heat", "lat1", "vert1", "stor1", "table")


def center_kernel(*refs, halo, half, kinds):
    tables, sp, out = refs[:3], refs[3], refs[4:]
    s = dict(zip(SHARED, out))
    first = {name: s[name + "1"] for name in ("lat", "vert", "stor")}
    layers, height, hh = s["u"].shape[1], s["u"].shape[2], halo // 2
    body_rows = slice(PAD + hh, PAD + hh + half)
    zeros = jnp.zeros((PAD, LANES), F32)
    for pj in range(4):
        for k in range(layers):
            for name in ("u", "lat"):
                s[name][pj, k, :PAD] = zeros
                s[name][pj, k, height - PAD :] = zeros
            s["u"][pj, k, body_rows] = sp[k, pj]
            s["diag"][pj, k, body_rows] = sp[layers + k, pj]
        s["heat"][pj, body_rows] = sp[2 * layers, pj]
    for ref in first.values():
        for k in range(layers):
            ref[k, :PAD] = zeros
            ref[k, height - PAD :] = zeros
    for i in range(3):
        for n in range(kinds):
            s["table"][i * kinds + n] = jnp.full((8, LANES), tables[i][n], F32)
    look_up(s, first, s["heat"], kinds, *bounds(hh, half, 0))
    split_setup(s, *bounds(hh, half, 1))


def bounds(hh, half, inner):
    if inner:
        return -(-(hh + 1) // 8), (hh + half - 1) // 8
    return hh // 8, -(-(hh + half) // 8)


def down_kernel(*refs, halo, half, kinds, geos):
    ra, rb = refs[:2]
    refs = list(refs[2 + len(SHARED) :])
    s = dict(zip(SHARED, refs[: len(SHARED)]))
    refs = refs[len(SHARED) :]
    nats = [{} for level in range(1, FIRST)]
    for n, now in enumerate(nats):
        now.update(zip(NAT_KEPT, refs[: len(NAT_KEPT)]), geo=geos[n])
        refs = refs[len(NAT_KEPT) :]
    payload = refs.pop(0)
    heat = s["heat"]
    for n, now in enumerate(nats):
        for name in NAT_OTHER:
            now[name] = s[name + "1"] if n == 0 and name != "diag" else refs.pop(0)
    ress = [refs.pop(0) for level in range(1, FIRST)]
    layers = s["u"].shape[1]
    height = s["u"].shape[2]
    hh = halo // 2
    steps = (height - 2 * PAD) // 8
    even = lax.axis_index("gx") % 2 == 0
    zeros = jnp.zeros((PAD, LANES), F32)

    def place(ref, index, q, pj):
        at = (4 * q + pj) * hh
        first, second = ra[at : at + hh], rb[at : at + hh]
        ref[index + (slice(PAD, PAD + hh),)] = jnp.where(even, second, first)
        ref[index + (slice(PAD + hh + half, PAD + 2 * hh + half),)] = jnp.where(even, first, second)

    for pj in range(4):
        for k in range(layers):
            place(s["u"], (pj, k), k, pj)
            place(s["diag"], (pj, k), layers + k, pj)
        place(heat, (pj,), 2 * layers, pj)
    for j in range(2):
        for k in range(layers):
            s["fro"][j, k, height - PAD :] = zeros
    first = nats[0]
    for ref in [first["f"]] + ress:
        for k in range(ref.shape[0]):
            ref[k, :PAD] = zeros
            ref[k, ref.shape[1] - PAD :] = zeros
    lo, hi = bounds(hh, half, 1)
    for begin, end in ((0, lo), (hi, steps)):
        look_up(s, first, heat, kinds, begin, end)
    for begin, end in ((0, lo), (hi, steps)):
        split_setup(s, begin, end)
    split_sweeps(s, 0, steps, layers)

    def remain(t):
        sums = {}
        for pj, k, total in split_block(s, 0, t, layers):
            r = total - s["diag"][pj, k, rows(t)] * s["u"][pj, k, rows(t)]
            sums[k] = sums[k] + r if k in sums else r
            if pj >= 2:
                first["f"][k, rows(t)] = sums[k] * 0.25

    over(0, steps, MOST["remain"], remain)

    for level in range(1, FIRST):
        now = nats[level - 1]
        nat_setup(now, 0.25**level)
        count = (now["u"].shape[1] - 2 * PAD) // 8
        nat_down(now, ress[level - 1], count)
        if level < FIRST - 1:
            below = nats[level]
            pairs = [(now[name], below[name]) for name in ("lat", "vert", "stor")]
            restrict_all(pairs + [(ress[level - 1], below["f"])], now["geo"], below["geo"])

    pack_own(payload, nats[-1], ress[-1], layers, 2 * half >> FIRST, halo >> (FIRST - 1))


def mid_kernel(own, ra, rb, ta, tb, *refs, geos):
    refs = list(refs)
    count = LOCAL - FIRST
    nats = []
    for n in range(count):
        nats.append(dict(zip(NAT_KEPT, refs[: len(NAT_KEPT)]), geo=geos[n]))
        refs = refs[len(NAT_KEPT) :]
    payload = refs.pop(0)
    for n in range(count):
        for name in NAT_OTHER:
            nats[n][name] = refs.pop(0)
    ress = refs
    layers = geos[0][0] * geos[0][2]
    mine = own.shape[0] // layers
    assert geos[0][0] == 1
    even_y, even_x = lax.axis_index("gy") % 2 == 0, lax.axis_index("gx") % 2 == 0
    zeros = jnp.zeros((PAD, LANES), F32)
    for now, res in zip(nats, ress):
        for ref in [now[name] for name in ("lat", "vert", "stor", "f")] + [res]:
            for k in range(ref.shape[0]):
                ref[k, :PAD] = zeros
                ref[k, ref.shape[1] - PAD :] = zeros
    group = iota((mine, LANES), 1) // mine

    def assemble(v, middle_of, a_of, b_of):
        for k in range(layers):
            lines = slice(k * mine, (k + 1) * mine)
            middle, a, b = middle_of(lines), a_of(lines), b_of(lines)
            left, right = jnp.where(even_y, b, a), jnp.where(even_y, a, b)
            middle, right = pltpu.roll(middle, mine, 1), pltpu.roll(right, 2 * mine, 1)
            for n, name in enumerate(("f", "lat", "vert", "stor")):
                value = jnp.where(group == (n + 1) % 4, middle, right)
                value = jnp.where(group == n, left, value)
                value = jnp.where(group == (n + 3) % 4, 0.0, value)
                if n:
                    value = pltpu.roll(value, LANES - n * mine, 1)
                nats[0][name][k, PAD + v * mine : PAD + (v + 1) * mine] = value

    def rows_from(ref):
        return [lambda lines, n=n: ref[n, lines] for n in range(3)]

    def outer(above, below):
        assemble(0, *rows_from(above))
        assemble(2, *rows_from(below))

    assemble(1, *[lambda lines, ref=ref: ref[lines] for ref in (own, ra, rb)])
    pl.when(even_x)(lambda: outer(tb, ta))
    pl.when(jnp.logical_not(even_x))(lambda: outer(ta, tb))
    for n, level in enumerate(range(FIRST, LOCAL)):
        now = nats[n]
        nat_setup(now, 0.25**level)
        nat_down(now, ress[n], (now["u"].shape[1] - 2 * PAD) // 8)
        if n < count - 1:
            pairs = [(now[name], nats[n + 1][name]) for name in ("lat", "vert", "stor")]
            restrict_all(pairs + [(ress[n], nats[n + 1]["f"])], geos[n], geos[n + 1])
    pack_own(payload, nats[-1], ress[-1], layers, mine >> count, mine >> (count - 1))


def conjugate(s):
    fold, width, deep = s["geo"]
    n = s["u"].shape[1] - 2 * PAD
    here, after = slice(PAD, PAD + n), slice(PAD + 1, PAD + 1 + n)
    row = iota((n, LANES), 0)
    planes = range(deep)
    above = [jnp.where(row > 0, s["wr"][k, here], 0.0) for k in planes]
    below = [jnp.where(row < n - 1, s["wr"][k, after], 0.0) for k in planes]
    before, behind, diag, inv, r = [
        [s[name][k, here] for k in planes] for name in ("wc", "wcr", "diag", "invd", "f")
    ]
    faces = [s["wl"][k, here] if k or fold > 1 else None for k in planes]

    def apply(v):
        out = []
        for k in planes:
            total = above[k] * pltpu.roll(v[k], 1, 0) + below[k] * pltpu.roll(v[k], n - 1, 0)
            total += before[k] * pltpu.roll(v[k], 1, 1) + behind[k] * pltpu.roll(v[k], LANES - 1, 1)
            if k > 0:
                total += faces[k] * v[k - 1]
            elif fold > 1:
                total += faces[0] * pltpu.roll(v[deep - 1], width, 1)
            if k < deep - 1:
                total += faces[k + 1] * v[k + 1]
            elif fold > 1:
                total += pltpu.roll(faces[0] * v[0], LANES - width, 1)
            out.append(diag[k] * v[k] - total)
        return out

    def inner(a, b):
        total = a[0] * b[0]
        for x, y in zip(a[1:], b[1:]):
            total += x * y
        return jnp.sum(jnp.sum(total, axis=0, keepdims=True), axis=1, keepdims=True)

    def step(_, carry):
        e, r, p = carry[:deep], carry[deep : 2 * deep], carry[2 * deep :]
        q = apply(p)
        z = [x * y for x, y in zip(r, inv)]
        w = [x * y for x, y in zip(q, inv)]
        rz, pq, zq, wq = inner(r, z), inner(p, q), inner(z, q), inner(w, q)
        alpha = rz / pq
        beta = (rz + alpha * (alpha * wq - 2.0 * zq)) / rz
        e = [x + alpha * y for x, y in zip(e, p)]
        r = [x - alpha * y for x, y in zip(r, q)]
        p = [x - alpha * y + beta * d for x, y, d in zip(z, w, p)]
        return (*e, *r, *p)

    start = (*[jnp.zeros((n, LANES), F32)] * deep, *r, *[x * y for x, y in zip(r, inv)])
    out = lax.fori_loop(0, COARSE_ITERS, step, start)
    for k in planes:
        s["u"][k, here] = out[k]


WHOLE = ("u", "f", "invd", "wr", "wc", "wcr", "wl", "lat", "vert", "stor", "diag")


def up_kernel(*refs, halo, half, spans, geos, whole_geos):
    refs = list(refs)
    gathered = refs.pop(0)
    s = dict(zip(SPLIT_KEPT, refs[: len(SPLIT_KEPT)]))
    refs = refs[len(SPLIT_KEPT) :]
    nats = []
    for geo in geos:
        nats.append(dict(zip(NAT_KEPT, refs[: len(NAT_KEPT)]), geo=geo))
        refs = refs[len(NAT_KEPT) :]
    out = refs.pop(0)
    wholes = []
    for geo in whole_geos:
        wholes.append(dict(zip(WHOLE, refs[: len(WHOLE)]), geo=geo))
        refs = refs[len(WHOLE) :]
    ress = [refs.pop(0) for level in range(LOCAL, LEVELS)]
    fresh = [refs.pop(0) for level in range(LOCAL)]
    wider = refs.pop(0)
    nx, ny = spans
    layers = s["u"].shape[1]
    top = wholes[0]
    fold, width, deep = top["geo"]
    mine = 2 * half >> LOCAL
    group = 4 * mine
    per = LANES // group
    lane = iota((mine, LANES), 1)

    for whole in wholes:
        planes, height, _ = whole["u"].shape
        for name in ("u", "lat"):
            zeros = jnp.zeros((planes, PAD, LANES), F32)
            whole[name][:, :PAD] = zeros
            whole[name][:, height - PAD :] = zeros

    def gather(x):
        at = pl.ds(pl.multiple_of(x * mine, 8) + PAD, mine)
        parts = []
        for wide in range(-(-layers // per)):
            lines = slice(wide * mine, (wide + 1) * mine)
            turned = [gathered[x * ny + y, lines] for y in range(ny)]
            parts.append([pltpu.roll(v, y * mine, 1) if y else v for y, v in enumerate(turned)])
        for k in range(deep):
            for n, name in enumerate(("f", "lat", "vert", "stor")):
                value = None
                for g in range(fold):
                    layer = g * deep + k
                    base = (layer % per) * group + n * mine
                    total = jnp.zeros((mine, LANES), F32)
                    for y in range(ny):
                        spot = (base + y * mine) % LANES
                        hit = (lane >= spot) & (lane < spot + mine)
                        total = jnp.where(hit, parts[layer // per][y], total)
                    turn = (g * width - base) % LANES
                    total = pltpu.roll(total, turn, 1) if turn else total
                    value = total if value is None else value + total
                top[name][k, at] = value

    def gather_some(step, carry):
        for n in range(4):
            gather(jnp.minimum(4 * step + n, nx - 1))
        return carry

    lax.fori_loop(0, -(-nx // 4), gather_some, 0)

    for n, level in enumerate(range(LOCAL, LEVELS)):
        now, below = wholes[n], wholes[n + 1]
        nat_setup(now, 0.25**level)
        nat_down(now, ress[n], (now["u"].shape[1] - 2 * PAD) // 8)
        pairs = [(now[name], below[name]) for name in ("lat", "vert", "stor")]
        restrict_all(pairs + [(ress[n], below["f"])], now["geo"], below["geo"])
    nat_setup(wholes[-1], 0.25**LEVELS)
    conjugate(wholes[-1])

    def planes_of(ref):
        return lambda k: ref[k, PAD : ref.shape[1] - PAD]

    for n in reversed(range(len(wholes) - 1)):
        now, below = wholes[n], wholes[n + 1]
        prolong_into(now, now["u"], planes_of(below["u"]), below["geo"], False)
        nat_up(now, 0, (now["u"].shape[1] - 2 * PAD) // 8)

    x, y = lax.axis_index("gx"), lax.axis_index("gy")
    reach = (2 * half >> FIRST) >> (LOCAL - FIRST)
    height = top["u"].shape[1]
    need = (nats[-1]["u"].shape[1] - 2 * PAD) // 2
    lanes = iota((height, LANES), 1)
    for layer in range(layers):
        g, k = layer // deep, layer % deep
        value = top["u"][k]
        if g:
            value = pltpu.roll(value, LANES - g * width, 1)
        wider[layer, :height] = jnp.where(lanes < width, value, 0.0)
        wider[layer, height:] = jnp.zeros((PAD, LANES), F32)
    begin = PAD + x * mine - reach
    turn = lax.rem(LANES + reach - y * mine, LANES)

    def coarse(k):
        return pltpu.roll(wider[k, pl.ds(begin, need)], turn, 1)

    coarse_geo = (1, nats[-1]["geo"][1] // 2, layers)
    margins, above = [], 0
    for level in range(LOCAL):
        margins.append(above + 4)
        above = -(-margins[-1] // 2)
    for level in reversed(range(1, LOCAL)):
        now = dict(nats[level - 1])
        before = now["u"]
        now["u"] = fresh[level]
        planes, height, _ = before.shape
        now["u"][:, :PAD] = jnp.zeros((planes, PAD, LANES), F32)
        now["u"][:, height - PAD :] = jnp.zeros((planes, PAD, LANES), F32)
        prolong_into(now, before, coarse, coarse_geo, level == LOCAL - 1)
        own = 2 * half >> level
        side = halo >> level if level < FIRST else (2 * half >> FIRST) >> (level - FIRST)
        reach = margins[level]
        nat_up(now, (side - reach) // 8, min(-(-(side + own + reach) // 8), (height - 2 * PAD) // 8))
        coarse, coarse_geo = planes_of(now["u"]), now["geo"]
        if level == FIRST:
            assert coarse_geo[0] == 1
            skip, blocks = side - (halo >> FIRST), now["u"]

            def coarse(k):
                return pltpu.roll(
                    blocks[k, PAD + skip : blocks.shape[1] - PAD], LANES - skip, 1
                )

            coarse_geo = (1, (2 * half + 2 * halo) >> FIRST, layers)

    now = dict(s)
    now["u"] = fresh[0]
    hh = halo // 2
    lo, hi = (hh - 2) // 8, -(-(hh + half + 2) // 8)
    steps = (s["u"].shape[2] - 2 * PAD) // 8

    def add(t):
        for k in range(layers):
            value = fresh[1][k, rows(t)]
            for pj in range(4):
                now["u"][pj, k, rows(t)] = s["u"][pj, k, rows(t)] + value

    over(lo - 1, min(hi + 1, steps), MOST["add"], add)
    split_sweeps(now, lo, hi, layers)
    source, target = iota((2 * LANES, 2 * half), 0), iota((2 * LANES, 2 * half), 1)
    pick = ((source % LANES == hh + target // 2) & (source // LANES == target % 2)).astype(F32)
    body_rows = slice(PAD + hh, PAD + hh + half)
    spots = [(k, p) for k in range(layers) for p in range(2)]
    both = [
        jnp.concatenate([now["u"][2 * p + j, k, body_rows] for k, p in spots], 0) for j in range(2)
    ]
    every = pick_dot(jnp.concatenate(both, 1), pick)
    for n, (k, p) in enumerate(spots):
        out[k, pl.ds(p, half, stride=2), :] = every[n * half : (n + 1) * half]


def swap(values, axis, first):
    count = lax.axis_size(axis)
    pairs = [(i, i + 1) for i in range(first, count - 1, 2)]
    return lax.ppermute(values, axis, pairs + [(b, a) for a, b in pairs])


def shape(*dims):
    return jax.ShapeDtypeStruct(dims, F32)


def packed_shape(layers, mine):
    per = LANES // (4 * mine)
    return shape(-(-layers // per) * mine, LANES)


def other_scratch(shapes):
    out = []
    for d in shapes:
        out += [pltpu.VMEM(d, F32)] * len(NAT_OTHER)
    return out + [pltpu.VMEM(d, F32) for d in shapes]


def on_device(u0, sub, cat, planar, vertical, ratio, watt):
    nx, ny = lax.axis_size("gx"), lax.axis_size("gy")
    layers, height, width = u0.shape
    halo = halo_cells()
    half, hh = height // 2, halo // 2
    planes = 2 * layers + 1
    assert height == width == LANES and 2 * halo <= LANES and halo + half <= LANES

    own, a, b = pl.pallas_call(
        functools.partial(prep_kernel, halo=halo),
        out_shape=(shape(planes, height, width), shape(planes, halo, height), shape(planes, halo, height)),
        in_specs=[HBM] * 4,
        out_specs=(VMEM,) * 3,
        scratch_shapes=[
            pltpu.SMEM(watt.shape, F32),
            pltpu.VMEM(cat.shape, jnp.int32),
            pltpu.VMEM(sub.shape, jnp.int32),
            pltpu.SemaphoreType.DMA((4,)),
        ],
        compiler_params=limit(8),
        name="prep",
    )(*[pltpu.with_memory_space_constraint(x, pltpu.HBM) for x in (watt, cat, u0, sub)])
    a, b = swap(a, "gy", 0), swap(b, "gy", 1)

    lines = planes * 4 * hh
    sp, a, b = pl.pallas_call(
        functools.partial(split_kernel, halo=halo),
        out_shape=(shape(planes, 4, half, LANES), shape(lines, LANES), shape(lines, LANES)),
        in_specs=[VMEM] * 3,
        out_specs=(VMEM,) * 3,
        scratch_shapes=[pltpu.VMEM((2, 2, height, LANES), F32)],
        compiler_params=limit(20),
        name="split",
    )(own, a, b)
    a, b = swap(a, "gx", 0), swap(b, "gx", 1)

    tall = up8(half + 2 * hh) + 2 * PAD
    four, two = (4, layers, tall, LANES), (2, layers, tall, LANES)
    sides = [(height + 2 * halo) >> level for level in range(1, FIRST)]
    geos = [geometry(layers, side) for side in sides]
    assert geos[0][0] == 1
    nat_shapes = [(geo[2], up8(side) + 2 * PAD, LANES) for geo, side in zip(geos, sides)]
    sizes = [four if name in ("u", "f", "invd", "fl") else two for name in SPLIT_KEPT]
    sizes += [four] * 4 + [(4, tall, LANES)] + [nat_shapes[0]] * 3
    sizes.append((3 * planar.shape[0], 8, LANES))
    shared = pl.pallas_call(
        functools.partial(center_kernel, halo=halo, half=half, kinds=planar.shape[0]),
        out_shape=tuple(shape(*d) for d in sizes),
        in_specs=[SMEM] * 3 + [VMEM],
        out_specs=(VMEM,) * len(sizes),
        compiler_params=limit(24),
        name="center",
    )(planar, vertical, ratio, sp)
    kept = []
    for d in nat_shapes:
        kept += [shape(*d)] * len(NAT_KEPT)
    *saved, block = pl.pallas_call(
        functools.partial(
            down_kernel, halo=halo, half=half, kinds=planar.shape[0], geos=tuple(geos)
        ),
        out_shape=(*[shape(*d) for d in sizes], *kept, packed_shape(layers, height >> FIRST)),
        in_specs=[VMEM] * (2 + len(sizes)),
        out_specs=(VMEM,) * (len(sizes) + len(kept) + 1),
        scratch_shapes=other_scratch(nat_shapes)[3:],
        input_output_aliases={2 + n: n for n in range(len(sizes))},
        compiler_params=limit(26),
        name="down",
    )(a, b, *shared)
    saved = saved[: len(SPLIT_KEPT)] + saved[len(sizes) :]

    a, b = swap(block, "gy", 0), swap(block, "gy", 1)
    column = jnp.stack([block, a, b])
    above, below = swap(column, "gx", 0), swap(column, "gx", 1)
    mine = height >> FIRST
    assert 4 * mine <= LANES
    sides = [3 * mine >> n for n in range(LOCAL - FIRST)]
    block_geos = [geometry(layers, side) for side in sides]
    block_shapes = [(geo[2], up8(side) + 2 * PAD, LANES) for geo, side in zip(block_geos, sides)]
    kept = []
    for d in block_shapes:
        kept += [shape(*d)] * len(NAT_KEPT)
    *more, payload = pl.pallas_call(
        functools.partial(mid_kernel, geos=tuple(block_geos)),
        out_shape=(*kept, packed_shape(layers, height >> LOCAL)),
        in_specs=[VMEM] * 5,
        out_specs=(VMEM,) * (len(kept) + 1),
        scratch_shapes=other_scratch(block_shapes),
        compiler_params=limit(20),
        name="mid",
    )(block, a, b, above, below)
    saved += more
    nat_shapes += block_shapes

    sent = jnp.broadcast_to(payload[None], (nx * ny,) + payload.shape)
    gathered = lax.all_to_all(sent, ("gx", "gy"), 0, 0)

    whole_geos = [geometry(layers, ny * width >> level) for level in range(LOCAL, LEVELS + 1)]
    wholes = [
        (geo[2], up8(nx * height >> level) + 2 * PAD, LANES)
        for geo, level in zip(whole_geos, range(LOCAL, LEVELS + 1))
    ]
    scratch = []
    for d in wholes:
        scratch += [pltpu.VMEM(d, F32)] * len(WHOLE)
    scratch += [pltpu.VMEM(d, F32) for d in wholes[:-1]]
    scratch += [pltpu.VMEM(four, F32)] + [pltpu.VMEM(d, F32) for d in nat_shapes]
    scratch.append(pltpu.VMEM((layers, wholes[0][1] + PAD, LANES), F32))
    return pl.pallas_call(
        functools.partial(
            up_kernel,
            halo=halo,
            half=half,
            spans=(nx, ny),
            geos=tuple(geos + block_geos),
            whole_geos=tuple(whole_geos),
        ),
        out_shape=shape(layers, height, width),
        in_specs=[VMEM] * (1 + len(saved)),
        out_specs=VMEM,
        scratch_shapes=scratch,
        compiler_params=limit(16, scratch),
        name="up",
    )(gathered, *saved)


def solution(mesh):
    placed = (P(None, "gx", "gy"), P(None, "gx", "gy"), P("gx", "gy"), P(), P(), P(), P())
    return jax.shard_map(
        on_device, mesh=mesh, in_specs=placed, out_specs=P(None, "gx", "gy"), check_vma=False
    )
```

```python
import functools
import math

import jax
import jax.numpy as jnp
from jax import lax
from jax.experimental import pallas as pl
from jax.experimental.pallas import tpu as pltpu
from jax.sharding import PartitionSpec as P

TILE = 16
LEVELS = 6
FIRST = 2
LOCAL = 4
COARSE_ITERS = 12
LANES = 128
PAD = 8
MOST = dict(split=12, nat=12, first=12, residual=12, setup=12, look=1, faces=4, remain=12, add=12)
HI = lax.Precision.HIGHEST
F32 = jnp.float32
VMEM = pl.BlockSpec(memory_space=pltpu.VMEM)
SMEM = pl.BlockSpec(memory_space=pltpu.SMEM)
HBM = pl.BlockSpec(memory_space=pltpu.HBM)


def limit(mib, scratch=()):
    held = sum(4 * math.prod(ref.shape) for ref in scratch)
    return pltpu.CompilerParams(vmem_limit_bytes=mib * 1024 * 1024 + held + held // 4)


def up8(n):
    return -(-n // 8) * 8


def halo_cells():
    need, above = [], 0
    for level in range(FIRST):
        need.append(above + 4)
        above = -(-need[-1] // 2)
    f = 0
    for level in reversed(range(FIRST)):
        inner = max(need[level], 2 * f + 1)
        f = inner + (4 if level == 0 else 3)
    unit = 2**FIRST
    return -(-f // unit) * unit


def iota(shape, axis):
    return lax.broadcasted_iota(jnp.int32, shape, axis)


def rows(t, off=0):
    first, count = t
    start = first * 8 if isinstance(first, int) else pl.multiple_of(first * 8, 8)
    return pl.ds(start + (PAD + off), 8 * count)


def over(lo, hi, most, body):
    steps = -(-(hi - lo) // most)
    size = -(-(hi - lo) // steps)
    if steps == 1:
        body((lo, size))
        return

    def step(i, carry):
        body((jnp.minimum(lo + i * size, hi - size), size))
        return carry

    lax.fori_loop(0, steps, step, 0)


def dot(a, b):
    return jnp.dot(a, b, precision=HI, preferred_element_type=F32)


def pick_dot(x, pick, pieces=3):
    pick = pick.astype(jnp.bfloat16)
    total = None
    for n in range(pieces):
        piece = x.astype(jnp.bfloat16)
        part = jnp.dot(piece, pick, preferred_element_type=F32)
        total = part if total is None else total + part
        if n < pieces - 1:
            x = x - piece.astype(F32)
    return total


def prep_kernel(watt_hbm, cat_hbm, u_hbm, sub_hbm, planes, a_ref, b_ref, watt, cat_ref, sub_ref, sems, *, halo):
    layers, height, width = u_hbm.shape
    copies = [
        pltpu.make_async_copy(source, target, sems.at[n])
        for n, (source, target) in enumerate(
            ((u_hbm, planes.at[pl.ds(0, layers)]), (sub_hbm, sub_ref), (cat_hbm, cat_ref), (watt_hbm, watt))
        )
    ]
    for copy in copies:
        copy.start()
    even = lax.axis_index("gy") % 2 == 0

    def send(q):
        turned = planes[q].T
        low, high = turned[:halo], turned[width - halo :]
        a_ref[q] = jnp.where(even, high, low)
        b_ref[q] = jnp.where(even, low, high)

    for copy in copies:
        copy.wait()
    cat = cat_ref[...]
    power = jnp.zeros(cat.shape, F32)
    for n in range(watt.shape[0]):
        power = power + jnp.where(cat == n, watt[n], 0.0)
    spread_r = (iota((height, cat.shape[0]), 0) // TILE == iota((height, cat.shape[0]), 1)).astype(F32)
    spread_c = (iota((cat.shape[1], width), 1) // TILE == iota((cat.shape[1], width), 0)).astype(F32)
    planes[2 * layers] = dot(dot(spread_r, power), spread_c)
    for q in range(2 * layers + 1):
        if layers <= q < 2 * layers:
            planes[q] = (sub_ref[q - layers] + 1).astype(F32)
        send(q)


def split_kernel(own, ra, rb, out, a_ref, b_ref, scr, *, halo):
    count, height, width = own.shape
    layers = count // 2
    even_y, even_x = lax.axis_index("gy") % 2 == 0, lax.axis_index("gx") % 2 == 0
    half, hh = height // 2, halo // 2
    source, target = iota((width + LANES, 2 * LANES), 0), iota((width + LANES, 2 * LANES), 1)
    cell = 2 * (target % LANES) + target // LANES
    want = jnp.where(
        cell < halo, width + cell, jnp.where(cell < halo + width, cell - halo, cell)
    )
    pick = ((source == want) & (cell < 2 * halo + width)).astype(F32)
    planes = []
    for q in range(count):
        left = jnp.where(even_y, rb[q], ra[q])
        right = jnp.where(even_y, ra[q], rb[q])
        sides = jnp.concatenate([left, right, jnp.zeros((LANES - 2 * halo, height), F32)], 0).T
        planes.append(jnp.concatenate([own[q], sides], 1))
    first = pick_dot(jnp.concatenate(planes[:layers] + planes[2 * layers :], 0), pick)
    second = pick_dot(jnp.concatenate(planes[layers : 2 * layers], 0), pick, 1)
    for q in range(2 * layers + 1):
        if layers <= q < 2 * layers:
            both = second[(q - layers) * height : (q - layers + 1) * height]
        else:
            at = q if q < layers else layers
            both = first[at * height : (at + 1) * height]
        scr[q % 2, 0] = both[:, :LANES]
        scr[q % 2, 1] = both[:, LANES:]
        for p in range(2):
            for j in range(2):
                z = scr[q % 2, j, pl.ds(p, half, stride=2), :]
                out[q, 2 * p + j] = z
                at = (4 * q + 2 * p + j) * hh
                first_rows, last_rows = z[:hh], z[half - hh :]
                a_ref[at : at + hh] = jnp.where(even_x, last_rows, first_rows)
                b_ref[at : at + hh] = jnp.where(even_x, first_rows, last_rows)


def split_block(s, colour, t, layers):
    u, at = s["u"], rows(t)
    other = {
        (p, j, k): u[2 * p + j, k, at]
        for k in range(layers)
        for p in range(2)
        for j in range(2)
        if (p + j + k) % 2 != colour
    }
    for k in range(layers):
        for p in range(2):
            for j in range(2):
                if (p + j + k) % 2 != colour:
                    continue
                pj = 2 * p + j
                total = s["f"][pj, k, at] + s["fri"][j, k, at] * other[1 - p, j, k]
                if p == 0:
                    total += s["fro"][j, k, at] * u[2 + j, k, rows(t, -1)]
                else:
                    total += s["fro"][j, k, rows(t, 1)] * u[j, k, rows(t, 1)]
                beside = other[p, 1 - j, k]
                total += s["fci"][p, k, at] * beside
                if j == 0:
                    total += s["fco"][p, k, at] * pltpu.roll(beside, 1, 1)
                else:
                    total += s["fcr"][p, k, at] * pltpu.roll(beside, LANES - 1, 1)
                if k > 0:
                    total += s["fl"][pj, k, at] * other[p, j, k - 1]
                if k < layers - 1:
                    total += s["fl"][pj, k + 1, at] * other[p, j, k + 1]
                yield pj, k, total


def split_half(s, colour, lo, hi, layers):
    def body(t):
        for pj, k, total in split_block(s, colour, t, layers):
            s["u"][pj, k, rows(t)] = total * s["invd"][pj, k, rows(t)]

    over(lo, hi, MOST["split"], body)


def split_sweeps(s, lo, hi, layers):
    for sweep in range(2):
        split_half(s, 0, lo, hi, layers)
        split_half(s, 1, lo, hi, layers)


def geometry(layers, width):
    assert width <= LANES
    fold = max(f for f in range(1, layers + 1) if layers % f == 0 and f * width <= LANES)
    return fold, width, layers // fold


def places(extent, geo):
    lane = iota(extent, 1)
    group = jnp.zeros(extent, jnp.int32)
    for g in range(1, geo[0] + 1):
        if g * geo[1] < LANES:
            group = group + (lane >= g * geo[1]).astype(jnp.int32)
    return group, lane - group * geo[1]


def odd_cells(t, geo):
    extent = (8 * t[1], LANES)
    group, col = places(extent, geo)
    return (iota(extent, 0) + col + group * geo[2]) % 2


def nat_setup(s, factor):
    fold, width, deep = s["geo"]
    height = s["lat"].shape[1]
    c = 0.5 * factor

    def body(t):
        at = rows(t)
        group, col = places((8 * t[1], LANES), s["geo"])
        first, last = col == 0, col == width - 1
        between = None
        for k in range(deep):
            lat, stor, vert = s["lat"][k, at], s["stor"][k, at], s["vert"][k, at]
            above = c * (lat + s["lat"][k, rows(t, -1)])
            below = c * (lat + s["lat"][k, rows(t, 1)])
            before = c * (lat + jnp.where(first, 0.0, pltpu.roll(lat, 1, 1)))
            after = c * (lat + jnp.where(last, 0.0, pltpu.roll(lat, LANES - 1, 1)))
            diag = stor + above + below + before + after
            if k > 0:
                face = 0.5 * (vert + s["vert"][k - 1, at])
                s["wl"][k, at] = face
                diag += face
            elif fold > 1:
                between = 0.5 * (vert + pltpu.roll(s["vert"][deep - 1, at], width, 1))
                between = jnp.where((group > 0) & (group < fold), between, 0.0)
                s["wl"][0, at] = between
                diag += between
            if k < deep - 1:
                diag += 0.5 * (vert + s["vert"][k + 1, at])
            elif fold > 1:
                diag += pltpu.roll(between, LANES - width, 1)
            inside = stor > 0.0
            s["wr"][k, at] = above
            s["wc"][k, at] = jnp.where(first, 0.0, before)
            s["wcr"][k, at] = jnp.where(last, 0.0, after)
            s["diag"][k, at] = diag
            s["invd"][k, at] = jnp.where(inside, 1.0 / jnp.where(inside, diag, 1.0), 0.0)

    s["wr"][:, height - PAD :] = jnp.zeros((deep, PAD, LANES), F32)
    over(0, (height - 2 * PAD) // 8, MOST["setup"], body)


def nat_block(s, t):
    u, at = s["u"], rows(t)
    fold, width, deep = s["geo"]
    mid = [u[k, at] for k in range(deep)]
    wl = s["wl"][0, at] if fold > 1 else None
    between = None if wl is None else pltpu.roll(wl * mid[0], LANES - width, 1)
    for k in range(deep):
        total = s["f"][k, at] + s["wr"][k, at] * u[k, rows(t, -1)]
        total += s["wr"][k, rows(t, 1)] * u[k, rows(t, 1)]
        beside = s["wc"][k, at] * pltpu.roll(mid[k], 1, 1)
        beside += s["wcr"][k, at] * pltpu.roll(mid[k], LANES - 1, 1)
        if k > 0:
            total += wl * mid[k - 1]
        elif fold > 1:
            total += wl * pltpu.roll(mid[deep - 1], width, 1)
        if k < deep - 1:
            wl = s["wl"][k + 1, at]
            total += wl * mid[k + 1]
        elif fold > 1:
            total += between
        yield k, total + beside, mid[k]


def nat_half(s, colour, lo, hi):
    def body(t):
        odd = odd_cells(t, s["geo"])
        for k, total, old in nat_block(s, t):
            value = total * s["invd"][k, rows(t)]
            s["u"][k, rows(t)] = jnp.where(odd == (colour + k) % 2, value, old)

    over(lo, hi, MOST["nat"], body)


def nat_first(s, lo, hi):
    deep, height, _ = s["u"].shape
    zeros = jnp.zeros((deep, PAD, LANES), F32)
    s["u"][:, :PAD] = zeros
    s["u"][:, height - PAD :] = zeros

    def body(t):
        odd = odd_cells(t, s["geo"])
        for k in range(deep):
            value = s["f"][k, rows(t)] * s["invd"][k, rows(t)]
            s["u"][k, rows(t)] = jnp.where(odd == k % 2, value, 0.0)

    over(lo, hi, MOST["first"], body)


def nat_residual(s, res, lo, hi):
    def body(t):
        for k, total, old in nat_block(s, t):
            res[k, rows(t)] = total - s["diag"][k, rows(t)] * old

    over(lo, hi, MOST["residual"], body)


def nat_down(s, res, steps):
    nat_first(s, 0, steps)
    for colour in (1, 0, 1):
        nat_half(s, colour, 0, steps)
    nat_residual(s, res, 0, steps)


def move(parts, a, b, relation, scale):
    jobs = {}
    for ka in range(a[2]):
        for kb in range(b[2]):
            key = tuple(
                (ga, gb)
                for ga in range(a[0])
                for gb in range(b[0])
                if ga * a[2] + ka == gb * b[2] + kb
            )
            if key:
                jobs.setdefault(key, []).append((ka, kb))
    c, m = iota((LANES, LANES), 0), iota((LANES, LANES), 1)
    out = [None] * b[2]
    count = parts[0].shape[0]
    for key, members in jobs.items():
        hit = None
        for ga, gb in key:
            ca, mb = c - ga * a[1], m - gb * b[1]
            here = (ca >= 0) & (ca < a[1]) & (mb >= 0) & (mb < b[1]) & relation(ca, mb)
            hit = here if hit is None else hit | here
        moved = pick_dot(
            jnp.concatenate([parts[ka] for ka, _ in members], 0), jnp.where(hit, scale, 0.0), 2
        )
        for n, (_, kb) in enumerate(members):
            part = moved[n * count : (n + 1) * count]
            out[kb] = part if out[kb] is None else out[kb] + part
    return out


def pair_rows(ref, k, start, count):
    part = ref[k, pl.ds(start, count, stride=2), :]
    return part + ref[k, pl.ds(start + 1, count, stride=2), :]


def restrict_all(pairs, a, b):
    deep, height = pairs[0][1].shape[0], pairs[0][1].shape[1] - 2 * PAD
    zeros = jnp.zeros((deep, PAD, LANES), F32)
    for _, target in pairs:
        target[:, :PAD] = zeros
        target[:, PAD + height :] = zeros
    parts = [
        jnp.concatenate([pair_rows(source, k, PAD, height) for source, _ in pairs], 0)
        for k in range(a[2])
    ]
    out = move(parts, a, b, lambda c, m: c // 2 == m, 0.25)
    for n, (_, target) in enumerate(pairs):
        for k in range(deep):
            target[k, PAD : PAD + height] = out[k][n * height : (n + 1) * height]


def prolong_into(s, u_in, coarse, geo, mask):
    deep, height, _ = s["u"].shape
    n = (height - 2 * PAD) // 2
    tall = up8(n)
    parts = [coarse(k)[:tall] for k in range(geo[2])]
    out = move(parts, geo, s["geo"], lambda c, m: c == m // 2, 1.0)
    for k in range(deep):
        wide = out[k][:n]
        for p in range(2):
            at = pl.ds(PAD + p, n, stride=2)
            add = wide
            if mask:
                add = jnp.where(s["invd"][k, at, :] > 0.0, wide, 0.0)
            s["u"][k, at, :] = u_in[k, at, :] + add


def nat_up(s, lo, hi):
    for sweep in range(2):
        nat_half(s, 0, lo, hi)
        nat_half(s, 1, lo, hi)


SPLIT_KEPT = ("u", "f", "invd", "fri", "fro", "fci", "fco", "fcr", "fl")
NAT_KEPT = ("u", "f", "invd", "wr", "wc", "wcr", "wl")
NAT_OTHER = ("lat", "vert", "stor", "diag")


def pack_own(payload, last, res, layers, mine, off):
    group = 4 * mine
    per = LANES // group
    quantities = (res, last["lat"], last["vert"], last["stor"])
    parts = [
        jnp.concatenate([pair_rows(ref, k, PAD + off, mine) for ref in quantities], 0)
        for k in range(last["geo"][2])
    ]
    packed = move(
        parts, last["geo"], (1, mine, layers), lambda c, m: (c >= off) & ((c - off) // 2 == m), 0.25
    )
    for wide in range(-(-layers // per)):
        total = jnp.zeros((mine, LANES), F32)
        for n in range(wide * per * 4, min(layers, (wide + 1) * per) * 4):
            part = packed[n // 4][n % 4 * mine : (n % 4 + 1) * mine]
            base = (n - wide * per * 4) * mine
            total += pltpu.roll(part, base, 1) if base else part
        payload[wide * mine : (wide + 1) * mine] = total


def look_up(s, first, heat, kinds, lo, hi):
    layers = s["u"].shape[1]

    def look(t):
        for k in range(layers):
            sums = [None, None, None]
            for pj in range(4):
                at = (pj, k, rows(t))
                label = s["diag"][at]
                value = [jnp.zeros_like(label)] * 3
                for n in range(kinds):
                    hit = label == float(n + 1)
                    value = [jnp.where(hit, s["table"][i * kinds + n], value[i]) for i in range(3)]
                for i, name in enumerate(("lat", "vert", "stor")):
                    s[name][at] = value[i]
                    sums[i] = value[i] if sums[i] is None else sums[i] + value[i]
                f = value[2] * s["u"][at]
                if k == 0:
                    f = f + heat[pj, rows(t)]
                s["f"][at] = f
            for i, name in enumerate(("lat", "vert", "stor")):
                first[name][k, rows(t)] = sums[i] * 0.25

    over(lo, hi, MOST["look"], look)


def split_setup(s, lo, hi):
    layers = s["u"].shape[1]

    def faces(t):
        at = rows(t)
        for k in range(layers):
            lat = [s["lat"][pj, k, at] for pj in range(4)]
            inner_r = [0.5 * (lat[j] + lat[2 + j]) for j in range(2)]
            before_r = [0.5 * (s["lat"][2 + j, k, rows(t, -1)] + lat[j]) for j in range(2)]
            after_r = [0.5 * (lat[2 + j] + s["lat"][j, k, rows(t, 1)]) for j in range(2)]
            inner_c = [0.5 * (lat[2 * p] + lat[2 * p + 1]) for p in range(2)]
            before_c = [0.5 * (pltpu.roll(lat[2 * p + 1], 1, 1) + lat[2 * p]) for p in range(2)]
            after_c = [0.5 * (lat[2 * p + 1] + pltpu.roll(lat[2 * p], LANES - 1, 1)) for p in range(2)]
            for x in range(2):
                s["fri"][x, k, at] = inner_r[x]
                s["fro"][x, k, at] = before_r[x]
                s["fci"][x, k, at] = inner_c[x]
                s["fco"][x, k, at] = before_c[x]
                s["fcr"][x, k, at] = after_c[x]
            for p in range(2):
                for j in range(2):
                    pj = 2 * p + j
                    stor = s["stor"][pj, k, at]
                    diag = stor + inner_r[j] + (after_r[j] if p else before_r[j])
                    diag += inner_c[p] + (after_c[p] if j else before_c[p])
                    vert = s["vert"][pj, k, at]
                    if k > 0:
                        face = 0.5 * (vert + s["vert"][pj, k - 1, at])
                        s["fl"][pj, k, at] = face
                        diag += face
                    if k < layers - 1:
                        diag += 0.5 * (vert + s["vert"][pj, k + 1, at])
                    inside = stor > 0.0
                    s["invd"][pj, k, at] = jnp.where(inside, 1.0 / jnp.where(inside, diag, 1.0), 0.0)
                    s["diag"][pj, k, at] = diag

    over(lo, hi, MOST["faces"], faces)


SHARED = SPLIT_KEPT + ("lat", "vert", "stor", "diag", "heat", "lat1", "vert1", "stor1", "table")


def center_kernel(*refs, halo, half, kinds):
    tables, sp, out = refs[:3], refs[3], refs[4:]
    s = dict(zip(SHARED, out))
    first = {name: s[name + "1"] for name in ("lat", "vert", "stor")}
    layers, height, hh = s["u"].shape[1], s["u"].shape[2], halo // 2
    body_rows = slice(PAD + hh, PAD + hh + half)
    zeros = jnp.zeros((PAD, LANES), F32)
    for pj in range(4):
        for k in range(layers):
            for name in ("u", "lat"):
                s[name][pj, k, :PAD] = zeros
                s[name][pj, k, height - PAD :] = zeros
            s["u"][pj, k, body_rows] = sp[k, pj]
            s["diag"][pj, k, body_rows] = sp[layers + k, pj]
        s["heat"][pj, body_rows] = sp[2 * layers, pj]
    for ref in first.values():
        for k in range(layers):
            ref[k, :PAD] = zeros
            ref[k, height - PAD :] = zeros
    for i in range(3):
        for n in range(kinds):
            s["table"][i * kinds + n] = jnp.full((8, LANES), tables[i][n], F32)
    look_up(s, first, s["heat"], kinds, *bounds(hh, half, 0))
    split_setup(s, *bounds(hh, half, 1))


def bounds(hh, half, inner):
    if inner:
        return -(-(hh + 1) // 8), (hh + half - 1) // 8
    return hh // 8, -(-(hh + half) // 8)


def down_kernel(*refs, halo, half, kinds, geos):
    ra, rb = refs[:2]
    refs = list(refs[2 + len(SHARED) :])
    s = dict(zip(SHARED, refs[: len(SHARED)]))
    refs = refs[len(SHARED) :]
    nats = [{} for level in range(1, FIRST)]
    for n, now in enumerate(nats):
        now.update(zip(NAT_KEPT, refs[: len(NAT_KEPT)]), geo=geos[n])
        refs = refs[len(NAT_KEPT) :]
    payload = refs.pop(0)
    heat = s["heat"]
    for n, now in enumerate(nats):
        for name in NAT_OTHER:
            now[name] = s[name + "1"] if n == 0 and name != "diag" else refs.pop(0)
    ress = [refs.pop(0) for level in range(1, FIRST)]
    layers = s["u"].shape[1]
    height = s["u"].shape[2]
    hh = halo // 2
    steps = (height - 2 * PAD) // 8
    even = lax.axis_index("gx") % 2 == 0
    zeros = jnp.zeros((PAD, LANES), F32)

    def place(ref, index, q, pj):
        at = (4 * q + pj) * hh
        first, second = ra[at : at + hh], rb[at : at + hh]
        ref[index + (slice(PAD, PAD + hh),)] = jnp.where(even, second, first)
        ref[index + (slice(PAD + hh + half, PAD + 2 * hh + half),)] = jnp.where(even, first, second)

    for pj in range(4):
        for k in range(layers):
            place(s["u"], (pj, k), k, pj)
            place(s["diag"], (pj, k), layers + k, pj)
        place(heat, (pj,), 2 * layers, pj)
    for j in range(2):
        for k in range(layers):
            s["fro"][j, k, height - PAD :] = zeros
    first = nats[0]
    for ref in [first["f"]] + ress:
        for k in range(ref.shape[0]):
            ref[k, :PAD] = zeros
            ref[k, ref.shape[1] - PAD :] = zeros
    lo, hi = bounds(hh, half, 1)
    for begin, end in ((0, lo), (hi, steps)):
        look_up(s, first, heat, kinds, begin, end)
    for begin, end in ((0, lo), (hi, steps)):
        split_setup(s, begin, end)
    split_sweeps(s, 0, steps, layers)

    def remain(t):
        sums = {}
        for pj, k, total in split_block(s, 0, t, layers):
            r = total - s["diag"][pj, k, rows(t)] * s["u"][pj, k, rows(t)]
            sums[k] = sums[k] + r if k in sums else r
            if pj >= 2:
                first["f"][k, rows(t)] = sums[k] * 0.25

    over(0, steps, MOST["remain"], remain)

    for level in range(1, FIRST):
        now = nats[level - 1]
        nat_setup(now, 0.25**level)
        count = (now["u"].shape[1] - 2 * PAD) // 8
        nat_down(now, ress[level - 1], count)
        if level < FIRST - 1:
            below = nats[level]
            pairs = [(now[name], below[name]) for name in ("lat", "vert", "stor")]
            restrict_all(pairs + [(ress[level - 1], below["f"])], now["geo"], below["geo"])

    pack_own(payload, nats[-1], ress[-1], layers, 2 * half >> FIRST, halo >> (FIRST - 1))


def mid_kernel(own, ra, rb, ta, tb, *refs, geos):
    refs = list(refs)
    count = LOCAL - FIRST
    nats = []
    for n in range(count):
        nats.append(dict(zip(NAT_KEPT, refs[: len(NAT_KEPT)]), geo=geos[n]))
        refs = refs[len(NAT_KEPT) :]
    payload = refs.pop(0)
    for n in range(count):
        for name in NAT_OTHER:
            nats[n][name] = refs.pop(0)
    ress = refs
    layers = geos[0][0] * geos[0][2]
    mine = own.shape[0] // layers
    assert geos[0][0] == 1
    even_y, even_x = lax.axis_index("gy") % 2 == 0, lax.axis_index("gx") % 2 == 0
    zeros = jnp.zeros((PAD, LANES), F32)
    for now, res in zip(nats, ress):
        for ref in [now[name] for name in ("lat", "vert", "stor", "f")] + [res]:
            for k in range(ref.shape[0]):
                ref[k, :PAD] = zeros
                ref[k, ref.shape[1] - PAD :] = zeros
    group = iota((mine, LANES), 1) // mine

    def assemble(v, middle_of, a_of, b_of):
        for k in range(layers):
            lines = slice(k * mine, (k + 1) * mine)
            middle, a, b = middle_of(lines), a_of(lines), b_of(lines)
            left, right = jnp.where(even_y, b, a), jnp.where(even_y, a, b)
            middle, right = pltpu.roll(middle, mine, 1), pltpu.roll(right, 2 * mine, 1)
            for n, name in enumerate(("f", "lat", "vert", "stor")):
                value = jnp.where(group == (n + 1) % 4, middle, right)
                value = jnp.where(group == n, left, value)
                value = jnp.where(group == (n + 3) % 4, 0.0, value)
                if n:
                    value = pltpu.roll(value, LANES - n * mine, 1)
                nats[0][name][k, PAD + v * mine : PAD + (v + 1) * mine] = value

    def rows_from(ref):
        return [lambda lines, n=n: ref[n, lines] for n in range(3)]

    def outer(above, below):
        assemble(0, *rows_from(above))
        assemble(2, *rows_from(below))

    assemble(1, *[lambda lines, ref=ref: ref[lines] for ref in (own, ra, rb)])
    pl.when(even_x)(lambda: outer(tb, ta))
    pl.when(jnp.logical_not(even_x))(lambda: outer(ta, tb))
    for n, level in enumerate(range(FIRST, LOCAL)):
        now = nats[n]
        nat_setup(now, 0.25**level)
        nat_down(now, ress[n], (now["u"].shape[1] - 2 * PAD) // 8)
        if n < count - 1:
            pairs = [(now[name], nats[n + 1][name]) for name in ("lat", "vert", "stor")]
            restrict_all(pairs + [(ress[n], nats[n + 1]["f"])], geos[n], geos[n + 1])
    pack_own(payload, nats[-1], ress[-1], layers, mine >> count, mine >> (count - 1))


def conjugate(s):
    fold, width, deep = s["geo"]
    n = s["u"].shape[1] - 2 * PAD
    here, after = slice(PAD, PAD + n), slice(PAD + 1, PAD + 1 + n)
    row = iota((n, LANES), 0)
    planes = range(deep)
    above = [jnp.where(row > 0, s["wr"][k, here], 0.0) for k in planes]
    below = [jnp.where(row < n - 1, s["wr"][k, after], 0.0) for k in planes]
    before, behind, diag, inv, r = [
        [s[name][k, here] for k in planes] for name in ("wc", "wcr", "diag", "invd", "f")
    ]
    faces = [s["wl"][k, here] if k or fold > 1 else None for k in planes]

    def apply(v):
        out = []
        for k in planes:
            total = above[k] * pltpu.roll(v[k], 1, 0) + below[k] * pltpu.roll(v[k], n - 1, 0)
            total += before[k] * pltpu.roll(v[k], 1, 1) + behind[k] * pltpu.roll(v[k], LANES - 1, 1)
            if k > 0:
                total += faces[k] * v[k - 1]
            elif fold > 1:
                total += faces[0] * pltpu.roll(v[deep - 1], width, 1)
            if k < deep - 1:
                total += faces[k + 1] * v[k + 1]
            elif fold > 1:
                total += pltpu.roll(faces[0] * v[0], LANES - width, 1)
            out.append(diag[k] * v[k] - total)
        return out

    def inner(a, b):
        total = a[0] * b[0]
        for x, y in zip(a[1:], b[1:]):
            total += x * y
        return jnp.sum(jnp.sum(total, axis=0, keepdims=True), axis=1, keepdims=True)

    def step(_, carry):
        e, r, p = carry[:deep], carry[deep : 2 * deep], carry[2 * deep :]
        q = apply(p)
        z = [x * y for x, y in zip(r, inv)]
        w = [x * y for x, y in zip(q, inv)]
        rz, pq, zq, wq = inner(r, z), inner(p, q), inner(z, q), inner(w, q)
        alpha = rz / pq
        beta = (rz + alpha * (alpha * wq - 2.0 * zq)) / rz
        e = [x + alpha * y for x, y in zip(e, p)]
        r = [x - alpha * y for x, y in zip(r, q)]
        p = [x - alpha * y + beta * d for x, y, d in zip(z, w, p)]
        return (*e, *r, *p)

    start = (*[jnp.zeros((n, LANES), F32)] * deep, *r, *[x * y for x, y in zip(r, inv)])
    out = lax.fori_loop(0, COARSE_ITERS, step, start)
    for k in planes:
        s["u"][k, here] = out[k]


WHOLE = ("u", "f", "invd", "wr", "wc", "wcr", "wl", "lat", "vert", "stor", "diag")


def up_kernel(*refs, halo, half, spans, geos, whole_geos):
    refs = list(refs)
    gathered, traded = refs.pop(0), refs.pop(0)
    s = dict(zip(SPLIT_KEPT, refs[: len(SPLIT_KEPT)]))
    refs = refs[len(SPLIT_KEPT) :]
    nats = []
    for geo in geos:
        nats.append(dict(zip(NAT_KEPT, refs[: len(NAT_KEPT)]), geo=geo))
        refs = refs[len(NAT_KEPT) :]
    out = refs.pop(0)
    wholes = []
    for geo in whole_geos:
        wholes.append(dict(zip(WHOLE, refs[: len(WHOLE)]), geo=geo))
        refs = refs[len(WHOLE) :]
    ress = [refs.pop(0) for level in range(LOCAL, LEVELS)]
    fresh = [refs.pop(0) for level in range(LOCAL)]
    wider = refs.pop(0)
    nx, ny = spans
    layers = s["u"].shape[1]
    top = wholes[0]
    fold, width, deep = top["geo"]
    mine = 2 * half >> LOCAL
    group = 4 * mine
    per = LANES // group
    lane = iota((mine, LANES), 1)

    for whole in wholes:
        planes, height, _ = whole["u"].shape
        for name in ("u", "lat"):
            zeros = jnp.zeros((planes, PAD, LANES), F32)
            whole[name][:, :PAD] = zeros
            whole[name][:, height - PAD :] = zeros

    parity = lax.axis_index("gx") % 2

    def gather(x, core):
        at = pl.ds(pl.multiple_of(x * mine, 8) + PAD, mine)
        parts = []
        for wide in range(-(-layers // per)):
            lines = slice(wide * mine, (wide + 1) * mine)
            at_x = lax.div(x, 2) * ny
            turned = [
                jnp.where(parity == core, gathered[at_x + y, lines], traded[at_x + y, lines])
                for y in range(ny)
            ]
            parts.append([pltpu.roll(v, y * mine, 1) if y else v for y, v in enumerate(turned)])
        for k in range(deep):
            for n, name in enumerate(("f", "lat", "vert", "stor")):
                value = None
                for g in range(fold):
                    layer = g * deep + k
                    base = (layer % per) * group + n * mine
                    total = jnp.zeros((mine, LANES), F32)
                    for y in range(ny):
                        spot = (base + y * mine) % LANES
                        hit = (lane >= spot) & (lane < spot + mine)
                        total = jnp.where(hit, parts[layer // per][y], total)
                    turn = (g * width - base) % LANES
                    total = pltpu.roll(total, turn, 1) if turn else total
                    value = total if value is None else value + total
                top[name][k, at] = value

    def gather_some(step, carry):
        for n in range(4):
            gather(4 * step + n, n % 2)
        return carry

    lax.fori_loop(0, nx // 4, gather_some, 0)

    for n, level in enumerate(range(LOCAL, LEVELS)):
        now, below = wholes[n], wholes[n + 1]
        nat_setup(now, 0.25**level)
        nat_down(now, ress[n], (now["u"].shape[1] - 2 * PAD) // 8)
        pairs = [(now[name], below[name]) for name in ("lat", "vert", "stor")]
        restrict_all(pairs + [(ress[n], below["f"])], now["geo"], below["geo"])
    nat_setup(wholes[-1], 0.25**LEVELS)
    conjugate(wholes[-1])

    def planes_of(ref):
        return lambda k: ref[k, PAD : ref.shape[1] - PAD]

    for n in reversed(range(len(wholes) - 1)):
        now, below = wholes[n], wholes[n + 1]
        prolong_into(now, now["u"], planes_of(below["u"]), below["geo"], False)
        nat_up(now, 0, (now["u"].shape[1] - 2 * PAD) // 8)

    x, y = lax.axis_index("gx"), lax.axis_index("gy")
    reach = (2 * half >> FIRST) >> (LOCAL - FIRST)
    height = top["u"].shape[1]
    need = (nats[-1]["u"].shape[1] - 2 * PAD) // 2
    lanes = iota((height, LANES), 1)
    for layer in range(layers):
        g, k = layer // deep, layer % deep
        value = top["u"][k]
        if g:
            value = pltpu.roll(value, LANES - g * width, 1)
        wider[layer, :height] = jnp.where(lanes < width, value, 0.0)
        wider[layer, height:] = jnp.zeros((PAD, LANES), F32)
    begin = PAD + x * mine - reach
    turn = lax.rem(LANES + reach - y * mine, LANES)

    def coarse(k):
        return pltpu.roll(wider[k, pl.ds(begin, need)], turn, 1)

    coarse_geo = (1, nats[-1]["geo"][1] // 2, layers)
    margins, above = [], 0
    for level in range(LOCAL):
        margins.append(above + 4)
        above = -(-margins[-1] // 2)
    for level in reversed(range(1, LOCAL)):
        now = dict(nats[level - 1])
        before = now["u"]
        now["u"] = fresh[level]
        planes, height, _ = before.shape
        now["u"][:, :PAD] = jnp.zeros((planes, PAD, LANES), F32)
        now["u"][:, height - PAD :] = jnp.zeros((planes, PAD, LANES), F32)
        prolong_into(now, before, coarse, coarse_geo, level == LOCAL - 1)
        own = 2 * half >> level
        side = halo >> level if level < FIRST else (2 * half >> FIRST) >> (level - FIRST)
        reach = margins[level]
        nat_up(now, (side - reach) // 8, min(-(-(side + own + reach) // 8), (height - 2 * PAD) // 8))
        coarse, coarse_geo = planes_of(now["u"]), now["geo"]
        if level == FIRST:
            assert coarse_geo[0] == 1
            skip, blocks = side - (halo >> FIRST), now["u"]

            def coarse(k):
                return pltpu.roll(
                    blocks[k, PAD + skip : blocks.shape[1] - PAD], LANES - skip, 1
                )

            coarse_geo = (1, (2 * half + 2 * halo) >> FIRST, layers)

    now = dict(s)
    now["u"] = fresh[0]
    hh = halo // 2
    lo, hi = (hh - 2) // 8, -(-(hh + half + 2) // 8)
    steps = (s["u"].shape[2] - 2 * PAD) // 8

    def add(t):
        for k in range(layers):
            value = fresh[1][k, rows(t)]
            for pj in range(4):
                now["u"][pj, k, rows(t)] = s["u"][pj, k, rows(t)] + value

    over(lo - 1, min(hi + 1, steps), MOST["add"], add)
    split_sweeps(now, lo, hi, layers)
    source, target = iota((2 * LANES, 2 * half), 0), iota((2 * LANES, 2 * half), 1)
    pick = ((source % LANES == hh + target // 2) & (source // LANES == target % 2)).astype(F32)
    body_rows = slice(PAD + hh, PAD + hh + half)
    spots = [(k, p) for k in range(layers) for p in range(2)]
    both = [
        jnp.concatenate([now["u"][2 * p + j, k, body_rows] for k, p in spots], 0) for j in range(2)
    ]
    every = pick_dot(jnp.concatenate(both, 1), pick)
    for n, (k, p) in enumerate(spots):
        out[k, pl.ds(p, half, stride=2), :] = every[n * half : (n + 1) * half]


def swap(values, axis, first):
    count = lax.axis_size(axis)
    pairs = [(i, i + 1) for i in range(first, count - 1, 2)]
    return lax.ppermute(values, axis, pairs + [(b, a) for a, b in pairs])


def shape(*dims):
    return jax.ShapeDtypeStruct(dims, F32)


def packed_shape(layers, mine):
    per = LANES // (4 * mine)
    return shape(-(-layers // per) * mine, LANES)


def other_scratch(shapes):
    out = []
    for d in shapes:
        out += [pltpu.VMEM(d, F32)] * len(NAT_OTHER)
    return out + [pltpu.VMEM(d, F32) for d in shapes]


def on_device(u0, sub, cat, planar, vertical, ratio, watt):
    nx, ny = lax.axis_size("gx"), lax.axis_size("gy")
    layers, height, width = u0.shape
    halo = halo_cells()
    half, hh = height // 2, halo // 2
    planes = 2 * layers + 1
    assert height == width == LANES and 2 * halo <= LANES and halo + half <= LANES

    own, a, b = pl.pallas_call(
        functools.partial(prep_kernel, halo=halo),
        out_shape=(shape(planes, height, width), shape(planes, halo, height), shape(planes, halo, height)),
        in_specs=[HBM] * 4,
        out_specs=(VMEM,) * 3,
        scratch_shapes=[
            pltpu.SMEM(watt.shape, F32),
            pltpu.VMEM(cat.shape, jnp.int32),
            pltpu.VMEM(sub.shape, jnp.int32),
            pltpu.SemaphoreType.DMA((4,)),
        ],
        compiler_params=limit(8),
        name="prep",
    )(*[pltpu.with_memory_space_constraint(x, pltpu.HBM) for x in (watt, cat, u0, sub)])
    a, b = swap(a, "gy", 0), swap(b, "gy", 1)

    lines = planes * 4 * hh
    sp, a, b = pl.pallas_call(
        functools.partial(split_kernel, halo=halo),
        out_shape=(shape(planes, 4, half, LANES), shape(lines, LANES), shape(lines, LANES)),
        in_specs=[VMEM] * 3,
        out_specs=(VMEM,) * 3,
        scratch_shapes=[pltpu.VMEM((2, 2, height, LANES), F32)],
        compiler_params=limit(20),
        name="split",
    )(own, a, b)
    a, b = swap(a, "gx", 0), swap(b, "gx", 1)

    tall = up8(half + 2 * hh) + 2 * PAD
    four, two = (4, layers, tall, LANES), (2, layers, tall, LANES)
    sides = [(height + 2 * halo) >> level for level in range(1, FIRST)]
    geos = [geometry(layers, side) for side in sides]
    assert geos[0][0] == 1
    nat_shapes = [(geo[2], up8(side) + 2 * PAD, LANES) for geo, side in zip(geos, sides)]
    sizes = [four if name in ("u", "f", "invd", "fl") else two for name in SPLIT_KEPT]
    sizes += [four] * 4 + [(4, tall, LANES)] + [nat_shapes[0]] * 3
    sizes.append((3 * planar.shape[0], 8, LANES))
    shared = pl.pallas_call(
        functools.partial(center_kernel, halo=halo, half=half, kinds=planar.shape[0]),
        out_shape=tuple(shape(*d) for d in sizes),
        in_specs=[SMEM] * 3 + [VMEM],
        out_specs=(VMEM,) * len(sizes),
        compiler_params=limit(24),
        name="center",
    )(planar, vertical, ratio, sp)
    kept = []
    for d in nat_shapes:
        kept += [shape(*d)] * len(NAT_KEPT)
    *saved, block = pl.pallas_call(
        functools.partial(
            down_kernel, halo=halo, half=half, kinds=planar.shape[0], geos=tuple(geos)
        ),
        out_shape=(*[shape(*d) for d in sizes], *kept, packed_shape(layers, height >> FIRST)),
        in_specs=[VMEM] * (2 + len(sizes)),
        out_specs=(VMEM,) * (len(sizes) + len(kept) + 1),
        scratch_shapes=other_scratch(nat_shapes)[3:],
        input_output_aliases={2 + n: n for n in range(len(sizes))},
        compiler_params=limit(26),
        name="down",
    )(a, b, *shared)
    saved = saved[: len(SPLIT_KEPT)] + saved[len(sizes) :]

    a, b = swap(block, "gy", 0), swap(block, "gy", 1)
    column = jnp.stack([block, a, b])
    above, below = swap(column, "gx", 0), swap(column, "gx", 1)
    mine = height >> FIRST
    assert 4 * mine <= LANES
    sides = [3 * mine >> n for n in range(LOCAL - FIRST)]
    block_geos = [geometry(layers, side) for side in sides]
    block_shapes = [(geo[2], up8(side) + 2 * PAD, LANES) for geo, side in zip(block_geos, sides)]
    kept = []
    for d in block_shapes:
        kept += [shape(*d)] * len(NAT_KEPT)
    *more, payload = pl.pallas_call(
        functools.partial(mid_kernel, geos=tuple(block_geos)),
        out_shape=(*kept, packed_shape(layers, height >> LOCAL)),
        in_specs=[VMEM] * 5,
        out_specs=(VMEM,) * (len(kept) + 1),
        scratch_shapes=other_scratch(block_shapes),
        compiler_params=limit(20),
        name="mid",
    )(block, a, b, above, below)
    saved += more
    nat_shapes += block_shapes

    assert nx % 4 == 0
    groups = [[x * ny + y for x in range(c, nx, 2) for y in range(ny)] for c in range(2)]
    sent = jnp.broadcast_to(payload[None], (nx // 2 * ny,) + payload.shape)
    gathered = lax.all_to_all(sent, ("gx", "gy"), 0, 0, axis_index_groups=groups)
    traded = swap(gathered, "gx", 0)

    whole_geos = [geometry(layers, ny * width >> level) for level in range(LOCAL, LEVELS + 1)]
    wholes = [
        (geo[2], up8(nx * height >> level) + 2 * PAD, LANES)
        for geo, level in zip(whole_geos, range(LOCAL, LEVELS + 1))
    ]
    scratch = []
    for d in wholes:
        scratch += [pltpu.VMEM(d, F32)] * len(WHOLE)
    scratch += [pltpu.VMEM(d, F32) for d in wholes[:-1]]
    scratch += [pltpu.VMEM(four, F32)] + [pltpu.VMEM(d, F32) for d in nat_shapes]
    scratch.append(pltpu.VMEM((layers, wholes[0][1] + PAD, LANES), F32))
    return pl.pallas_call(
        functools.partial(
            up_kernel,
            halo=halo,
            half=half,
            spans=(nx, ny),
            geos=tuple(geos + block_geos),
            whole_geos=tuple(whole_geos),
        ),
        out_shape=shape(layers, height, width),
        in_specs=[VMEM] * (2 + len(saved)),
        out_specs=VMEM,
        scratch_shapes=scratch,
        compiler_params=limit(16, scratch),
        name="up",
    )(gathered, traded, *saved)


def solution(mesh):
    placed = (P(None, "gx", "gy"), P(None, "gx", "gy"), P("gx", "gy"), P(), P(), P(), P())
    return jax.shard_map(
        on_device, mesh=mesh, in_specs=placed, out_specs=P(None, "gx", "gy"), check_vma=False
    )
```

```python
import functools
import math

import jax
import jax.numpy as jnp
from jax import lax
from jax.experimental import pallas as pl
from jax.experimental.pallas import tpu as pltpu
from jax.sharding import PartitionSpec as P

TILE = 16
LEVELS = 6
FIRST = 2
LOCAL = 4
COARSE_ITERS = 12
LANES = 128
PAD = 8
MOST = dict(split=12, nat=12, first=12, residual=12, setup=12, look=1, faces=4, remain=12, add=12)
HI = lax.Precision.HIGHEST
F32 = jnp.float32
VMEM = pl.BlockSpec(memory_space=pltpu.VMEM)
SMEM = pl.BlockSpec(memory_space=pltpu.SMEM)
HBM = pl.BlockSpec(memory_space=pltpu.HBM)


def limit(mib, scratch=()):
    held = sum(4 * math.prod(ref.shape) for ref in scratch)
    return pltpu.CompilerParams(vmem_limit_bytes=mib * 1024 * 1024 + held + held // 4)


def up8(n):
    return -(-n // 8) * 8


def halo_cells():
    need, above = [], 0
    for level in range(FIRST):
        need.append(above + 4)
        above = -(-need[-1] // 2)
    f = 0
    for level in reversed(range(FIRST)):
        inner = max(need[level], 2 * f + 1)
        f = inner + (4 if level == 0 else 3)
    unit = 2**FIRST
    return -(-f // unit) * unit


def iota(shape, axis):
    return lax.broadcasted_iota(jnp.int32, shape, axis)


def rows(t, off=0):
    first, count = t
    start = first * 8 if isinstance(first, int) else pl.multiple_of(first * 8, 8)
    return pl.ds(start + (PAD + off), 8 * count)


def over(lo, hi, most, body):
    steps = -(-(hi - lo) // most)
    size = -(-(hi - lo) // steps)
    if steps == 1:
        body((lo, size))
        return

    def step(i, carry):
        body((jnp.minimum(lo + i * size, hi - size), size))
        return carry

    lax.fori_loop(0, steps, step, 0)


def dot(a, b):
    return jnp.dot(a, b, precision=HI, preferred_element_type=F32)


def pick_dot(x, pick, pieces=3):
    pick = pick.astype(jnp.bfloat16)
    total = None
    for n in range(pieces):
        piece = x.astype(jnp.bfloat16)
        part = jnp.dot(piece, pick, preferred_element_type=F32)
        total = part if total is None else total + part
        if n < pieces - 1:
            x = x - piece.astype(F32)
    return total


def prep_kernel(watt_hbm, cat_hbm, u_hbm, sub_hbm, planes, a_ref, b_ref, watt, cat_ref, sub_ref, sems, *, halo):
    layers, height, width = u_hbm.shape
    copies = [
        pltpu.make_async_copy(source, target, sems.at[n])
        for n, (source, target) in enumerate(
            ((u_hbm, planes.at[pl.ds(0, layers)]), (sub_hbm, sub_ref), (cat_hbm, cat_ref), (watt_hbm, watt))
        )
    ]
    for copy in copies:
        copy.start()
    even = lax.axis_index("gy") % 2 == 0

    def send(q):
        turned = planes[q].T
        low, high = turned[:halo], turned[width - halo :]
        a_ref[q] = jnp.where(even, high, low)
        b_ref[q] = jnp.where(even, low, high)

    for copy in copies:
        copy.wait()
    cat = cat_ref[...]
    power = jnp.zeros(cat.shape, F32)
    for n in range(watt.shape[0]):
        power = power + jnp.where(cat == n, watt[n], 0.0)
    spread_r = (iota((height, cat.shape[0]), 0) // TILE == iota((height, cat.shape[0]), 1)).astype(F32)
    spread_c = (iota((cat.shape[1], width), 1) // TILE == iota((cat.shape[1], width), 0)).astype(F32)
    planes[2 * layers] = dot(dot(spread_r, power), spread_c)
    for q in range(2 * layers + 1):
        if layers <= q < 2 * layers:
            planes[q] = (sub_ref[q - layers] + 1).astype(F32)
        send(q)


def split_kernel(own, ra, rb, out, a_ref, b_ref, scr, *, halo):
    count, height, width = own.shape
    layers = count // 2
    even_y, even_x = lax.axis_index("gy") % 2 == 0, lax.axis_index("gx") % 2 == 0
    half, hh = height // 2, halo // 2
    source, target = iota((width + LANES, 2 * LANES), 0), iota((width + LANES, 2 * LANES), 1)
    cell = 2 * (target % LANES) + target // LANES
    want = jnp.where(
        cell < halo, width + cell, jnp.where(cell < halo + width, cell - halo, cell)
    )
    pick = ((source == want) & (cell < 2 * halo + width)).astype(F32)
    planes = []
    for q in range(count):
        left = jnp.where(even_y, rb[q], ra[q])
        right = jnp.where(even_y, ra[q], rb[q])
        sides = jnp.concatenate([left, right, jnp.zeros((LANES - 2 * halo, height), F32)], 0).T
        planes.append(jnp.concatenate([own[q], sides], 1))
    first = pick_dot(jnp.concatenate(planes[:layers] + planes[2 * layers :], 0), pick, 2)
    second = pick_dot(jnp.concatenate(planes[layers : 2 * layers], 0), pick, 1)
    for q in range(2 * layers + 1):
        if layers <= q < 2 * layers:
            both = second[(q - layers) * height : (q - layers + 1) * height]
        else:
            at = q if q < layers else layers
            both = first[at * height : (at + 1) * height]
        scr[q % 2, 0] = both[:, :LANES]
        scr[q % 2, 1] = both[:, LANES:]
        for p in range(2):
            for j in range(2):
                z = scr[q % 2, j, pl.ds(p, half, stride=2), :]
                out[q, 2 * p + j] = z
                at = (4 * q + 2 * p + j) * hh
                first_rows, last_rows = z[:hh], z[half - hh :]
                a_ref[at : at + hh] = jnp.where(even_x, last_rows, first_rows)
                b_ref[at : at + hh] = jnp.where(even_x, first_rows, last_rows)


def split_block(s, colour, t, layers):
    u, at = s["u"], rows(t)
    other = {
        (p, j, k): u[2 * p + j, k, at]
        for k in range(layers)
        for p in range(2)
        for j in range(2)
        if (p + j + k) % 2 != colour
    }
    for k in range(layers):
        for p in range(2):
            for j in range(2):
                if (p + j + k) % 2 != colour:
                    continue
                pj = 2 * p + j
                total = s["f"][pj, k, at] + s["fri"][j, k, at] * other[1 - p, j, k]
                if p == 0:
                    total += s["fro"][j, k, at] * u[2 + j, k, rows(t, -1)]
                else:
                    total += s["fro"][j, k, rows(t, 1)] * u[j, k, rows(t, 1)]
                beside = other[p, 1 - j, k]
                total += s["fci"][p, k, at] * beside
                if j == 0:
                    total += s["fco"][p, k, at] * pltpu.roll(beside, 1, 1)
                else:
                    total += s["fcr"][p, k, at] * pltpu.roll(beside, LANES - 1, 1)
                if k > 0:
                    total += s["fl"][pj, k, at] * other[p, j, k - 1]
                if k < layers - 1:
                    total += s["fl"][pj, k + 1, at] * other[p, j, k + 1]
                yield pj, k, total


def split_half(s, colour, lo, hi, layers):
    def body(t):
        for pj, k, total in split_block(s, colour, t, layers):
            s["u"][pj, k, rows(t)] = total * s["invd"][pj, k, rows(t)]

    over(lo, hi, MOST["split"], body)


def split_sweeps(s, lo, hi, layers):
    for sweep in range(2):
        split_half(s, 0, lo, hi, layers)
        split_half(s, 1, lo, hi, layers)


def geometry(layers, width):
    assert width <= LANES
    fold = max(f for f in range(1, layers + 1) if layers % f == 0 and f * width <= LANES)
    return fold, width, layers // fold


def places(extent, geo):
    lane = iota(extent, 1)
    group = jnp.zeros(extent, jnp.int32)
    for g in range(1, geo[0] + 1):
        if g * geo[1] < LANES:
            group = group + (lane >= g * geo[1]).astype(jnp.int32)
    return group, lane - group * geo[1]


def odd_cells(t, geo):
    extent = (8 * t[1], LANES)
    group, col = places(extent, geo)
    return (iota(extent, 0) + col + group * geo[2]) % 2


def nat_setup(s, factor):
    fold, width, deep = s["geo"]
    height = s["lat"].shape[1]
    c = 0.5 * factor

    def body(t):
        at = rows(t)
        group, col = places((8 * t[1], LANES), s["geo"])
        first, last = col == 0, col == width - 1
        between = None
        for k in range(deep):
            lat, stor, vert = s["lat"][k, at], s["stor"][k, at], s["vert"][k, at]
            above = c * (lat + s["lat"][k, rows(t, -1)])
            below = c * (lat + s["lat"][k, rows(t, 1)])
            before = c * (lat + jnp.where(first, 0.0, pltpu.roll(lat, 1, 1)))
            after = c * (lat + jnp.where(last, 0.0, pltpu.roll(lat, LANES - 1, 1)))
            diag = stor + above + below + before + after
            if k > 0:
                face = 0.5 * (vert + s["vert"][k - 1, at])
                s["wl"][k, at] = face
                diag += face
            elif fold > 1:
                between = 0.5 * (vert + pltpu.roll(s["vert"][deep - 1, at], width, 1))
                between = jnp.where((group > 0) & (group < fold), between, 0.0)
                s["wl"][0, at] = between
                diag += between
            if k < deep - 1:
                diag += 0.5 * (vert + s["vert"][k + 1, at])
            elif fold > 1:
                diag += pltpu.roll(between, LANES - width, 1)
            inside = stor > 0.0
            s["wr"][k, at] = above
            s["wc"][k, at] = jnp.where(first, 0.0, before)
            s["wcr"][k, at] = jnp.where(last, 0.0, after)
            s["diag"][k, at] = diag
            s["invd"][k, at] = jnp.where(inside, 1.0 / jnp.where(inside, diag, 1.0), 0.0)

    s["wr"][:, height - PAD :] = jnp.zeros((deep, PAD, LANES), F32)
    over(0, (height - 2 * PAD) // 8, MOST["setup"], body)


def nat_block(s, t):
    u, at = s["u"], rows(t)
    fold, width, deep = s["geo"]
    mid = [u[k, at] for k in range(deep)]
    wl = s["wl"][0, at] if fold > 1 else None
    between = None if wl is None else pltpu.roll(wl * mid[0], LANES - width, 1)
    for k in range(deep):
        total = s["f"][k, at] + s["wr"][k, at] * u[k, rows(t, -1)]
        total += s["wr"][k, rows(t, 1)] * u[k, rows(t, 1)]
        beside = s["wc"][k, at] * pltpu.roll(mid[k], 1, 1)
        beside += s["wcr"][k, at] * pltpu.roll(mid[k], LANES - 1, 1)
        if k > 0:
            total += wl * mid[k - 1]
        elif fold > 1:
            total += wl * pltpu.roll(mid[deep - 1], width, 1)
        if k < deep - 1:
            wl = s["wl"][k + 1, at]
            total += wl * mid[k + 1]
        elif fold > 1:
            total += between
        yield k, total + beside, mid[k]


def nat_half(s, colour, lo, hi):
    def body(t):
        odd = odd_cells(t, s["geo"])
        for k, total, old in nat_block(s, t):
            value = total * s["invd"][k, rows(t)]
            s["u"][k, rows(t)] = jnp.where(odd == (colour + k) % 2, value, old)

    over(lo, hi, MOST["nat"], body)


def nat_first(s, lo, hi):
    deep, height, _ = s["u"].shape
    zeros = jnp.zeros((deep, PAD, LANES), F32)
    s["u"][:, :PAD] = zeros
    s["u"][:, height - PAD :] = zeros

    def body(t):
        odd = odd_cells(t, s["geo"])
        for k in range(deep):
            value = s["f"][k, rows(t)] * s["invd"][k, rows(t)]
            s["u"][k, rows(t)] = jnp.where(odd == k % 2, value, 0.0)

    over(lo, hi, MOST["first"], body)


def nat_residual(s, res, lo, hi):
    def body(t):
        for k, total, old in nat_block(s, t):
            res[k, rows(t)] = total - s["diag"][k, rows(t)] * old

    over(lo, hi, MOST["residual"], body)


def nat_down(s, res, steps):
    nat_first(s, 0, steps)
    for colour in (1, 0, 1):
        nat_half(s, colour, 0, steps)
    nat_residual(s, res, 0, steps)


def move(parts, a, b, relation, scale):
    jobs = {}
    for ka in range(a[2]):
        for kb in range(b[2]):
            key = tuple(
                (ga, gb)
                for ga in range(a[0])
                for gb in range(b[0])
                if ga * a[2] + ka == gb * b[2] + kb
            )
            if key:
                jobs.setdefault(key, []).append((ka, kb))
    c, m = iota((LANES, LANES), 0), iota((LANES, LANES), 1)
    out = [None] * b[2]
    count = parts[0].shape[0]
    for key, members in jobs.items():
        hit = None
        for ga, gb in key:
            ca, mb = c - ga * a[1], m - gb * b[1]
            here = (ca >= 0) & (ca < a[1]) & (mb >= 0) & (mb < b[1]) & relation(ca, mb)
            hit = here if hit is None else hit | here
        moved = pick_dot(
            jnp.concatenate([parts[ka] for ka, _ in members], 0), jnp.where(hit, scale, 0.0), 2
        )
        for n, (_, kb) in enumerate(members):
            part = moved[n * count : (n + 1) * count]
            out[kb] = part if out[kb] is None else out[kb] + part
    return out


def pair_rows(ref, k, start, count):
    part = ref[k, pl.ds(start, count, stride=2), :]
    return part + ref[k, pl.ds(start + 1, count, stride=2), :]


def restrict_all(pairs, a, b):
    deep, height = pairs[0][1].shape[0], pairs[0][1].shape[1] - 2 * PAD
    zeros = jnp.zeros((deep, PAD, LANES), F32)
    for _, target in pairs:
        target[:, :PAD] = zeros
        target[:, PAD + height :] = zeros
    parts = [
        jnp.concatenate([pair_rows(source, k, PAD, height) for source, _ in pairs], 0)
        for k in range(a[2])
    ]
    out = move(parts, a, b, lambda c, m: c // 2 == m, 0.25)
    for n, (_, target) in enumerate(pairs):
        for k in range(deep):
            target[k, PAD : PAD + height] = out[k][n * height : (n + 1) * height]


def prolong_into(s, u_in, coarse, geo, mask):
    deep, height, _ = s["u"].shape
    n = (height - 2 * PAD) // 2
    tall = up8(n)
    parts = [coarse(k)[:tall] for k in range(geo[2])]
    out = move(parts, geo, s["geo"], lambda c, m: c == m // 2, 1.0)
    for k in range(deep):
        wide = out[k][:n]
        for p in range(2):
            at = pl.ds(PAD + p, n, stride=2)
            add = wide
            if mask:
                add = jnp.where(s["invd"][k, at, :] > 0.0, wide, 0.0)
            s["u"][k, at, :] = u_in[k, at, :] + add


def nat_up(s, lo, hi):
    for sweep in range(2):
        nat_half(s, 0, lo, hi)
        nat_half(s, 1, lo, hi)


SPLIT_KEPT = ("u", "f", "invd", "fri", "fro", "fci", "fco", "fcr", "fl")
NAT_KEPT = ("u", "f", "invd", "wr", "wc", "wcr", "wl")
NAT_OTHER = ("lat", "vert", "stor", "diag")


def pack_own(payload, last, res, layers, mine, off):
    group = 4 * mine
    per = LANES // group
    quantities = (res, last["lat"], last["vert"], last["stor"])
    parts = [
        jnp.concatenate([pair_rows(ref, k, PAD + off, mine) for ref in quantities], 0)
        for k in range(last["geo"][2])
    ]
    packed = move(
        parts, last["geo"], (1, mine, layers), lambda c, m: (c >= off) & ((c - off) // 2 == m), 0.25
    )
    for wide in range(-(-layers // per)):
        total = jnp.zeros((mine, LANES), F32)
        for n in range(wide * per * 4, min(layers, (wide + 1) * per) * 4):
            part = packed[n // 4][n % 4 * mine : (n % 4 + 1) * mine]
            base = (n - wide * per * 4) * mine
            total += pltpu.roll(part, base, 1) if base else part
        payload[wide * mine : (wide + 1) * mine] = total


def look_up(s, first, heat, kinds, lo, hi):
    layers = s["u"].shape[1]

    def look(t):
        for k in range(layers):
            sums = [None, None, None]
            for pj in range(4):
                at = (pj, k, rows(t))
                label = s["diag"][at]
                value = [jnp.zeros_like(label)] * 3
                for n in range(kinds):
                    hit = label == float(n + 1)
                    value = [jnp.where(hit, s["table"][i * kinds + n], value[i]) for i in range(3)]
                for i, name in enumerate(("lat", "vert", "stor")):
                    s[name][at] = value[i]
                    sums[i] = value[i] if sums[i] is None else sums[i] + value[i]
                f = value[2] * s["u"][at]
                if k == 0:
                    f = f + heat[pj, rows(t)]
                s["f"][at] = f
            for i, name in enumerate(("lat", "vert", "stor")):
                first[name][k, rows(t)] = sums[i] * 0.25

    over(lo, hi, MOST["look"], look)


def split_setup(s, lo, hi):
    layers = s["u"].shape[1]

    def faces(t):
        at = rows(t)
        for k in range(layers):
            lat = [s["lat"][pj, k, at] for pj in range(4)]
            inner_r = [0.5 * (lat[j] + lat[2 + j]) for j in range(2)]
            before_r = [0.5 * (s["lat"][2 + j, k, rows(t, -1)] + lat[j]) for j in range(2)]
            after_r = [0.5 * (lat[2 + j] + s["lat"][j, k, rows(t, 1)]) for j in range(2)]
            inner_c = [0.5 * (lat[2 * p] + lat[2 * p + 1]) for p in range(2)]
            before_c = [0.5 * (pltpu.roll(lat[2 * p + 1], 1, 1) + lat[2 * p]) for p in range(2)]
            after_c = [0.5 * (lat[2 * p + 1] + pltpu.roll(lat[2 * p], LANES - 1, 1)) for p in range(2)]
            for x in range(2):
                s["fri"][x, k, at] = inner_r[x]
                s["fro"][x, k, at] = before_r[x]
                s["fci"][x, k, at] = inner_c[x]
                s["fco"][x, k, at] = before_c[x]
                s["fcr"][x, k, at] = after_c[x]
            for p in range(2):
                for j in range(2):
                    pj = 2 * p + j
                    stor = s["stor"][pj, k, at]
                    diag = stor + inner_r[j] + (after_r[j] if p else before_r[j])
                    diag += inner_c[p] + (after_c[p] if j else before_c[p])
                    vert = s["vert"][pj, k, at]
                    if k > 0:
                        face = 0.5 * (vert + s["vert"][pj, k - 1, at])
                        s["fl"][pj, k, at] = face
                        diag += face
                    if k < layers - 1:
                        diag += 0.5 * (vert + s["vert"][pj, k + 1, at])
                    inside = stor > 0.0
                    s["invd"][pj, k, at] = jnp.where(inside, 1.0 / jnp.where(inside, diag, 1.0), 0.0)
                    s["diag"][pj, k, at] = diag

    over(lo, hi, MOST["faces"], faces)


SHARED = SPLIT_KEPT + ("lat", "vert", "stor", "diag", "heat", "lat1", "vert1", "stor1", "table")


def center_kernel(*refs, halo, half, kinds):
    tables, sp, out = refs[:3], refs[3], refs[4:]
    s = dict(zip(SHARED, out))
    first = {name: s[name + "1"] for name in ("lat", "vert", "stor")}
    layers, height, hh = s["u"].shape[1], s["u"].shape[2], halo // 2
    body_rows = slice(PAD + hh, PAD + hh + half)
    zeros = jnp.zeros((PAD, LANES), F32)
    for pj in range(4):
        for k in range(layers):
            for name in ("u", "lat"):
                s[name][pj, k, :PAD] = zeros
                s[name][pj, k, height - PAD :] = zeros
            s["u"][pj, k, body_rows] = sp[k, pj]
            s["diag"][pj, k, body_rows] = sp[layers + k, pj]
        s["heat"][pj, body_rows] = sp[2 * layers, pj]
    for ref in first.values():
        for k in range(layers):
            ref[k, :PAD] = zeros
            ref[k, height - PAD :] = zeros
    for i in range(3):
        for n in range(kinds):
            s["table"][i * kinds + n] = jnp.full((8, LANES), tables[i][n], F32)
    look_up(s, first, s["heat"], kinds, *bounds(hh, half, 0))
    split_setup(s, *bounds(hh, half, 1))


def bounds(hh, half, inner):
    if inner:
        return -(-(hh + 1) // 8), (hh + half - 1) // 8
    return hh // 8, -(-(hh + half) // 8)


def down_kernel(*refs, halo, half, kinds, geos):
    ra, rb = refs[:2]
    refs = list(refs[2 + len(SHARED) :])
    s = dict(zip(SHARED, refs[: len(SHARED)]))
    refs = refs[len(SHARED) :]
    nats = [{} for level in range(1, FIRST)]
    for n, now in enumerate(nats):
        now.update(zip(NAT_KEPT, refs[: len(NAT_KEPT)]), geo=geos[n])
        refs = refs[len(NAT_KEPT) :]
    payload = refs.pop(0)
    heat = s["heat"]
    for n, now in enumerate(nats):
        for name in NAT_OTHER:
            now[name] = s[name + "1"] if n == 0 and name != "diag" else refs.pop(0)
    ress = [refs.pop(0) for level in range(1, FIRST)]
    layers = s["u"].shape[1]
    height = s["u"].shape[2]
    hh = halo // 2
    steps = (height - 2 * PAD) // 8
    even = lax.axis_index("gx") % 2 == 0
    zeros = jnp.zeros((PAD, LANES), F32)

    def place(ref, index, q, pj):
        at = (4 * q + pj) * hh
        first, second = ra[at : at + hh], rb[at : at + hh]
        ref[index + (slice(PAD, PAD + hh),)] = jnp.where(even, second, first)
        ref[index + (slice(PAD + hh + half, PAD + 2 * hh + half),)] = jnp.where(even, first, second)

    for pj in range(4):
        for k in range(layers):
            place(s["u"], (pj, k), k, pj)
            place(s["diag"], (pj, k), layers + k, pj)
        place(heat, (pj,), 2 * layers, pj)
    for j in range(2):
        for k in range(layers):
            s["fro"][j, k, height - PAD :] = zeros
    first = nats[0]
    for ref in [first["f"]] + ress:
        for k in range(ref.shape[0]):
            ref[k, :PAD] = zeros
            ref[k, ref.shape[1] - PAD :] = zeros
    lo, hi = bounds(hh, half, 1)
    for begin, end in ((0, lo), (hi, steps)):
        look_up(s, first, heat, kinds, begin, end)
    for begin, end in ((0, lo), (hi, steps)):
        split_setup(s, begin, end)
    split_sweeps(s, 0, steps, layers)

    def remain(t):
        sums = {}
        for pj, k, total in split_block(s, 0, t, layers):
            r = total - s["diag"][pj, k, rows(t)] * s["u"][pj, k, rows(t)]
            sums[k] = sums[k] + r if k in sums else r
            if pj >= 2:
                first["f"][k, rows(t)] = sums[k] * 0.25

    over(0, steps, MOST["remain"], remain)

    for level in range(1, FIRST):
        now = nats[level - 1]
        nat_setup(now, 0.25**level)
        count = (now["u"].shape[1] - 2 * PAD) // 8
        nat_down(now, ress[level - 1], count)
        if level < FIRST - 1:
            below = nats[level]
            pairs = [(now[name], below[name]) for name in ("lat", "vert", "stor")]
            restrict_all(pairs + [(ress[level - 1], below["f"])], now["geo"], below["geo"])

    pack_own(payload, nats[-1], ress[-1], layers, 2 * half >> FIRST, halo >> (FIRST - 1))


def mid_kernel(own, ra, rb, ta, tb, *refs, geos):
    refs = list(refs)
    count = LOCAL - FIRST
    nats = []
    for n in range(count):
        nats.append(dict(zip(NAT_KEPT, refs[: len(NAT_KEPT)]), geo=geos[n]))
        refs = refs[len(NAT_KEPT) :]
    payload = refs.pop(0)
    for n in range(count):
        for name in NAT_OTHER:
            nats[n][name] = refs.pop(0)
    ress = refs
    layers = geos[0][0] * geos[0][2]
    mine = own.shape[0] // layers
    assert geos[0][0] == 1
    even_y, even_x = lax.axis_index("gy") % 2 == 0, lax.axis_index("gx") % 2 == 0
    zeros = jnp.zeros((PAD, LANES), F32)
    for now, res in zip(nats, ress):
        for ref in [now[name] for name in ("lat", "vert", "stor", "f")] + [res]:
            for k in range(ref.shape[0]):
                ref[k, :PAD] = zeros
                ref[k, ref.shape[1] - PAD :] = zeros
    group = iota((mine, LANES), 1) // mine

    def assemble(v, middle_of, a_of, b_of):
        for k in range(layers):
            lines = slice(k * mine, (k + 1) * mine)
            middle, a, b = middle_of(lines), a_of(lines), b_of(lines)
            left, right = jnp.where(even_y, b, a), jnp.where(even_y, a, b)
            middle, right = pltpu.roll(middle, mine, 1), pltpu.roll(right, 2 * mine, 1)
            for n, name in enumerate(("f", "lat", "vert", "stor")):
                value = jnp.where(group == (n + 1) % 4, middle, right)
                value = jnp.where(group == n, left, value)
                value = jnp.where(group == (n + 3) % 4, 0.0, value)
                if n:
                    value = pltpu.roll(value, LANES - n * mine, 1)
                nats[0][name][k, PAD + v * mine : PAD + (v + 1) * mine] = value

    def rows_from(ref):
        return [lambda lines, n=n: ref[n, lines] for n in range(3)]

    def outer(above, below):
        assemble(0, *rows_from(above))
        assemble(2, *rows_from(below))

    assemble(1, *[lambda lines, ref=ref: ref[lines] for ref in (own, ra, rb)])
    pl.when(even_x)(lambda: outer(tb, ta))
    pl.when(jnp.logical_not(even_x))(lambda: outer(ta, tb))
    for n, level in enumerate(range(FIRST, LOCAL)):
        now = nats[n]
        nat_setup(now, 0.25**level)
        nat_down(now, ress[n], (now["u"].shape[1] - 2 * PAD) // 8)
        if n < count - 1:
            pairs = [(now[name], nats[n + 1][name]) for name in ("lat", "vert", "stor")]
            restrict_all(pairs + [(ress[n], nats[n + 1]["f"])], geos[n], geos[n + 1])
    pack_own(payload, nats[-1], ress[-1], layers, mine >> count, mine >> (count - 1))


def conjugate(s):
    fold, width, deep = s["geo"]
    n = s["u"].shape[1] - 2 * PAD
    here, after = slice(PAD, PAD + n), slice(PAD + 1, PAD + 1 + n)
    row = iota((n, LANES), 0)
    planes = range(deep)
    above = [jnp.where(row > 0, s["wr"][k, here], 0.0) for k in planes]
    below = [jnp.where(row < n - 1, s["wr"][k, after], 0.0) for k in planes]
    before, behind, diag, inv, r = [
        [s[name][k, here] for k in planes] for name in ("wc", "wcr", "diag", "invd", "f")
    ]
    faces = [s["wl"][k, here] if k or fold > 1 else None for k in planes]

    def apply(v):
        out = []
        for k in planes:
            total = above[k] * pltpu.roll(v[k], 1, 0) + below[k] * pltpu.roll(v[k], n - 1, 0)
            total += before[k] * pltpu.roll(v[k], 1, 1) + behind[k] * pltpu.roll(v[k], LANES - 1, 1)
            if k > 0:
                total += faces[k] * v[k - 1]
            elif fold > 1:
                total += faces[0] * pltpu.roll(v[deep - 1], width, 1)
            if k < deep - 1:
                total += faces[k + 1] * v[k + 1]
            elif fold > 1:
                total += pltpu.roll(faces[0] * v[0], LANES - width, 1)
            out.append(diag[k] * v[k] - total)
        return out

    def inner(a, b):
        total = a[0] * b[0]
        for x, y in zip(a[1:], b[1:]):
            total += x * y
        return jnp.sum(jnp.sum(total, axis=0, keepdims=True), axis=1, keepdims=True)

    def step(_, carry):
        e, r, p = carry[:deep], carry[deep : 2 * deep], carry[2 * deep :]
        q = apply(p)
        z = [x * y for x, y in zip(r, inv)]
        w = [x * y for x, y in zip(q, inv)]
        rz, pq, zq, wq = inner(r, z), inner(p, q), inner(z, q), inner(w, q)
        alpha = rz / pq
        beta = (rz + alpha * (alpha * wq - 2.0 * zq)) / rz
        e = [x + alpha * y for x, y in zip(e, p)]
        r = [x - alpha * y for x, y in zip(r, q)]
        p = [x - alpha * y + beta * d for x, y, d in zip(z, w, p)]
        return (*e, *r, *p)

    start = (*[jnp.zeros((n, LANES), F32)] * deep, *r, *[x * y for x, y in zip(r, inv)])
    out = lax.fori_loop(0, COARSE_ITERS, step, start, unroll=3)
    for k in planes:
        s["u"][k, here] = out[k]


WHOLE = ("u", "f", "invd", "wr", "wc", "wcr", "wl", "lat", "vert", "stor", "diag")


def up_kernel(*refs, halo, half, spans, geos, whole_geos):
    refs = list(refs)
    gathered, traded = refs.pop(0), refs.pop(0)
    s = dict(zip(SPLIT_KEPT, refs[: len(SPLIT_KEPT)]))
    refs = refs[len(SPLIT_KEPT) :]
    nats = []
    for geo in geos:
        nats.append(dict(zip(NAT_KEPT, refs[: len(NAT_KEPT)]), geo=geo))
        refs = refs[len(NAT_KEPT) :]
    out = refs.pop(0)
    wholes = []
    for geo in whole_geos:
        wholes.append(dict(zip(WHOLE, refs[: len(WHOLE)]), geo=geo))
        refs = refs[len(WHOLE) :]
    ress = [refs.pop(0) for level in range(LOCAL, LEVELS)]
    fresh = [refs.pop(0) for level in range(LOCAL)]
    wider = refs.pop(0)
    nx, ny = spans
    layers = s["u"].shape[1]
    top = wholes[0]
    fold, width, deep = top["geo"]
    mine = 2 * half >> LOCAL
    group = 4 * mine
    per = LANES // group
    lane = iota((mine, LANES), 1)

    for whole in wholes:
        planes, height, _ = whole["u"].shape
        for name in ("u", "lat"):
            zeros = jnp.zeros((planes, PAD, LANES), F32)
            whole[name][:, :PAD] = zeros
            whole[name][:, height - PAD :] = zeros

    parity = lax.axis_index("gx") % 2

    def gather(x, core):
        at = pl.ds(pl.multiple_of(x * mine, 8) + PAD, mine)
        parts = []
        for wide in range(-(-layers // per)):
            lines = slice(wide * mine, (wide + 1) * mine)
            at_x = lax.div(x, 2) * ny
            turned = [
                jnp.where(parity == core, gathered[at_x + y, lines], traded[at_x + y, lines])
                for y in range(ny)
            ]
            parts.append([pltpu.roll(v, y * mine, 1) if y else v for y, v in enumerate(turned)])
        for k in range(deep):
            for n, name in enumerate(("f", "lat", "vert", "stor")):
                value = None
                for g in range(fold):
                    layer = g * deep + k
                    base = (layer % per) * group + n * mine
                    total = jnp.zeros((mine, LANES), F32)
                    for y in range(ny):
                        spot = (base + y * mine) % LANES
                        hit = (lane >= spot) & (lane < spot + mine)
                        total = jnp.where(hit, parts[layer // per][y], total)
                    turn = (g * width - base) % LANES
                    total = pltpu.roll(total, turn, 1) if turn else total
                    value = total if value is None else value + total
                top[name][k, at] = value

    def gather_some(step, carry):
        for n in range(8):
            gather(8 * step + n, n % 2)
        return carry

    lax.fori_loop(0, nx // 8, gather_some, 0)

    for n, level in enumerate(range(LOCAL, LEVELS)):
        now, below = wholes[n], wholes[n + 1]
        nat_setup(now, 0.25**level)
        nat_down(now, ress[n], (now["u"].shape[1] - 2 * PAD) // 8)
        pairs = [(now[name], below[name]) for name in ("lat", "vert", "stor")]
        restrict_all(pairs + [(ress[n], below["f"])], now["geo"], below["geo"])
    nat_setup(wholes[-1], 0.25**LEVELS)
    conjugate(wholes[-1])

    def planes_of(ref):
        return lambda k: ref[k, PAD : ref.shape[1] - PAD]

    for n in reversed(range(len(wholes) - 1)):
        now, below = wholes[n], wholes[n + 1]
        prolong_into(now, now["u"], planes_of(below["u"]), below["geo"], False)
        nat_up(now, 0, (now["u"].shape[1] - 2 * PAD) // 8)

    x, y = lax.axis_index("gx"), lax.axis_index("gy")
    reach = (2 * half >> FIRST) >> (LOCAL - FIRST)
    height = top["u"].shape[1]
    need = (nats[-1]["u"].shape[1] - 2 * PAD) // 2
    lanes = iota((height, LANES), 1)
    for layer in range(layers):
        g, k = layer // deep, layer % deep
        value = top["u"][k]
        if g:
            value = pltpu.roll(value, LANES - g * width, 1)
        wider[layer, :height] = jnp.where(lanes < width, value, 0.0)
        wider[layer, height:] = jnp.zeros((PAD, LANES), F32)
    begin = PAD + x * mine - reach
    turn = lax.rem(LANES + reach - y * mine, LANES)

    def coarse(k):
        return pltpu.roll(wider[k, pl.ds(begin, need)], turn, 1)

    coarse_geo = (1, nats[-1]["geo"][1] // 2, layers)
    margins, above = [], 0
    for level in range(LOCAL):
        margins.append(above + 4)
        above = -(-margins[-1] // 2)
    for level in reversed(range(1, LOCAL)):
        now = dict(nats[level - 1])
        before = now["u"]
        now["u"] = fresh[level]
        planes, height, _ = before.shape
        now["u"][:, :PAD] = jnp.zeros((planes, PAD, LANES), F32)
        now["u"][:, height - PAD :] = jnp.zeros((planes, PAD, LANES), F32)
        prolong_into(now, before, coarse, coarse_geo, level == LOCAL - 1)
        own = 2 * half >> level
        side = halo >> level if level < FIRST else (2 * half >> FIRST) >> (level - FIRST)
        reach = margins[level]
        nat_up(now, (side - reach) // 8, min(-(-(side + own + reach) // 8), (height - 2 * PAD) // 8))
        coarse, coarse_geo = planes_of(now["u"]), now["geo"]
        if level == FIRST:
            assert coarse_geo[0] == 1
            skip, blocks = side - (halo >> FIRST), now["u"]

            def coarse(k):
                return pltpu.roll(
                    blocks[k, PAD + skip : blocks.shape[1] - PAD], LANES - skip, 1
                )

            coarse_geo = (1, (2 * half + 2 * halo) >> FIRST, layers)

    now = dict(s)
    now["u"] = fresh[0]
    hh = halo // 2
    lo, hi = (hh - 2) // 8, -(-(hh + half + 2) // 8)
    steps = (s["u"].shape[2] - 2 * PAD) // 8

    def add(t):
        for k in range(layers):
            value = fresh[1][k, rows(t)]
            for pj in range(4):
                now["u"][pj, k, rows(t)] = s["u"][pj, k, rows(t)] + value

    over(lo - 1, min(hi + 1, steps), MOST["add"], add)
    split_sweeps(now, lo, hi, layers)
    source, target = iota((2 * LANES, 2 * half), 0), iota((2 * LANES, 2 * half), 1)
    pick = ((source % LANES == hh + target // 2) & (source // LANES == target % 2)).astype(F32)
    body_rows = slice(PAD + hh, PAD + hh + half)
    spots = [(k, p) for k in range(layers) for p in range(2)]
    both = [
        jnp.concatenate([now["u"][2 * p + j, k, body_rows] for k, p in spots], 0) for j in range(2)
    ]
    every = pick_dot(jnp.concatenate(both, 1), pick, 2)
    for n, (k, p) in enumerate(spots):
        out[k, pl.ds(p, half, stride=2), :] = every[n * half : (n + 1) * half]


def swap(values, axis, first):
    count = lax.axis_size(axis)
    pairs = [(i, i + 1) for i in range(first, count - 1, 2)]
    return lax.ppermute(values, axis, pairs + [(b, a) for a, b in pairs])


def shape(*dims):
    return jax.ShapeDtypeStruct(dims, F32)


def packed_shape(layers, mine):
    per = LANES // (4 * mine)
    return shape(-(-layers // per) * mine, LANES)


def other_scratch(shapes):
    out = []
    for d in shapes:
        out += [pltpu.VMEM(d, F32)] * len(NAT_OTHER)
    return out + [pltpu.VMEM(d, F32) for d in shapes]


def on_device(u0, sub, cat, planar, vertical, ratio, watt):
    nx, ny = lax.axis_size("gx"), lax.axis_size("gy")
    layers, height, width = u0.shape
    halo = halo_cells()
    half, hh = height // 2, halo // 2
    planes = 2 * layers + 1
    assert height == width == LANES and 2 * halo <= LANES and halo + half <= LANES

    own, a, b = pl.pallas_call(
        functools.partial(prep_kernel, halo=halo),
        out_shape=(shape(planes, height, width), shape(planes, halo, height), shape(planes, halo, height)),
        in_specs=[HBM] * 4,
        out_specs=(VMEM,) * 3,
        scratch_shapes=[
            pltpu.SMEM(watt.shape, F32),
            pltpu.VMEM(cat.shape, jnp.int32),
            pltpu.VMEM(sub.shape, jnp.int32),
            pltpu.SemaphoreType.DMA((4,)),
        ],
        compiler_params=limit(8),
        name="prep",
    )(*[pltpu.with_memory_space_constraint(x, pltpu.HBM) for x in (watt, cat, u0, sub)])
    a, b = swap(a, "gy", 0), swap(b, "gy", 1)

    lines = planes * 4 * hh
    sp, a, b = pl.pallas_call(
        functools.partial(split_kernel, halo=halo),
        out_shape=(shape(planes, 4, half, LANES), shape(lines, LANES), shape(lines, LANES)),
        in_specs=[VMEM] * 3,
        out_specs=(VMEM,) * 3,
        scratch_shapes=[pltpu.VMEM((2, 2, height, LANES), F32)],
        compiler_params=limit(20),
        name="split",
    )(own, a, b)
    a, b = swap(a, "gx", 0), swap(b, "gx", 1)

    tall = up8(half + 2 * hh) + 2 * PAD
    four, two = (4, layers, tall, LANES), (2, layers, tall, LANES)
    sides = [(height + 2 * halo) >> level for level in range(1, FIRST)]
    geos = [geometry(layers, side) for side in sides]
    assert geos[0][0] == 1
    nat_shapes = [(geo[2], up8(side) + 2 * PAD, LANES) for geo, side in zip(geos, sides)]
    sizes = [four if name in ("u", "f", "invd", "fl") else two for name in SPLIT_KEPT]
    sizes += [four] * 4 + [(4, tall, LANES)] + [nat_shapes[0]] * 3
    sizes.append((3 * planar.shape[0], 8, LANES))
    shared = pl.pallas_call(
        functools.partial(center_kernel, halo=halo, half=half, kinds=planar.shape[0]),
        out_shape=tuple(shape(*d) for d in sizes),
        in_specs=[SMEM] * 3 + [VMEM],
        out_specs=(VMEM,) * len(sizes),
        compiler_params=limit(24),
        name="center",
    )(planar, vertical, ratio, sp)
    kept = []
    for d in nat_shapes:
        kept += [shape(*d)] * len(NAT_KEPT)
    *saved, block = pl.pallas_call(
        functools.partial(
            down_kernel, halo=halo, half=half, kinds=planar.shape[0], geos=tuple(geos)
        ),
        out_shape=(*[shape(*d) for d in sizes], *kept, packed_shape(layers, height >> FIRST)),
        in_specs=[VMEM] * (2 + len(sizes)),
        out_specs=(VMEM,) * (len(sizes) + len(kept) + 1),
        scratch_shapes=other_scratch(nat_shapes)[3:],
        input_output_aliases={2 + n: n for n in range(len(sizes))},
        compiler_params=limit(26),
        name="down",
    )(a, b, *shared)
    saved = saved[: len(SPLIT_KEPT)] + saved[len(sizes) :]

    a, b = swap(block, "gy", 0), swap(block, "gy", 1)
    column = jnp.stack([block, a, b])
    above, below = swap(column, "gx", 0), swap(column, "gx", 1)
    mine = height >> FIRST
    assert 4 * mine <= LANES
    sides = [3 * mine >> n for n in range(LOCAL - FIRST)]
    block_geos = [geometry(layers, side) for side in sides]
    block_shapes = [(geo[2], up8(side) + 2 * PAD, LANES) for geo, side in zip(block_geos, sides)]
    kept = []
    for d in block_shapes:
        kept += [shape(*d)] * len(NAT_KEPT)
    *more, payload = pl.pallas_call(
        functools.partial(mid_kernel, geos=tuple(block_geos)),
        out_shape=(*kept, packed_shape(layers, height >> LOCAL)),
        in_specs=[VMEM] * 5,
        out_specs=(VMEM,) * (len(kept) + 1),
        scratch_shapes=other_scratch(block_shapes),
        compiler_params=limit(20),
        name="mid",
    )(block, a, b, above, below)
    saved += more
    nat_shapes += block_shapes

    assert nx % 8 == 0
    groups = [[x * ny + y for x in range(c, nx, 2) for y in range(ny)] for c in range(2)]
    sent = jnp.broadcast_to(payload[None], (nx // 2 * ny,) + payload.shape)
    gathered = lax.all_to_all(sent, ("gx", "gy"), 0, 0, axis_index_groups=groups)
    traded = swap(gathered, "gx", 0)

    whole_geos = [geometry(layers, ny * width >> level) for level in range(LOCAL, LEVELS + 1)]
    wholes = [
        (geo[2], up8(nx * height >> level) + 2 * PAD, LANES)
        for geo, level in zip(whole_geos, range(LOCAL, LEVELS + 1))
    ]
    scratch = []
    for d in wholes:
        scratch += [pltpu.VMEM(d, F32)] * len(WHOLE)
    scratch += [pltpu.VMEM(d, F32) for d in wholes[:-1]]
    scratch += [pltpu.VMEM(four, F32)] + [pltpu.VMEM(d, F32) for d in nat_shapes]
    scratch.append(pltpu.VMEM((layers, wholes[0][1] + PAD, LANES), F32))
    return pl.pallas_call(
        functools.partial(
            up_kernel,
            halo=halo,
            half=half,
            spans=(nx, ny),
            geos=tuple(geos + block_geos),
            whole_geos=tuple(whole_geos),
        ),
        out_shape=shape(layers, height, width),
        in_specs=[VMEM] * (2 + len(saved)),
        out_specs=VMEM,
        scratch_shapes=scratch,
        compiler_params=limit(16, scratch),
        name="up",
    )(gathered, traded, *saved)


def solution(mesh):
    placed = (P(None, "gx", "gy"), P(None, "gx", "gy"), P("gx", "gy"), P(), P(), P(), P())
    return jax.shard_map(
        on_device, mesh=mesh, in_specs=placed, out_specs=P(None, "gx", "gy"), check_vma=False
    )
```
